512 devices in a mesh: dp: 128 (over z, y, core), mp: 4 (over x).
Axes of the slice: x: 4, y: 8, z: 8, core: 2. Of those that a mesh axis runs over, the one named last changes fastest.
Arguments:
- bag_lengths: int32 [16, 16384], P('mp', 'dp'), may hold values from 1 to 8
- owners: int32 [16, 16384, 8, 1], P('mp', 'dp'), may hold values from 0 to 127; in each aligned block of 1024 rows (0 to 1023, 1024 to 2047, ..., all dimensions but the last counted through in order) at most 16 rows name the same one
- row_slots: int32 [16, 16384, 8], P('mp', 'dp'), may hold values from 0 to 511
- admit_mask: int32 [16, 16384, 8], P('mp', 'dp'), may hold values 0 or 1
- expired: int32 [16, 65536], P('mp', 'dp'), may hold values 0 or 1
- embeddings: float32 [16, 65536, 128], P('mp', 'dp'), may hold values from -3 to 3
- accumulator: float32 [16, 65536], P('mp', 'dp'), may hold values from 0.001 to 0.01
- hidden_weight: bfloat16 [2048, 1024], P(None, 'mp'), may hold values from -0.125 to 0.125
- output_weight: float32 [1024], P('mp'), may hold values from -0.9 to 0.9
- labels: int32 [16384], P('dp'), may hold values 0 or 1
Outputs:
- new_table: float32 [16, 65536, 128], P('mp', 'dp')
- new_accum: float32 [16, 65536], P('mp', 'dp')
- weight_grad: bfloat16 [2048, 1024], P(None, 'mp')
- logits: float32 [16384], P('dp')
The draws below stay inside these ranges and needn't reach their ends.
Inputs may be any that keep to these rules, and one draw needn't show every extreme that they name: Among the 128 x 8 lookups of one index of dp into one table (aligned blocks of owners' rows), at most 16 name the same owner; in some blocks one owner is named exactly 16 times.
All inputs are finite; a program needn't handle non-finite values. No bound on the sum of `admit_mask` or of `expired` or of `labels` on one device may be relied on, other than what follows from the above.
Results may differ from the reference program's by a relative error of at most 0.0085.
Values may be sent and summed in bfloat16 or wider, within the bound.
No kernel may reach another device: no remote copies, remote signals or barrier semaphores. Data moves between devices by JAX's collectives and lax.ppermute only.
A program may use at most 64 MiB of HBM per device.

```python
import math
import jax
import jax.numpy as jnp
import numpy as np
from jax import lax

TABLES = 16
EMB = 128
HIDDEN_SIZE = 1024
BAG = 8
ROWS_DEV = 512
TOK_DEV = 128
TOKENS = 16384
ROWS = 65536
CAP = 16
N_DP = 128


def set_ends(array, key, least, high):
    longest = array.shape.index(max(array.shape))
    spots = []
    for shift in (0, 1):
        where = [jax.random.randint(jax.random.fold_in(key, axis), (), 0, length) for axis, length in enumerate(array.shape)]
        where[longest] = (where[longest] + shift) % array.shape[longest]
        spots.append(tuple(where))
    return array.at[spots[0]].set(least).at[spots[1]].set(high)


def level_of(key, extent, cuts, smallest, top_value):
    gain, own = 1.0, jax.random.fold_in(key, 6)
    for dim, blocks in cuts:
        steps = jnp.exp(jax.random.uniform(jax.random.fold_in(own, dim), (blocks,), jnp.float32, smallest / len(cuts), top_value / len(cuts)))
        gain = gain * jnp.repeat(steps, extent[dim] // blocks).reshape([-1 if axis == dim else 1 for axis in range(len(extent))])
    return gain


def rank_table(count, skew):
    portions = [(1 << 20) // math.isqrt(rank ** skew) + 1 for rank in range(1, count + 1)]
    spread = 1 + sum(portions) // (1 << 30)
    return np.cumsum(np.array([max(1, weight // spread) for weight in portions]))


def skewed_ids(stream_key, extent, number_of, slope):
    table = rank_table(number_of, slope)
    ticket = jax.random.randint(jax.random.fold_in(stream_key, 1), extent, 0, int(table[number_of - 1]))
    rank = jnp.searchsorted(jnp.asarray(table, jnp.int32), ticket, side="right")
    return jax.random.permutation(jax.random.fold_in(stream_key, 2), number_of)[rank].astype(jnp.int32)


def deal_out(stream_key, own, number, rows, number_of, top, bound, skew):
    ranking = jax.random.permutation(stream_key, number_of)
    heavy_load, common = portions_of(number_of, rows * top, bound, skew, True), portions_of(number_of, rows * top, bound, skew, False)
    places = jnp.arange(number_of)

    def named(tallies, turn):
        used = int((tallies > 0).sum())
        fixed = max(1, used // 4)
        shifted = fixed + (places - fixed + turn * (used - fixed)) % max(1, number_of - fixed)
        return jnp.zeros((number_of,), jnp.int32).at[ranking[jnp.where(places < fixed, places, shifted)]].set(jnp.asarray(tallies, jnp.int32))

    tallies = jnp.where(number % 4 == 0, named(heavy_load, number // 4), named(common, number - number // 4 - 1))
    mixed = jax.random.permutation(jax.random.fold_in(own, 3), number_of)
    giver, receiver = mixed[0:number_of // 2 * 2:2], mixed[1:number_of // 2 * 2:2]
    margin = jnp.minimum(tallies[giver] - 1, bound - tallies[receiver]) // 2
    margin = jnp.where((giver == ranking[0]) | (receiver == ranking[0]) | (tallies[receiver] == 0), 0, jnp.maximum(margin, 0))
    shifted = jax.random.randint(jax.random.fold_in(own, 4), (number_of // 2,), 0, 1 << 20) % (margin + 1)
    tallies = tallies.at[giver].add(-shifted).at[receiver].add(shifted)
    items = jnp.searchsorted(jnp.cumsum(tallies), jnp.arange(rows * top), side="right").astype(jnp.int32)
    listing = items.reshape(top, rows).T
    listing = listing[jax.random.permutation(jax.random.fold_in(own, 1), rows)]
    turn = jax.random.randint(jax.random.fold_in(own, 2), (rows, 1), 0, top)
    return jnp.take_along_axis(listing, (jnp.arange(top)[None, :] + turn) % top, axis=1)


def portions_of(amount, total, bound, slope, full):
    portions = [(1 << 20) // math.isqrt(grade ** slope) + 1 for grade in range(1, amount + 1)]
    largest = bound if full else min(bound, max(-(-total // amount), total * portions[0] // sum(portions)))
    least = 1 if total - largest >= amount - 1 else 0
    holding, spare = [largest] + [least] * (amount - 1), total - largest - least * (amount - 1)
    while spare > 0:
        candidates = [i for i in range(1, amount) if holding[i] < largest] or [i for i in range(1, amount) if holding[i] < bound]
        pool, remaining = sum([portions[i] for i in candidates]), spare
        for i in candidates:
            more = min(bound - holding[i], max(1, remaining * portions[i] // pool), spare)
            holding[i] = holding[i] + more
            spare = spare - more
    return np.array(holding)


def scatter_about(stream_key, dims, deviation, bound, pieces=(), held_as=jnp.bfloat16):
    gain = level_of(stream_key, dims, pieces, -0.22, 0.18) if pieces else 1.0
    drawn = jax.random.normal(stream_key, dims, jnp.float32) * deviation * gain
    return jnp.minimum(jnp.maximum(drawn, -bound), bound).astype(held_as)


def setup_inputs(seed: int = 0) -> dict:
    seeds = jax.random.split(jax.random.key(seed), 11)
    bag_lengths = set_ends(jax.random.randint(seeds[0], (TABLES, TOKENS), 1, BAG + 1), jax.random.fold_in(seeds[0], 1), 1, BAG).astype(jnp.int32)
    owners_keys = jax.random.split(jax.random.fold_in(seeds[1], 1), TABLES * TOKENS * BAG // (TOK_DEV * BAG))
    owners_turns = jax.random.permutation(jax.random.fold_in(seeds[1], 3), TABLES * TOKENS * BAG // (TOK_DEV * BAG))
    owners = jax.vmap(lambda own, number: deal_out(jax.random.fold_in(seeds[1], 2), own, number, TOK_DEV * BAG, N_DP, 1, CAP, 2))(owners_keys, owners_turns).reshape((TABLES, TOKENS, BAG, 1))
    row_slots = set_ends(skewed_ids(seeds[2], (TABLES, TOKENS, BAG), ROWS_DEV, 2), jax.random.fold_in(seeds[2], 3), 0, ROWS_DEV - 1).astype(jnp.int32)
    admit_mask = set_ends((jax.random.randint(seeds[3], (TABLES, TOKENS, BAG), 0, 4) < 3).astype(jnp.int32), jax.random.fold_in(seeds[3], 1), 0, 1)
    expired = set_ends((jax.random.randint(seeds[4], (TABLES, ROWS), 0, 8) < 1).astype(jnp.int32), jax.random.fold_in(seeds[4], 1), 0, 1)
    embeddings = scatter_about(seeds[5], (TABLES, ROWS, EMB), 0.5, 3.0, ((0, 4), (1, 128)), jnp.float32)
    accumulator = jnp.clip(jnp.exp(math.log(0.01) - 2.30258502 * jax.random.uniform(seeds[6], (TABLES, ROWS), jnp.float32) ** level_of(seeds[6], (TABLES, ROWS), ((0, 4), (1, 128)), -0.2, 0.2)), 0.001, 0.01)
    hidden_weight = scatter_about(seeds[7], (TABLES * EMB, HIDDEN_SIZE), (TABLES * EMB) ** -0.5, 0.125, ((1, 4),))
    output_weight = scatter_about(seeds[8], (HIDDEN_SIZE,), 0.15, 0.9, ((0, 4),), jnp.float32)
    labels = set_ends((jax.random.randint(seeds[9], (TOKENS,), 0, 2) < 1).astype(jnp.int32), jax.random.fold_in(seeds[9], 1), 0, 1)
    return {"bag_lengths": bag_lengths, "owners": owners, "row_slots": row_slots, "admit_mask": admit_mask, "expired": expired, "embeddings": embeddings, "accumulator": accumulator, "hidden_weight": hidden_weight, "output_weight": output_weight, "labels": labels}


LEARN_RATE = 0.05
ACC_RESET = 0.001

def silu_slope(preact):
    sig = jax.nn.sigmoid(preact)
    return sig * (1.0 + preact * (1.0 - sig))

def reference(bag_lengths, owners, row_slots, admit_mask, expired, embeddings, accumulator, hidden_weight, output_weight, labels):
    places = jnp.arange(BAG, dtype=jnp.int32)
    live_mask = ((places[None, None, :] < bag_lengths[:, :, None]) & (admit_mask == 1)).astype(jnp.float32)
    counted = lax.optimization_barrier(jnp.sum(live_mask, axis=2))
    bag_weight = live_mask / jnp.maximum(counted, 1.0)[:, :, None]
    global_rows = (owners[..., 0] * ROWS_DEV + row_slots).astype(jnp.int32)
    fresh_rows = jnp.where(expired[:, :, None] == 1, jnp.float32(0.0), embeddings)
    fresh_acc = jnp.where(expired == 1, jnp.float32(ACC_RESET), accumulator)

    def pool_table(inputs):
        table_rows, table_weight, table_index = inputs
        values = jnp.take(table_rows.astype(jnp.bfloat16), table_index, axis=0)
        return lax.optimization_barrier(jnp.sum(table_weight[:, :, None] * values.astype(jnp.float32), axis=1))
    pooled = lax.map(pool_table, (fresh_rows, bag_weight, global_rows))
    features = pooled.transpose(1, 0, 2).reshape(TOKENS, TABLES * EMB).astype(jnp.bfloat16)
    preact = jnp.dot(features, hidden_weight, preferred_element_type=jnp.float32)
    hidden = jax.nn.silu(preact).astype(jnp.bfloat16)
    logits = lax.optimization_barrier(jnp.sum(hidden.astype(jnp.float32) * output_weight, axis=1))
    dlogit = jax.nn.sigmoid(logits) - labels.astype(jnp.float32)
    dhidden = (dlogit[:, None] * output_weight * silu_slope(preact)).astype(jnp.bfloat16)
    weight_grad = lax.dot_general(features, dhidden, (((0,), (0,)), ((), ())), preferred_element_type=jnp.float32).astype(jnp.bfloat16)
    feature_grad = jnp.dot(dhidden, hidden_weight.T, preferred_element_type=jnp.float32)
    feature_grad = feature_grad.reshape(TOKENS, TABLES, EMB).transpose(1, 0, 2)

    def update_table(inputs):
        table_rows, table_acc, table_weight, table_index, table_grad = inputs
        lookup_grads = (table_weight[:, :, None] * table_grad[:, None, :]).astype(jnp.bfloat16)
        summed = jax.ops.segment_sum(lookup_grads.astype(jnp.float32).reshape(-1, EMB), table_index.reshape(-1), num_segments=ROWS)
        new_acc = table_acc + lax.optimization_barrier(jnp.mean(summed * summed, axis=1))
        new_rows = table_rows - LEARN_RATE * summed / jnp.sqrt(new_acc)[:, None]
        return (new_rows, new_acc)
    new_table, new_accum = lax.map(update_table, (fresh_rows, fresh_acc, bag_weight, global_rows, feature_grad))
    return (new_table, new_accum, weight_grad, logits)
```

```python
import jax
import jax.numpy as jnp
from jax import lax
from jax.experimental import pallas as pl
from jax.experimental.pallas import tpu as pltpu
from jax.sharding import Mesh
from jax.sharding import PartitionSpec as P

DP = ("dp_0", "dp_1", "dp_2")
FAR = ("dp_0", "dp_1")
NEAR = "dp_2"

LEARN_RATE = 0.05
ACC_RESET = 0.001
F32, BF16, I32 = jnp.float32, jnp.bfloat16, jnp.int32
NT = (((1,), (1,)), ((), ()))


def iota(shape, dim):
    return lax.broadcasted_iota(I32, shape, dim)


def dot(a, b, dims=(((1,), (0,)), ((), ()))):
    return lax.dot_general(a, b, dims, preferred_element_type=F32)


def flag(cond):
    return jnp.where(cond, 1.0, 0.0).astype(BF16)


def slots_kernel(len_ref, own_ref, slot_ref, adm_ref, req_ref, sample_ref, inv_ref):
    tabs, bag, toks = own_ref.shape
    groups, width = req_ref.shape
    cap = width // tabs
    row_o, lane = iota((groups, toks), 0), iota((groups, toks), 1)
    tri = jnp.concatenate(
        [flag(row_o < lane), jnp.ones((groups, toks), BF16)], axis=1
    )
    rank_row = iota((cap, toks), 0).astype(F32)
    sample_no = (iota((1, toks), 1) + 1).astype(F32)
    for t in range(tabs):
        hot = [row_o == own_ref[t, p : p + 1, :] for p in range(bag)]
        hot16 = [flag(h) for h in hot]
        counts = dot(jnp.concatenate(hot16, axis=0), tri)
        base = jnp.zeros((groups, toks), F32)
        live_count = jnp.zeros((1, toks), F32)
        values = []
        for p in range(bag):
            part = counts[p * groups : (p + 1) * groups]
            rank = jnp.sum(
                jnp.where(hot[p], part[:, :toks] + base, 0.0), axis=0, keepdims=True
            )
            base = base + part[:, toks:]
            live = (p < len_ref[t : t + 1, :]) & (adm_ref[t, p : p + 1, :] == 1)
            live_count = live_count + jnp.where(live, 1.0, 0.0)
            slot = slot_ref[t, p : p + 1, :]
            here = rank_row == rank
            values.append(
                jnp.concatenate(
                    [
                        jnp.where(here, (slot >> 4).astype(F32), 0.0),
                        jnp.where(here, (slot & 15).astype(F32), 0.0),
                        jnp.where(here & live, sample_no, 0.0),
                    ],
                    axis=0,
                ).astype(BF16)
            )
        found = dot(
            jnp.concatenate(hot16, axis=1), jnp.concatenate(values, axis=1), NT
        )
        cols = slice(t * cap, (t + 1) * cap)
        req_ref[:, cols] = (16.0 * found[:, :cap] + found[:, cap : 2 * cap]).astype(I32)
        sample_ref[:, cols] = found[:, 2 * cap :]
        inv = 1.0 / jnp.maximum(live_count, 1.0)
        column = jnp.sum(
            jnp.where(iota((toks, toks), 0) == iota((toks, toks), 1), inv, 0.0),
            axis=1,
            keepdims=True,
        )
        inv_ref[t] = jnp.broadcast_to(column, (toks, toks))


def spread_rows(length, groups, cap, start):
    return flag((iota((length, groups), 0) + start) // cap == iota((length, groups), 1))


def samples_kernel(sample_ref, pick_ref, row_ref):
    tabs, slots, toks = pick_ref.shape
    groups, width = sample_ref.shape
    cap = width // tabs
    spread = spread_rows(slots, groups, cap, 0)
    every = dot(spread, sample_ref[...].astype(BF16))
    place = iota((slots, width), 0) % cap
    lane = iota((slots, width), 1)
    wanted = (iota((slots, toks), 1) + 1).astype(F32)
    for t in range(tabs):
        own = jnp.where(lane == place + t * cap, every, 0.0).astype(BF16)
        pick_ref[t] = flag(dot(own, jnp.ones((width, toks), BF16)) == wanted)
        row_ref[t] = dot(jnp.ones((8, width), BF16), own, NT)


def labels_kernel(label_ref, out_ref):
    dims = out_ref.shape
    row = label_ref[...].astype(F32)
    column = jnp.sum(
        jnp.where(iota(dims, 0) == iota(dims, 1), row, 0.0), axis=1, keepdims=True
    )
    out_ref[...] = jnp.broadcast_to(column, dims)


def halves_of(arrived):
    return jnp.concatenate(
        [(arrived >> 4).astype(F32), (arrived & 15).astype(F32)], axis=1
    ).astype(BF16)


def fetch_kernel(arrived_ref, expired_ref, emb_ref, out_ref):
    groups, width = arrived_ref.shape
    rows, emb = emb_ref.shape[1:]
    cap = out_ref.shape[1]
    t = pl.program_id(0)
    halves = halves_of(arrived_ref[...])
    table = emb_ref[0].astype(BF16)
    scale = jnp.where(iota((2 * width, emb), 0) < width, 16.0, 1.0).astype(BF16)
    gone = expired_ref[pl.ds(t, 1), :]
    names = jnp.where(gone == 1, -1.0, iota((1, rows), 1).astype(F32))
    part = 32
    for c in range(groups // part):
        length = part * cap
        spread = spread_rows(length, groups, cap, c * length)
        every = dot(spread, halves)
        lane = iota((length, 2 * width), 1) & (width - 1)
        own = jnp.where(
            lane == iota((length, 2 * width), 0) % cap + t * cap, every, 0.0
        ).astype(BF16)
        wanted = dot(own, scale)
        pick = jnp.concatenate(
            [flag(wanted == names[:, j : j + emb]) for j in range(0, rows, emb)], axis=1
        )
        out_ref[c * part : (c + 1) * part] = (
            dot(pick, table).astype(BF16).reshape(part, cap, emb)
        )


def wanted_kernel(arrived_ref, row_ref):
    groups, width = arrived_ref.shape
    tabs, eight, slots = row_ref.shape
    cap = width // tabs
    every = dot(spread_rows(slots, groups, cap, 0), halves_of(arrived_ref[...]))
    place = iota((slots, 2 * width), 0) % cap
    lane = iota((slots, 2 * width), 1) & (width - 1)
    scale = jnp.where(iota((eight, 2 * width), 1) < width, 16.0, 1.0).astype(BF16)
    for t in range(tabs):
        own = jnp.where(lane == place + t * cap, every, 0.0).astype(BF16)
        row_ref[t] = dot(scale, own, NT)


def pool_kernel(rows_ref, sample_ref, inv_ref, out_ref):
    groups, cap, emb = rows_ref.shape
    toks = inv_ref.shape[1]
    slots = groups * cap
    wanted = (iota((toks, slots), 0) + 1).astype(F32)
    pick = flag(sample_ref[0, 0:1, :] == wanted)
    pooled = dot(pick, rows_ref[...].reshape(slots, emb))
    out_ref[...] = (pooled * inv_ref[0]).astype(BF16)


def silu_slope(preact):
    sig = jax.nn.sigmoid(preact)
    return sig * (1.0 + preact * (1.0 - sig))


def dense_kernel(
    at_ref, feat_ref, w0, w1, w2, w3, u0, u1, u2, u3, labels_ref,
    logits_ref, grad_ref, mine_ref, other_ref,
):
    parts, toks, feats = feat_ref.shape
    weights, units = (w0, w1, w2, w3), (u0, u1, u2, u3)
    me, core = at_ref[0], at_ref[1]
    preacts, scores = [], []
    for w, u in zip(weights, units):
        pre = sum(
            dot(feat_ref[q], w[q * feats : (q + 1) * feats, :]) for q in range(parts)
        )
        hidden = jax.nn.silu(pre).astype(BF16).astype(F32)
        preacts.append(pre)
        scores.append(jnp.sum(hidden * u[...], axis=1, keepdims=True))
    logits = jnp.zeros((toks, 1), F32)
    for shard in range(parts):
        far = (me + parts - shard) % parts
        score = scores[0]
        for k in range(1, parts):
            score = jnp.where(far == k, scores[k], score)
        logits = logits + score
    dlogit = (jax.nn.sigmoid(logits) - labels_ref[...])[:, 0:1]
    logits_ref[...] = jnp.broadcast_to(logits, logits_ref.shape)
    start = pl.multiple_of(me * feats, feats)
    grads = jnp.zeros((toks, feats), F32)
    for k, (w, u, pre) in enumerate(zip(weights, units, preacts)):
        dhidden = (dlogit * u[...] * silu_slope(pre)).astype(BF16)
        if k == 0:
            half = dhidden.shape[1] // 2
            low, high = dhidden[:, :half], dhidden[:, half:]
            mine, other = jnp.where(core == 0, low, high), jnp.where(core == 0, high, low)
            for q in range(parts):
                lines = slice(q * feats, (q + 1) * feats)
                part = dot(
                    feat_ref[q],
                    jnp.concatenate([mine, other], axis=1),
                    (((0,), (0,)), ((), ())),
                ).astype(BF16)
                mine_ref[lines, :] = part[:, :half]
                other_ref[lines, :] = part[:, half:]
        grads = grads + dot(dhidden, w[pl.ds(start, feats), :], NT)
    grad_ref[...] = grads


def spread_kernel(grad_ref, inv_ref, pick_ref, out_ref):
    slots = pick_ref.shape[1]
    cap, emb = out_ref.shape[1:]
    grad = (inv_ref[0] * grad_ref[...]).astype(BF16)
    out_ref[...] = dot(pick_ref[0], grad).astype(BF16).reshape(slots // cap, cap, emb)


def update_kernel(grads_ref, wanted_ref, emb_ref, expired_ref, acc_ref, new_ref, new_acc_ref):
    groups, cap, emb = grads_ref.shape
    rows = emb_ref.shape[1]
    slots = groups * cap
    t = pl.program_id(0)
    grads = grads_ref[...].reshape(slots, emb)
    wanted = wanted_ref[0, 0:1, :]
    gone = expired_ref[pl.ds(t, 1), :]
    fresh_acc = jnp.where(gone == 1, ACC_RESET, acc_ref[pl.ds(t, 1), :])
    kept = jnp.where(gone == 1, 0.0, 1.0)
    diag = iota((emb, emb), 0) == iota((emb, emb), 1)
    for j in range(0, rows, emb):
        names = (iota((emb, slots), 0) + j).astype(F32)
        summed = dot(flag(wanted == names), grads)
        cols = slice(j, j + emb)
        old = jnp.sum(jnp.where(diag, fresh_acc[:, cols], 0.0), axis=1, keepdims=True)
        keep = jnp.sum(jnp.where(diag, kept[:, cols], 0.0), axis=1, keepdims=True)
        acc = old + jnp.sum(summed * summed, axis=1, keepdims=True) * (1.0 / emb)
        fresh = jnp.where(keep > 0.5, emb_ref[0, j : j + emb, :], 0.0)
        new_ref[0, j : j + emb, :] = fresh - LEARN_RATE * summed / jnp.sqrt(acc)
        line = jnp.sum(jnp.where(diag, acc, 0.0), axis=0, keepdims=True)
        for table in range(acc_ref.shape[0]):

            @pl.when(t == table)
            def _(table=table, cols=cols, line=line):
                new_acc_ref[table : table + 1, cols] = line


def shape(dims, dtype):
    return jax.ShapeDtypeStruct(dims, dtype)


def block(dims, index=None):
    if index is None:
        return pl.BlockSpec(dims, lambda *_: (0,) * len(dims))
    return pl.BlockSpec(dims, index)


def params(mib):
    return pltpu.CompilerParams(vmem_limit_bytes=mib << 20)


def cost(flops):
    return pl.CostEstimate(flops=flops, bytes_accessed=1 << 20, transcendentals=0)


def a2a(value, axis):
    return lax.all_to_all(value, axis, split_axis=0, concat_axis=0, tiled=True)


def from_everyone(value, axis):
    size = lax.axis_size(axis)
    return a2a(jnp.broadcast_to(value[None], (size, *value.shape)), axis)


def ring(value, axis, step):
    size = lax.axis_size(axis)
    return lax.ppermute(value, axis, [(i, (i + step) % size) for i in range(size)])


def shards(
    bag_lengths, owners, row_slots, admit_mask, expired, embeddings, accumulator,
    hidden_weight, output_weight, labels,
):
    groups = lax.axis_size(DP)
    parts = lax.axis_size("mp")
    tabs, toks, bag = row_slots.shape
    rows, emb = embeddings.shape[1:]
    cap = 2 * toks * bag // groups
    width = tabs * cap
    slots = groups * cap
    feats = tabs * emb
    core = lax.axis_index(NEAR).astype(I32)
    place = jnp.stack([lax.axis_index("mp").astype(I32), core])

    request, sample, inv = pl.pallas_call(
        slots_kernel,
        out_shape=(
            shape((groups, width), I32),
            shape((groups, width), F32),
            shape((tabs, toks, toks), F32),
        ),
        compiler_params=params(24),
        name="slots",
    )(
        bag_lengths,
        owners[..., 0].swapaxes(1, 2),
        row_slots.swapaxes(1, 2),
        admit_mask.swapaxes(1, 2),
    )
    arrived = a2a(request, DP)
    weight, _ = lax.optimization_barrier((hidden_weight, request))
    weights = [weight] + [ring(weight, "mp", k) for k in range(1, parts)]
    pick, sample_row = pl.pallas_call(
        samples_kernel,
        out_shape=(shape((tabs, slots, toks), BF16), shape((tabs, 8, slots), F32)),
        compiler_params=params(24),
        cost_estimate=cost(4 << 30),
        name="samples",
    )(sample)
    fetched = pl.pallas_call(
        fetch_kernel,
        grid=(tabs,),
        in_specs=[
            block((groups, width)),
            block((tabs, rows)),
            block((1, rows, emb), lambda t: (t, 0, 0)),
        ],
        out_specs=block((groups, cap, emb), lambda t: (0, t, 0)),
        out_shape=pltpu.HBM((groups, width, emb), BF16),
        compiler_params=params(24),
        name="fetch",
    )(arrived, expired, embeddings)
    returned = a2a(fetched, DP)
    unit, later = lax.optimization_barrier((output_weight, arrived))
    unit = unit.reshape(1, -1)
    units = [unit] + [ring(unit, "mp", k) for k in range(1, parts)]
    wanted = pl.pallas_call(
        wanted_kernel,
        out_shape=shape((tabs, 8, slots), F32),
        compiler_params=params(24),
        cost_estimate=cost(4 << 30),
        name="wanted",
    )(later)
    features = pl.pallas_call(
        pool_kernel,
        grid=(tabs,),
        in_specs=[
            block((groups, cap, emb), lambda t: (0, t, 0)),
            block((1, 8, slots), lambda t: (t, 0, 0)),
            block((1, toks, toks), lambda t: (t, 0, 0)),
        ],
        out_specs=block((toks, emb), lambda t: (0, t)),
        out_shape=shape((toks, feats), BF16),
        compiler_params=params(24),
        name="pool",
    )(returned, sample_row, inv)
    portion = from_everyone(features, "mp")
    label_column = pl.pallas_call(
        labels_kernel,
        out_shape=shape((toks, toks), F32),
        compiler_params=params(4),
        name="labels",
    )(labels.reshape(1, toks))
    units_dev = hidden_weight.shape[1]
    lines, half = hidden_weight.shape[0], units_dev // 2
    logits, grad, mine, other = pl.pallas_call(
        dense_kernel,
        in_specs=[pl.BlockSpec(memory_space=pltpu.SMEM)]
        + [pl.BlockSpec(memory_space=pltpu.VMEM)] * (2 * parts + 2),
        out_shape=(
            shape((toks, toks), F32),
            shape((toks, feats), F32),
            shape((lines, half), BF16),
            shape((lines, half), BF16),
        ),
        compiler_params=params(24),
        name="dense",
    )(place, portion, *weights, *units, label_column)
    joined = ring(other, NEAR, 1)
    share = lines // groups
    outgoing = pl.pallas_call(
        spread_kernel,
        grid=(tabs,),
        in_specs=[
            block((toks, emb), lambda t: (0, t)),
            block((1, toks, toks), lambda t: (t, 0, 0)),
            block((1, slots, toks), lambda t: (t, 0, 0)),
        ],
        out_specs=block((groups, cap, emb), lambda t: (0, t, 0)),
        out_shape=shape((groups, width + share, emb), BF16),
        compiler_params=params(24),
        cost_estimate=cost(4 << 30),
        name="spread",
    )(grad, inv, pick)
    pair = (mine.astype(F32) + joined.astype(F32)).astype(BF16)
    pair = pair.reshape(2, groups // 2, share, half).swapaxes(0, 1)
    outgoing = lax.dynamic_update_slice(
        outgoing, pair.reshape(groups, share, half), (0, width, 0)
    )
    gradients = a2a(outgoing, DP)
    shares = gradients[:, width:].reshape(groups // 2, 2, 2, share // 2, half)
    own = shares.astype(F32).sum(axis=0).astype(BF16).swapaxes(0, 1)
    near = from_everyone(own, FAR)
    near = near.transpose(0, 1, 3, 2, 4).reshape(lines // 2, units_dev)
    far = ring(near, NEAR, 1)
    weight_grad = jnp.concatenate(
        [jnp.where(core == 0, near, far), jnp.where(core == 0, far, near)]
    )
    new_rows, new_acc = pl.pallas_call(
        update_kernel,
        grid=(tabs,),
        in_specs=[
            block((groups, cap, emb), lambda t: (0, t, 0)),
            block((1, 8, slots), lambda t: (t, 0, 0)),
            block((1, rows, emb), lambda t: (t, 0, 0)),
            block((tabs, rows)),
            block((tabs, rows)),
        ],
        out_specs=(
            block((1, rows, emb), lambda t: (t, 0, 0)),
            block((tabs, rows)),
        ),
        out_shape=(shape(embeddings.shape, F32), shape(accumulator.shape, F32)),
        compiler_params=params(24),
        cost_estimate=cost(4 << 30),
        name="update",
    )(gradients, wanted, embeddings, expired, accumulator)
    return (new_rows, new_acc, weight_grad, logits[:, 0])


def solution(mesh):
    split = Mesh(mesh.devices.reshape(8, 8, 2, mesh.shape["mp"]), (*DP, "mp"))

    return jax.shard_map(
        shards,
        mesh=split,
        in_specs=(
            P("mp", DP),
            P("mp", DP, None, None),
            P("mp", DP, None),
            P("mp", DP, None),
            P("mp", DP),
            P("mp", DP, None),
            P("mp", DP),
            P(None, "mp"),
            P("mp"),
            P(DP),
        ),
        out_specs=(P("mp", DP, None), P("mp", DP), P(None, "mp"), P(DP)),
        check_vma=False,
    )
```

```python
import functools

import jax
import jax.numpy as jnp
from jax import lax
from jax.experimental import pallas as pl
from jax.experimental.pallas import tpu as pltpu
from jax.sharding import Mesh
from jax.sharding import PartitionSpec as P

DP = ("dp_0", "dp_1", "dp_2")
FAR = ("dp_0", "dp_1")
NEAR = "dp_2"

LEARN_RATE = 0.05
ACC_RESET = 0.001
F32, BF16, I32 = jnp.float32, jnp.bfloat16, jnp.int32
NT = (((1,), (1,)), ((), ()))


def iota(shape, dim):
    return lax.broadcasted_iota(I32, shape, dim)


def dot(a, b, dims=(((1,), (0,)), ((), ()))):
    return lax.dot_general(a, b, dims, preferred_element_type=F32)


def flag(cond):
    return jnp.where(cond, 1.0, 0.0).astype(BF16)


def slots_kernel(len_ref, own_ref, slot_ref, adm_ref, req_ref, sample_ref, inv_ref):
    tabs, bag, toks = own_ref.shape
    groups, width = req_ref.shape
    cap = width // tabs
    row_o, lane = iota((groups, toks), 0), iota((groups, toks), 1)
    tri = jnp.concatenate(
        [flag(row_o < lane), jnp.ones((groups, toks), BF16)], axis=1
    )
    rank_row = iota((cap, toks), 0).astype(F32)
    sample_no = (iota((1, toks), 1) + 1).astype(F32)
    for t in range(tabs):
        hot = [row_o == own_ref[t, p : p + 1, :] for p in range(bag)]
        hot16 = [flag(h) for h in hot]
        counts = dot(jnp.concatenate(hot16, axis=0), tri)
        base = jnp.zeros((groups, toks), F32)
        live_count = jnp.zeros((1, toks), F32)
        values = []
        for p in range(bag):
            part = counts[p * groups : (p + 1) * groups]
            rank = jnp.sum(
                jnp.where(hot[p], part[:, :toks] + base, 0.0), axis=0, keepdims=True
            )
            base = base + part[:, toks:]
            live = (p < len_ref[t : t + 1, :]) & (adm_ref[t, p : p + 1, :] == 1)
            live_count = live_count + jnp.where(live, 1.0, 0.0)
            slot = slot_ref[t, p : p + 1, :]
            here = rank_row == rank
            values.append(
                jnp.concatenate(
                    [
                        jnp.where(here, (slot >> 4).astype(F32), 0.0),
                        jnp.where(here, (slot & 15).astype(F32), 0.0),
                        jnp.where(here & live, sample_no, 0.0),
                    ],
                    axis=0,
                ).astype(BF16)
            )
        found = dot(
            jnp.concatenate(hot16, axis=1), jnp.concatenate(values, axis=1), NT
        )
        cols = slice(t * cap, (t + 1) * cap)
        req_ref[:, cols] = (16.0 * found[:, :cap] + found[:, cap : 2 * cap]).astype(I32)
        sample_ref[:, cols] = found[:, 2 * cap :]
        inv = 1.0 / jnp.maximum(live_count, 1.0)
        column = jnp.sum(
            jnp.where(iota((toks, toks), 0) == iota((toks, toks), 1), inv, 0.0),
            axis=1,
            keepdims=True,
        )
        inv_ref[t] = jnp.broadcast_to(column, (toks, toks))


def spread_rows(length, groups, cap):
    return flag(iota((length, groups), 0) // cap == iota((length, groups), 1))


def own_lines(table, slots):
    groups, lanes = table.shape
    cap = slots // groups
    every = dot(spread_rows(slots, groups, cap), table)
    rank = iota((slots, lanes), 0) % cap
    return jnp.where(iota((slots, lanes), 1) % cap == rank, every, 0.0).astype(BF16)


def of_table(shape, lane_dim, t, kind, width, cap):
    lane = iota(shape, lane_dim)
    return flag((lane // width == kind) & (lane % width // cap == t))


def samples_kernel(sample_ref, pick_ref, row_ref):
    tabs, slots, toks = pick_ref.shape
    width = sample_ref.shape[1]
    cap = width // tabs
    own = own_lines(sample_ref[...].astype(BF16), slots)
    wanted = (iota((slots, toks), 1) + 1).astype(F32)
    for t in range(tabs):
        mine = of_table((width, toks), 0, t, 0, width, cap)
        pick_ref[t] = flag(dot(own, mine) == wanted)
        row_ref[t] = dot(of_table((8, width), 1, t, 0, width, cap), own, NT)


def labels_kernel(label_ref, out_ref):
    dims = out_ref.shape
    row = label_ref[...].astype(F32)
    column = jnp.sum(
        jnp.where(iota(dims, 0) == iota(dims, 1), row, 0.0), axis=1, keepdims=True
    )
    out_ref[...] = jnp.broadcast_to(column, dims)


def rows_kernel(expired_ref, emb_ref, out_ref):
    tabs, rows, emb = emb_ref.shape
    diag = iota((emb, emb), 0) == iota((emb, emb), 1)
    for t in range(tabs):
        for j in range(0, rows, emb):
            gone = expired_ref[t : t + 1, j : j + emb].astype(F32)
            column = jnp.sum(jnp.where(diag, gone, 0.0), axis=1, keepdims=True)
            out_ref[t, j : j + emb, :] = jnp.where(
                column > 0.5, 0.0, emb_ref[t, j : j + emb, :]
            ).astype(BF16)


def halves_of(arrived):
    return jnp.concatenate(
        [(arrived >> 7).astype(F32), (arrived & 127).astype(F32)], axis=1
    ).astype(BF16)


def fetch_kernel(arrived_ref, rows_ref, out_ref, own_ref):
    groups, width = arrived_ref.shape
    rows, emb = rows_ref.shape[1:]
    cap = out_ref.shape[1]
    slots = groups * cap
    t = pl.program_id(0)

    @pl.when(t == 0)
    def _():
        own_ref[...] = own_lines(halves_of(arrived_ref[...]), slots)

    lanes = (2 * width, emb)
    which = jnp.concatenate(
        [of_table(lanes, 0, t, 1, width, cap), of_table(lanes, 0, t, 0, width, cap)],
        axis=1,
    )
    part = slots // 4
    lane = iota((16, emb), 1).astype(F32).astype(BF16)
    lane = jnp.concatenate([lane] * (part // 16), axis=0)
    one, zero = jnp.ones((part, emb), BF16), jnp.zeros((part, emb), BF16)
    for c in range(0, slots, part):
        found = dot(own_ref[c : c + part, :], which)
        hot = jnp.where(found[:, :emb].astype(BF16) == lane, one, zero)
        at = found[:, emb:].astype(BF16)
        pick = jnp.concatenate(
            [jnp.where(at == jnp.full_like(at, j), hot, zero) for j in range(rows // emb)],
            axis=1,
        )
        out_ref[c // cap : (c + part) // cap] = (
            dot(pick, rows_ref[0]).astype(BF16).reshape(part // cap, cap, emb)
        )


def wanted_kernel(arrived_ref, row_ref):
    width = arrived_ref.shape[1]
    tabs, _, slots = row_ref.shape
    cap = width // tabs
    own = own_lines(halves_of(arrived_ref[...]), slots)
    for t in range(tabs):
        for kind in range(2):
            row_ref[t, 8 * kind : 8 * kind + 8, :] = dot(
                of_table((8, 2 * width), 1, t, kind, width, cap), own, NT
            )


def sublanes(length, wide):
    column = iota((length, 128), 0).astype(F32).astype(BF16)
    return jnp.concatenate([column] * (wide // 128), axis=1)


def down(row, length):
    return jnp.concatenate([row] * (length // 8), axis=0).astype(BF16)


def pool_kernel(rows_ref, sample_ref, inv_ref, out_ref):
    groups, cap, emb = rows_ref.shape
    toks = inv_ref.shape[1]
    slots = groups * cap
    row = down(sample_ref[0] - 1.0, 16)
    row = jnp.concatenate([row] * (toks // 16), axis=0)
    one, zero = jnp.ones((toks, slots), BF16), jnp.zeros((toks, slots), BF16)
    pick = jnp.where(row == sublanes(toks, slots), one, zero)
    pooled = dot(pick, rows_ref[...].reshape(slots, emb))
    feature = (pooled * inv_ref[0]).astype(BF16)
    for k in range(out_ref.shape[0]):
        out_ref[k] = feature


def silu_slope(preact):
    sig = jax.nn.sigmoid(preact)
    return sig * (1.0 + preact * (1.0 - sig))


def dense_kernel(
    at_ref, feat_ref, w0, w1, w2, w3, u0, u1, u2, u3, labels_ref,
    logits_ref, dhidden_ref, mine_ref, other_ref, held_ref, sem_ref,
):
    parts, toks, feats = feat_ref.shape
    weights, units = (w0, w1, w2, w3), (u0, u1, u2, u3)
    copies = [
        pltpu.make_async_copy(w, held_ref.at[k], sem_ref.at[k])
        for k, w in enumerate(weights)
    ]
    for copy in copies:
        copy.start()
    me, core = at_ref[0], at_ref[1]
    preacts, scores = [], []
    for k, u in enumerate(units):
        copies[k].wait()
        pre = sum(
            dot(feat_ref[q], held_ref[k, q * feats : (q + 1) * feats, :])
            for q in range(parts)
        )
        hidden = jax.nn.silu(pre).astype(BF16).astype(F32)
        preacts.append(pre)
        scores.append(jnp.sum(hidden * u[...], axis=1, keepdims=True))
    logits = jnp.zeros((toks, 1), F32)
    for shard in range(parts):
        far = (me + parts - shard) % parts
        score = scores[0]
        for k in range(1, parts):
            score = jnp.where(far == k, scores[k], score)
        logits = logits + score
    dlogit = (jax.nn.sigmoid(logits) - labels_ref[...])[:, 0:1]
    logits_ref[...] = jnp.broadcast_to(logits, logits_ref.shape)
    for k, (u, pre) in enumerate(zip(units, preacts)):
        dhidden = (dlogit * u[...] * silu_slope(pre)).astype(BF16)
        dhidden_ref[k] = dhidden
        if k == 0:
            half = dhidden.shape[1] // 2
            low, high = dhidden[:, :half], dhidden[:, half:]
            mine, other = jnp.where(core == 0, low, high), jnp.where(core == 0, high, low)
            both = jnp.concatenate([mine, other], axis=1)
            for q in range(parts):
                lines = slice(q * feats, (q + 1) * feats)
                part = dot(feat_ref[q], both, (((0,), (0,)), ((), ()))).astype(BF16)
                mine_ref[lines, :] = part[:, :half]
                other_ref[lines, :] = part[:, half:]


def spread_kernel(
    at_ref, dhidden_ref, w0, w1, w2, w3, inv_ref, pick_ref, out_ref,
    held_ref, grad_ref, sem_ref,
):
    parts, feats, _ = held_ref.shape
    slots = pick_ref.shape[1]
    cap, emb = out_ref.shape[1:]
    t = pl.program_id(0)

    @pl.when(t == 0)
    def _():
        start = pl.multiple_of(at_ref[0] * feats, feats)
        copies = [
            pltpu.make_async_copy(w.at[pl.ds(start, feats)], held_ref.at[k], sem_ref.at[k])
            for k, w in enumerate((w0, w1, w2, w3))
        ]
        for copy in copies:
            copy.start()
        for copy in copies:
            copy.wait()
        grads = sum(dot(dhidden_ref[k], held_ref[k], NT) for k in range(parts))
        for j in range(feats // emb):
            grad_ref[j] = grads[:, j * emb : (j + 1) * emb]

    grad = (inv_ref[0] * grad_ref[t]).astype(BF16)
    out_ref[...] = dot(pick_ref[0], grad).astype(BF16).reshape(slots // cap, cap, emb)


def update_kernel(grads_ref, wanted_ref, emb_ref, expired_ref, acc_ref, new_ref, new_acc_ref):
    groups, cap, emb = grads_ref.shape
    rows = emb_ref.shape[1]
    slots = groups * cap
    t = pl.program_id(0)
    grads = grads_ref[...].reshape(slots, emb)
    at = down(wanted_ref[0, 0:8, :], 16)
    low = down(wanted_ref[0, 8:16, :], 16)
    low = jnp.concatenate([low] * (emb // 16), axis=0)
    one, zero = jnp.ones((emb, slots), BF16), jnp.zeros((emb, slots), BF16)
    hot = jnp.where(low == sublanes(emb, slots), one, zero)
    gone = expired_ref[pl.ds(t, 1), :]
    fresh_acc = jnp.where(gone == 1, ACC_RESET, acc_ref[pl.ds(t, 1), :])
    kept = jnp.where(gone == 1, 0.0, 1.0)
    diag = iota((emb, emb), 0) == iota((emb, emb), 1)
    for j in range(0, rows, emb):
        here = jnp.concatenate([at == jnp.full_like(at, j // emb)] * (emb // 16), axis=0)
        summed = dot(jnp.where(here, hot, zero), grads)
        cols = slice(j, j + emb)
        old = jnp.sum(jnp.where(diag, fresh_acc[:, cols], 0.0), axis=1, keepdims=True)
        keep = jnp.sum(jnp.where(diag, kept[:, cols], 0.0), axis=1, keepdims=True)
        acc = old + jnp.sum(summed * summed, axis=1, keepdims=True) * (1.0 / emb)
        fresh = jnp.where(keep > 0.5, emb_ref[0, j : j + emb, :], 0.0)
        new_ref[0, j : j + emb, :] = fresh - LEARN_RATE * summed / jnp.sqrt(acc)
        line = jnp.sum(jnp.where(diag, acc, 0.0), axis=0, keepdims=True)
        for table in range(acc_ref.shape[0]):

            @pl.when(t == table)
            def _(table=table, cols=cols, line=line):
                new_acc_ref[table : table + 1, cols] = line


def join_kernel(at_ref, near_ref, far_ref, out_ref):
    far, two, lines, half = near_ref.shape
    first = at_ref[1] == 0
    for c in range(2):
        for side in range(two):
            near, other = near_ref[:, side], far_ref[:, side]
            part = jnp.where(first, near, other) if c == 0 else jnp.where(first, other, near)
            out_ref[c * far * lines : (c + 1) * far * lines, side * half : (side + 1) * half] = (
                part.reshape(far * lines, half)
            )


def shape(dims, dtype):
    return jax.ShapeDtypeStruct(dims, dtype)


def block(dims, index=None):
    if index is None:
        return pl.BlockSpec(dims, lambda *_: (0,) * len(dims))
    return pl.BlockSpec(dims, index)


def params(mib):
    return pltpu.CompilerParams(vmem_limit_bytes=mib << 20)


def cost(flops):
    return pl.CostEstimate(flops=flops, bytes_accessed=1 << 20, transcendentals=0)


def a2a(value, axis):
    return lax.all_to_all(value, axis, split_axis=0, concat_axis=0, tiled=True)


def ring(value, axis, step):
    size = lax.axis_size(axis)
    return lax.ppermute(value, axis, [(i, (i + step) % size) for i in range(size)])


def shards(
    bag_lengths, owners, row_slots, admit_mask, expired, embeddings, accumulator,
    hidden_weight, output_weight, labels,
):
    groups = lax.axis_size(DP)
    parts = lax.axis_size("mp")
    tabs, toks, bag = row_slots.shape
    rows, emb = embeddings.shape[1:]
    cap = 2 * toks * bag // groups
    width = tabs * cap
    slots = groups * cap
    feats = tabs * emb
    core = lax.axis_index(NEAR).astype(I32)
    place = jnp.stack([lax.axis_index("mp").astype(I32), core])

    request, sample, inv = pl.pallas_call(
        slots_kernel,
        out_shape=(
            shape((groups, width), I32),
            shape((groups, width), F32),
            shape((tabs, toks, toks), F32),
        ),
        compiler_params=params(24),
        name="slots",
    )(
        *map(
            functools.partial(pltpu.with_memory_space_constraint, memory_space=pltpu.HBM),
            (
                bag_lengths,
                owners[..., 0].swapaxes(1, 2),
                row_slots.swapaxes(1, 2),
                admit_mask.swapaxes(1, 2),
            ),
        )
    )
    arrived = a2a(request, DP)
    weight, _ = lax.optimization_barrier((hidden_weight, request))
    weights = [weight] + [ring(weight, "mp", k) for k in range(1, parts)]
    pick, sample_row = pl.pallas_call(
        samples_kernel,
        out_shape=(
            pltpu.HBM((tabs, slots, toks), BF16),
            pltpu.HBM((tabs, 8, slots), F32),
        ),
        compiler_params=params(24),
        cost_estimate=cost(4 << 30),
        name="samples",
    )(sample)
    held = functools.partial(pltpu.with_memory_space_constraint, memory_space=pltpu.HBM)
    sent = pl.pallas_call(
        rows_kernel,
        out_shape=pltpu.HBM((tabs, rows, emb), BF16),
        compiler_params=params(8),
        cost_estimate=cost(1 << 30),
        name="rows",
    )(expired, held(embeddings))
    fetched = pl.pallas_call(
        fetch_kernel,
        grid=(tabs,),
        in_specs=[
            block((groups, width)),
            block((1, rows, emb), lambda t: (t, 0, 0)),
        ],
        out_specs=block((groups, cap, emb), lambda t: (0, t, 0)),
        out_shape=pltpu.HBM((groups, width, emb), BF16),
        scratch_shapes=[pltpu.VMEM((slots, 2 * width), BF16)],
        compiler_params=params(24),
        name="fetch",
    )(arrived, held(sent))
    returned = a2a(fetched, DP)
    unit, later = lax.optimization_barrier((output_weight, arrived))
    unit = unit.reshape(1, -1)
    units = [unit] + [ring(unit, "mp", k) for k in range(1, parts)]
    wanted = pl.pallas_call(
        wanted_kernel,
        out_shape=pltpu.HBM((tabs, 16, slots), F32),
        compiler_params=params(24),
        cost_estimate=cost(4 << 30),
        name="wanted",
    )(later)
    features = pl.pallas_call(
        pool_kernel,
        grid=(tabs,),
        in_specs=[
            block((groups, cap, emb), lambda t: (0, t, 0)),
            block((1, 8, slots), lambda t: (t, 0, 0)),
            block((1, toks, toks), lambda t: (t, 0, 0)),
        ],
        out_specs=block((parts, toks, emb), lambda t: (0, 0, t)),
        out_shape=pltpu.HBM((parts, toks, feats), BF16),
        compiler_params=params(24),
        name="pool",
    )(returned, held(sample_row), inv)
    portion = a2a(features, "mp")
    label_column = pl.pallas_call(
        labels_kernel,
        out_shape=shape((toks, toks), F32),
        compiler_params=params(4),
        name="labels",
    )(labels.reshape(1, toks))
    units_dev = hidden_weight.shape[1]
    lines, half = hidden_weight.shape[0], units_dev // 2
    smem, vmem, hbm = (
        pl.BlockSpec(memory_space=space) for space in (pltpu.SMEM, pltpu.VMEM, pltpu.HBM)
    )
    logits, dhidden, mine, other = pl.pallas_call(
        dense_kernel,
        in_specs=[smem, vmem] + [hbm] * parts + [vmem] * (parts + 1),
        out_shape=(
            shape((toks, toks), F32),
            shape((parts, toks, units_dev), BF16),
            shape((lines, half), BF16),
            shape((lines, half), BF16),
        ),
        scratch_shapes=[
            pltpu.VMEM((parts, lines, units_dev), BF16),
            pltpu.SemaphoreType.DMA((parts,)),
        ],
        compiler_params=params(24),
        name="dense",
    )(place, portion, *map(held, weights), *units, label_column)
    joined = ring(other, NEAR, 1)
    share = lines // groups
    outgoing = pl.pallas_call(
        spread_kernel,
        grid=(tabs,),
        in_specs=[
            smem,
            block((parts, toks, units_dev)),
            *[hbm] * parts,
            block((1, toks, toks), lambda t: (t, 0, 0)),
            block((1, slots, toks), lambda t: (t, 0, 0)),
        ],
        out_specs=block((groups, cap, emb), lambda t: (0, t, 0)),
        out_shape=shape((groups, width + share, emb), BF16),
        scratch_shapes=[
            pltpu.VMEM((parts, feats, units_dev), BF16),
            pltpu.VMEM((tabs, toks, emb), F32),
            pltpu.SemaphoreType.DMA((parts,)),
        ],
        compiler_params=params(24),
        cost_estimate=cost(4 << 30),
        name="spread",
    )(place, dhidden, *map(held, weights), inv, held(pick))
    pair = (mine.astype(F32) + joined.astype(F32)).astype(BF16)
    pair = pair.reshape(2, groups // 2, share, half).swapaxes(0, 1)
    shares = a2a(pair, FAR)
    own = shares.astype(F32).sum(axis=0).astype(BF16)
    own = jnp.broadcast_to(own[None], (groups // 2, *own.shape))
    outgoing = lax.dynamic_update_slice(
        outgoing, own.reshape(groups, share, half), (0, width, 0)
    )
    gradients = a2a(outgoing, DP)
    near = gradients[:, width:].reshape(groups // 2, 2, share, half)
    far = ring(near, NEAR, 1)
    weight_grad = pl.pallas_call(
        join_kernel,
        in_specs=[smem, vmem, vmem],
        out_shape=shape((lines, units_dev), BF16),
        compiler_params=params(8),
        name="join",
    )(place, near, far)
    new_rows, new_acc = pl.pallas_call(
        update_kernel,
        grid=(tabs,),
        in_specs=[
            block((groups, cap, emb), lambda t: (0, t, 0)),
            block((1, 16, slots), lambda t: (t, 0, 0)),
            block((1, rows, emb), lambda t: (t, 0, 0)),
            block((tabs, rows)),
            block((tabs, rows)),
        ],
        out_specs=(
            block((1, rows, emb), lambda t: (t, 0, 0)),
            block((tabs, rows)),
        ),
        out_shape=(shape(embeddings.shape, F32), shape(accumulator.shape, F32)),
        compiler_params=params(24),
        cost_estimate=cost(4 << 30),
        name="update",
    )(gradients, held(wanted), held(embeddings), expired, accumulator)
    return (new_rows, new_acc, weight_grad, logits[:, 0])


def solution(mesh):
    split = Mesh(mesh.devices.reshape(8, 8, 2, mesh.shape["mp"]), (*DP, "mp"))

    return jax.shard_map(
        shards,
        mesh=split,
        in_specs=(
            P("mp", DP),
            P("mp", DP, None, None),
            P("mp", DP, None),
            P("mp", DP, None),
            P("mp", DP),
            P("mp", DP, None),
            P("mp", DP),
            P(None, "mp"),
            P("mp"),
            P(DP),
        ),
        out_specs=(P("mp", DP, None), P("mp", DP), P(None, "mp"), P(DP)),
        check_vma=False,
    )
```

```python
import functools

import jax
import jax.numpy as jnp
from jax import lax
from jax.experimental import pallas as pl
from jax.experimental.pallas import tpu as pltpu
from jax.sharding import Mesh
from jax.sharding import PartitionSpec as P

DP = ("dp_0", "dp_1", "dp_2")
FAR = ("dp_0", "dp_1")
NEAR = "dp_2"

LEARN_RATE = 0.05
ACC_RESET = 0.001
F32, BF16, I32 = jnp.float32, jnp.bfloat16, jnp.int32
NT = (((1,), (1,)), ((), ()))


def iota(shape, dim):
    return lax.broadcasted_iota(I32, shape, dim)


def dot(a, b, dims=(((1,), (0,)), ((), ()))):
    return lax.dot_general(a, b, dims, preferred_element_type=F32)


def flag(cond):
    return jnp.where(cond, 1.0, 0.0).astype(BF16)


def slots_kernel(len_ref, own_ref, slot_ref, adm_ref, req_ref, sample_ref, inv_ref):
    tabs, bag, toks = own_ref.shape
    groups, width = req_ref.shape
    cap = width // tabs
    row_o, lane = iota((groups, toks), 0), iota((groups, toks), 1)
    tri = jnp.concatenate(
        [flag(row_o < lane), jnp.ones((groups, toks), BF16)], axis=1
    )
    rank_row = iota((cap, toks), 0).astype(F32)
    sample_no = (iota((1, toks), 1) + 1).astype(F32)
    for t in range(tabs):
        hot = [row_o == own_ref[t, p : p + 1, :] for p in range(bag)]
        hot16 = [flag(h) for h in hot]
        counts = dot(jnp.concatenate(hot16, axis=0), tri)
        base = jnp.zeros((groups, toks), F32)
        live_count = jnp.zeros((1, toks), F32)
        values = []
        for p in range(bag):
            part = counts[p * groups : (p + 1) * groups]
            rank = jnp.sum(
                jnp.where(hot[p], part[:, :toks] + base, 0.0), axis=0, keepdims=True
            )
            base = base + part[:, toks:]
            live = (p < len_ref[t : t + 1, :]) & (adm_ref[t, p : p + 1, :] == 1)
            live_count = live_count + jnp.where(live, 1.0, 0.0)
            slot = slot_ref[t, p : p + 1, :]
            here = rank_row == rank
            values.append(
                jnp.concatenate(
                    [
                        jnp.where(here, (slot >> 4).astype(F32), 0.0),
                        jnp.where(here, (slot & 15).astype(F32), 0.0),
                        jnp.where(here & live, sample_no, 0.0),
                    ],
                    axis=0,
                ).astype(BF16)
            )
        found = dot(
            jnp.concatenate(hot16, axis=1), jnp.concatenate(values, axis=1), NT
        )
        cols = slice(t * cap, (t + 1) * cap)
        req_ref[:, cols] = (16.0 * found[:, :cap] + found[:, cap : 2 * cap]).astype(I32)
        sample_ref[:, cols] = found[:, 2 * cap :]
        inv = 1.0 / jnp.maximum(live_count, 1.0)
        column = jnp.sum(
            jnp.where(iota((toks, toks), 0) == iota((toks, toks), 1), inv, 0.0),
            axis=1,
            keepdims=True,
        )
        inv_ref[t] = jnp.broadcast_to(column, (toks, toks))


def own_lines(table, slots):
    groups, lanes = table.shape
    cap = slots // groups
    mine = iota((cap, lanes), 1) % cap == iota((cap, lanes), 0)
    return jnp.concatenate(
        [
            jnp.where(mine, jnp.broadcast_to(table[o : o + 1], (cap, lanes)), 0.0)
            for o in range(groups)
        ],
        axis=0,
    ).astype(BF16)


def of_table(shape, lane_dim, t, kind, width, cap):
    lane = iota(shape, lane_dim)
    return flag((lane // width == kind) & (lane % width // cap == t))


def samples_kernel(sample_ref, pick_ref, row_ref):
    tabs, slots, toks = pick_ref.shape
    width = sample_ref.shape[1]
    cap = width // tabs
    own = own_lines(sample_ref[...], slots)
    wanted = (iota((slots, toks), 1) + 1).astype(F32)
    for t in range(tabs):
        mine = of_table((width, toks), 0, t, 0, width, cap)
        pick_ref[t] = flag(dot(own, mine) == wanted)
        row = dot(of_table((8, width), 1, t, 0, width, cap), own, NT)
        row_ref[t : t + 1, :] = row[0:1]


def labels_kernel(label_ref, out_ref):
    dims = out_ref.shape
    row = label_ref[...].astype(F32)
    column = jnp.sum(
        jnp.where(iota(dims, 0) == iota(dims, 1), row, 0.0), axis=1, keepdims=True
    )
    out_ref[...] = jnp.broadcast_to(column, dims)


def rows_kernel(expired_ref, emb_ref, out_ref):
    tabs, rows, emb = emb_ref.shape
    diag = iota((emb, emb), 0) == iota((emb, emb), 1)
    for t in range(tabs):
        for j in range(0, rows, emb):
            gone = expired_ref[t : t + 1, j : j + emb].astype(F32)
            column = jnp.sum(jnp.where(diag, gone, 0.0), axis=1, keepdims=True)
            out_ref[t, j : j + emb, :] = jnp.where(
                column > 0.5, 0.0, emb_ref[t, j : j + emb, :]
            ).astype(BF16)


def halves_of(arrived, block_rows):
    shift = block_rows.bit_length() - 1
    return jnp.concatenate(
        [(arrived >> shift).astype(F32), (arrived & (block_rows - 1)).astype(F32)], axis=1
    )


def fetch_kernel(arrived_ref, rows_ref, out_ref, table_ref, own_ref, sent_ref, in_sem, out_sem):
    groups, width = arrived_ref.shape
    tabs, rows, emb = rows_ref.shape
    cap = width // tabs
    slots = groups * cap
    half = rows // 2
    load = pltpu.make_async_copy(rows_ref, table_ref, in_sem)
    load.start()
    own_ref[...] = own_lines(halves_of(arrived_ref[...], half), slots)
    lane = iota((16, emb), 1).astype(F32)
    parts = out_sem.shape[0]
    part = slots // parts
    low = jnp.concatenate([lane.astype(BF16)] * (part // 16), axis=0)
    high = jnp.concatenate([(lane + emb).astype(BF16)] * (part // 16), axis=0)
    one, zero = jnp.ones((part, emb), BF16), jnp.zeros((part, emb), BF16)
    lanes = (2 * width, emb)
    stores = []
    for c in range(parts):
        own = own_ref[c * part : (c + 1) * part, :]
        mine = slice(c * part // cap, (c + 1) * part // cap)
        for t in range(tabs):
            which = jnp.concatenate(
                [of_table(lanes, 0, t, 1, width, cap), of_table(lanes, 0, t, 0, width, cap)],
                axis=1,
            )
            found = dot(own, which)
            at = found[:, :emb].astype(BF16)
            pick = jnp.concatenate(
                [jnp.where(at == low, one, zero), jnp.where(at == high, one, zero)], axis=1
            )
            if c == 0 and t == 0:
                load.wait()
            table = jnp.concatenate([table_ref[t, :half], table_ref[t, half:]], axis=1)
            both = dot(pick, table).astype(BF16)
            line = jnp.where(found[:, emb:].astype(BF16) == zero, both[:, :emb], both[:, emb:])
            sent_ref[mine, t * cap : (t + 1) * cap, :] = line.reshape(part // cap, cap, emb)
        store = pltpu.make_async_copy(sent_ref.at[mine], out_ref.at[mine], out_sem.at[c])
        store.start()
        stores.append(store)
    for store in stores:
        store.wait()


def wanted_kernel(arrived_ref, row_ref):
    width = arrived_ref.shape[1]
    tabs, _, slots = row_ref.shape
    cap = width // tabs
    own = own_lines(halves_of(arrived_ref[...], 128), slots)
    for t in range(tabs):
        for kind in range(2):
            row_ref[t, 8 * kind : 8 * kind + 8, :] = dot(
                of_table((8, 2 * width), 1, t, kind, width, cap), own, NT
            )


def sublanes(length, wide):
    column = iota((length, 128), 0).astype(F32).astype(BF16)
    return jnp.concatenate([column] * (wide // 128), axis=1)


def down(row, length):
    return jnp.concatenate([row] * (length // 8), axis=0).astype(BF16)


def pool_kernel(rows_ref, sample_ref, inv_ref, out_ref, feature_ref, sem_ref):
    groups, width, emb = rows_ref.shape
    tabs, toks, _ = inv_ref.shape
    cap = width // tabs
    slots = groups * cap
    one, zero = jnp.ones((toks, slots), BF16), jnp.zeros((toks, slots), BF16)
    samples = sublanes(toks, slots)
    copies = []
    for t in range(tabs):
        row = jnp.broadcast_to(sample_ref[t : t + 1, :] - 1.0, (16, slots)).astype(BF16)
        pick = jnp.where(jnp.concatenate([row] * (toks // 16), axis=0) == samples, one, zero)
        pooled = dot(pick, rows_ref[:, t * cap : (t + 1) * cap, :].reshape(slots, emb))
        cols = slice(t * emb, (t + 1) * emb)
        feature_ref[:, cols] = (pooled * inv_ref[t]).astype(BF16)
        for k in range(out_ref.shape[0]):
            copy = pltpu.make_async_copy(
                feature_ref.at[:, cols], out_ref.at[k, :, cols], sem_ref.at[t, k]
            )
            copy.start()
            copies.append(copy)
    for copy in copies:
        copy.wait()


def silu_slope(preact):
    sig = jax.nn.sigmoid(preact)
    return sig * (1.0 + preact * (1.0 - sig))


def dense_kernel(
    at_ref, feat_ref, w0, w1, w2, w3, u0, u1, u2, u3, labels_ref,
    logits_ref, grad_ref, mine_ref, other_ref,
):
    parts, toks, feats = feat_ref.shape
    weights, units = (w0, w1, w2, w3), (u0, u1, u2, u3)
    me, core = at_ref[0], at_ref[1]
    preacts, scores = [], []
    for w, u in zip(weights, units):
        pre = sum(
            dot(feat_ref[q], w[q * feats : (q + 1) * feats, :]) for q in range(parts)
        )
        hidden = jax.nn.silu(pre).astype(BF16).astype(F32)
        preacts.append(pre)
        scores.append(jnp.sum(hidden * u[...], axis=1, keepdims=True))
    logits = jnp.zeros((toks, 1), F32)
    for shard in range(parts):
        far = (me + parts - shard) % parts
        score = scores[0]
        for k in range(1, parts):
            score = jnp.where(far == k, scores[k], score)
        logits = logits + score
    dlogit = (jax.nn.sigmoid(logits) - labels_ref[...])[:, 0:1]
    logits_ref[...] = jnp.broadcast_to(logits, logits_ref.shape)
    start = pl.multiple_of(me * feats, feats)
    grads = jnp.zeros((toks, feats), F32)
    for k, (w, u, pre) in enumerate(zip(weights, units, preacts)):
        dhidden = (dlogit * u[...] * silu_slope(pre)).astype(BF16)
        if k == 0:
            half = dhidden.shape[1] // 2
            low, high = dhidden[:, :half], dhidden[:, half:]
            mine, other = jnp.where(core == 0, low, high), jnp.where(core == 0, high, low)
            for q in range(parts):
                lines = slice(q * feats, (q + 1) * feats)
                part = dot(
                    feat_ref[q],
                    jnp.concatenate([mine, other], axis=1),
                    (((0,), (0,)), ((), ())),
                ).astype(BF16)
                mine_ref[lines, :] = part[:, :half]
                other_ref[lines, :] = part[:, half:]
        grads = grads + dot(dhidden, w[pl.ds(start, feats), :], NT)
    grad_ref[...] = grads


def spread_kernel(grad_ref, inv_ref, pick_ref, out_ref):
    slots = pick_ref.shape[1]
    cap, emb = out_ref.shape[1:]
    grad = (inv_ref[0] * grad_ref[...]).astype(BF16)
    out_ref[...] = dot(pick_ref[0], grad).astype(BF16).reshape(slots // cap, cap, emb)


def update_kernel(grads_ref, wanted_ref, emb_ref, expired_ref, acc_ref, new_ref, new_acc_ref):
    groups, cap, emb = grads_ref.shape
    rows = emb_ref.shape[1]
    slots = groups * cap
    t = pl.program_id(0)
    grads = grads_ref[...].reshape(slots, emb)
    at = down(wanted_ref[0, 0:8, :], 16)
    low = down(wanted_ref[0, 8:16, :], 16)
    low = jnp.concatenate([low] * (emb // 16), axis=0)
    one, zero = jnp.ones((emb, slots), BF16), jnp.zeros((emb, slots), BF16)
    hot = jnp.where(low == sublanes(emb, slots), one, zero)
    gone = expired_ref[pl.ds(t, 1), :]
    fresh_acc = jnp.where(gone == 1, ACC_RESET, acc_ref[pl.ds(t, 1), :])
    kept = jnp.where(gone == 1, 0.0, 1.0)
    diag = iota((emb, emb), 0) == iota((emb, emb), 1)
    for j in range(0, rows, emb):
        here = jnp.concatenate([at == jnp.full_like(at, j // emb)] * (emb // 16), axis=0)
        summed = dot(jnp.where(here, hot, zero), grads)
        cols = slice(j, j + emb)
        old = jnp.sum(jnp.where(diag, fresh_acc[:, cols], 0.0), axis=1, keepdims=True)
        keep = jnp.sum(jnp.where(diag, kept[:, cols], 0.0), axis=1, keepdims=True)
        acc = old + jnp.sum(summed * summed, axis=1, keepdims=True) * (1.0 / emb)
        fresh = jnp.where(keep > 0.5, emb_ref[0, j : j + emb, :], 0.0)
        new_ref[0, j : j + emb, :] = fresh - LEARN_RATE * summed / jnp.sqrt(acc)
        line = jnp.sum(jnp.where(diag, acc, 0.0), axis=0, keepdims=True)
        for table in range(acc_ref.shape[0]):

            @pl.when(t == table)
            def _(table=table, cols=cols, line=line):
                new_acc_ref[table : table + 1, cols] = line


def shape(dims, dtype):
    return jax.ShapeDtypeStruct(dims, dtype)


def block(dims, index=None):
    if index is None:
        return pl.BlockSpec(dims, lambda *_: (0,) * len(dims))
    return pl.BlockSpec(dims, index)


def params(mib):
    return pltpu.CompilerParams(vmem_limit_bytes=mib << 20)


def cost(flops):
    return pl.CostEstimate(flops=flops, bytes_accessed=1 << 20, transcendentals=0)


def a2a(value, axis):
    return lax.all_to_all(value, axis, split_axis=0, concat_axis=0, tiled=True)


def from_everyone(value, axis):
    size = lax.axis_size(axis)
    return a2a(jnp.broadcast_to(value[None], (size, *value.shape)), axis)


def ring(value, axis, step):
    size = lax.axis_size(axis)
    return lax.ppermute(value, axis, [(i, (i + step) % size) for i in range(size)])


def shards(
    bag_lengths, owners, row_slots, admit_mask, expired, embeddings, accumulator,
    hidden_weight, output_weight, labels,
):
    groups = lax.axis_size(DP)
    parts = lax.axis_size("mp")
    tabs, toks, bag = row_slots.shape
    rows, emb = embeddings.shape[1:]
    cap = 2 * toks * bag // groups
    width = tabs * cap
    slots = groups * cap
    feats = tabs * emb
    core = lax.axis_index(NEAR).astype(I32)
    place = jnp.stack([lax.axis_index("mp").astype(I32), core])

    request, sample, inv = pl.pallas_call(
        slots_kernel,
        out_shape=(
            shape((groups, width), I32),
            shape((groups, width), F32),
            shape((tabs, toks, toks), F32),
        ),
        compiler_params=params(24),
        name="slots",
    )(
        *map(
            functools.partial(pltpu.with_memory_space_constraint, memory_space=pltpu.HBM),
            (
                bag_lengths,
                owners[..., 0].swapaxes(1, 2),
                row_slots.swapaxes(1, 2),
                admit_mask.swapaxes(1, 2),
            ),
        )
    )
    arrived = a2a(request, DP)
    weight, _ = lax.optimization_barrier((hidden_weight, request))
    weights = [weight] + [ring(weight, "mp", k) for k in range(1, parts)]
    pick, sample_row = pl.pallas_call(
        samples_kernel,
        out_shape=(
            pltpu.HBM((tabs, slots, toks), BF16),
            shape((tabs, slots), F32),
        ),
        compiler_params=params(24),
        cost_estimate=cost(4 << 30),
        name="samples",
    )(sample)
    held = functools.partial(pltpu.with_memory_space_constraint, memory_space=pltpu.HBM)
    sent = pl.pallas_call(
        rows_kernel,
        out_shape=pltpu.HBM((tabs, rows, emb), BF16),
        compiler_params=params(8),
        cost_estimate=cost(1 << 30),
        name="rows",
    )(expired, held(embeddings))
    _, vmem, hbm = (
        pl.BlockSpec(memory_space=space) for space in (pltpu.SMEM, pltpu.VMEM, pltpu.HBM)
    )
    dma = pltpu.SemaphoreType.DMA
    fetched = pl.pallas_call(
        fetch_kernel,
        in_specs=[vmem, hbm],
        out_specs=hbm,
        out_shape=pltpu.HBM((groups, width, emb), BF16),
        scratch_shapes=[
            pltpu.VMEM((tabs, rows, emb), BF16),
            pltpu.VMEM((slots, 2 * width), BF16),
            pltpu.VMEM((groups, width, emb), BF16),
            dma,
            dma((4,)),
        ],
        compiler_params=params(24),
        name="fetch",
    )(arrived, held(sent))
    returned = a2a(fetched, DP)
    unit, later = lax.optimization_barrier((output_weight, arrived))
    unit = unit.reshape(1, -1)
    units = [unit] + [ring(unit, "mp", k) for k in range(1, parts)]
    wanted = pl.pallas_call(
        wanted_kernel,
        out_shape=pltpu.HBM((tabs, 16, slots), F32),
        compiler_params=params(24),
        cost_estimate=cost(4 << 30),
        name="wanted",
    )(later)
    features = pl.pallas_call(
        pool_kernel,
        in_specs=[vmem, vmem, vmem],
        out_specs=hbm,
        out_shape=pltpu.HBM((parts, toks, feats), BF16),
        scratch_shapes=[pltpu.VMEM((toks, feats), BF16), dma((tabs, parts))],
        compiler_params=params(24),
        name="pool",
    )(returned, sample_row, inv)
    portion = a2a(features, "mp")
    label_column = pl.pallas_call(
        labels_kernel,
        out_shape=shape((toks, toks), F32),
        compiler_params=params(4),
        name="labels",
    )(labels.reshape(1, toks))
    units_dev = hidden_weight.shape[1]
    lines, half = hidden_weight.shape[0], units_dev // 2
    logits, grad, mine, other = pl.pallas_call(
        dense_kernel,
        in_specs=[pl.BlockSpec(memory_space=pltpu.SMEM)]
        + [pl.BlockSpec(memory_space=pltpu.VMEM)] * (2 * parts + 2),
        out_shape=(
            shape((toks, toks), F32),
            shape((toks, feats), F32),
            shape((lines, half), BF16),
            shape((lines, half), BF16),
        ),
        compiler_params=params(24),
        name="dense",
    )(place, portion, *weights, *units, label_column)
    joined = ring(other, NEAR, 1)
    share = lines // groups
    outgoing = pl.pallas_call(
        spread_kernel,
        grid=(tabs,),
        in_specs=[
            block((toks, emb), lambda t: (0, t)),
            block((1, toks, toks), lambda t: (t, 0, 0)),
            block((1, slots, toks), lambda t: (t, 0, 0)),
        ],
        out_specs=block((groups, cap, emb), lambda t: (0, t, 0)),
        out_shape=shape((groups, width + share, emb), BF16),
        compiler_params=params(24),
        cost_estimate=cost(4 << 30),
        name="spread",
    )(grad, inv, pick)
    pair = (mine.astype(F32) + joined.astype(F32)).astype(BF16)
    pair = pair.reshape(2, groups // 2, share, half).swapaxes(0, 1)
    outgoing = lax.dynamic_update_slice(
        outgoing, pair.reshape(groups, share, half), (0, width, 0)
    )
    gradients = a2a(outgoing, DP)
    shares = gradients[:, width:].reshape(groups // 2, 2, 2, share // 2, half)
    own = shares.astype(F32).sum(axis=0).astype(BF16).swapaxes(0, 1)
    near = from_everyone(own, FAR)
    near = near.transpose(0, 1, 3, 2, 4).reshape(lines // 2, units_dev)
    far = ring(near, NEAR, 1)
    weight_grad = jnp.concatenate(
        [jnp.where(core == 0, near, far), jnp.where(core == 0, far, near)]
    )
    new_rows, new_acc = pl.pallas_call(
        update_kernel,
        grid=(tabs,),
        in_specs=[
            block((groups, cap, emb), lambda t: (0, t, 0)),
            block((1, 16, slots), lambda t: (t, 0, 0)),
            block((1, rows, emb), lambda t: (t, 0, 0)),
            block((tabs, rows)),
            block((tabs, rows)),
        ],
        out_specs=(
            block((1, rows, emb), lambda t: (t, 0, 0)),
            block((tabs, rows)),
        ),
        out_shape=(shape(embeddings.shape, F32), shape(accumulator.shape, F32)),
        compiler_params=params(24),
        cost_estimate=cost(4 << 30),
        name="update",
    )(gradients, held(wanted), held(embeddings), expired, accumulator)
    return (new_rows, new_acc, weight_grad, logits[:, 0])


def solution(mesh):
    split = Mesh(mesh.devices.reshape(8, 8, 2, mesh.shape["mp"]), (*DP, "mp"))

    return jax.shard_map(
        shards,
        mesh=split,
        in_specs=(
            P("mp", DP),
            P("mp", DP, None, None),
            P("mp", DP, None),
            P("mp", DP, None),
            P("mp", DP),
            P("mp", DP, None),
            P("mp", DP),
            P(None, "mp"),
            P("mp"),
            P(DP),
        ),
        out_specs=(P("mp", DP, None), P("mp", DP), P(None, "mp"), P(DP)),
        check_vma=False,
    )
```

```python
import functools

import jax
import jax.numpy as jnp
from jax import lax
from jax.experimental import pallas as pl
from jax.experimental.pallas import tpu as pltpu
from jax.sharding import Mesh
from jax.sharding import PartitionSpec as P

DP = ("dp_0", "dp_1", "dp_2")
FAR = ("dp_0", "dp_1")
NEAR = "dp_2"

LEARN_RATE = 0.05
ACC_RESET = 0.001
F32, BF16, I32 = jnp.float32, jnp.bfloat16, jnp.int32
NT = (((1,), (1,)), ((), ()))


def iota(shape, dim):
    return lax.broadcasted_iota(I32, shape, dim)


def dot(a, b, dims=(((1,), (0,)), ((), ()))):
    return lax.dot_general(a, b, dims, preferred_element_type=F32)


def flag(cond):
    return jnp.where(cond, 1.0, 0.0).astype(BF16)


def slots_kernel(len_ref, own_ref, slot_ref, adm_ref, req_ref, sample_ref, inv_ref):
    tabs, bag, toks = own_ref.shape
    groups, width = req_ref.shape
    cap = width // tabs
    row_o, lane = iota((groups, toks), 0), iota((groups, toks), 1)
    tri = jnp.concatenate(
        [flag(row_o < lane), jnp.ones((groups, toks), BF16)], axis=1
    )
    rank_row = iota((cap, toks), 0).astype(F32)
    sample_no = (iota((1, toks), 1) + 1).astype(F32)
    for t in range(tabs):
        hot = [row_o == own_ref[t, p : p + 1, :] for p in range(bag)]
        hot16 = [flag(h) for h in hot]
        counts = dot(jnp.concatenate(hot16, axis=0), tri)
        base = jnp.zeros((groups, toks), F32)
        live_count = jnp.zeros((1, toks), F32)
        values = []
        for p in range(bag):
            part = counts[p * groups : (p + 1) * groups]
            rank = jnp.sum(
                jnp.where(hot[p], part[:, :toks] + base, 0.0), axis=0, keepdims=True
            )
            base = base + part[:, toks:]
            live = (p < len_ref[t : t + 1, :]) & (adm_ref[t, p : p + 1, :] == 1)
            live_count = live_count + jnp.where(live, 1.0, 0.0)
            slot = slot_ref[t, p : p + 1, :]
            here = rank_row == rank
            values.append(
                jnp.concatenate(
                    [
                        jnp.where(here, (slot >> 4).astype(F32), 0.0),
                        jnp.where(here, (slot & 15).astype(F32), 0.0),
                        jnp.where(here & live, sample_no, 0.0),
                    ],
                    axis=0,
                ).astype(BF16)
            )
        found = dot(
            jnp.concatenate(hot16, axis=1), jnp.concatenate(values, axis=1), NT
        )
        cols = slice(t * cap, (t + 1) * cap)
        req_ref[:, cols] = (16.0 * found[:, :cap] + found[:, cap : 2 * cap]).astype(I32)
        sample_ref[:, cols] = found[:, 2 * cap :]
        inv = 1.0 / jnp.maximum(live_count, 1.0)
        column = jnp.sum(
            jnp.where(iota((toks, toks), 0) == iota((toks, toks), 1), inv, 0.0),
            axis=1,
            keepdims=True,
        )
        inv_ref[t] = jnp.broadcast_to(column, (toks, toks))


def own_lines(table, slots):
    groups, lanes = table.shape
    cap = slots // groups
    mine = iota((cap, lanes), 1) % cap == iota((cap, lanes), 0)
    return jnp.concatenate(
        [
            jnp.where(mine, jnp.broadcast_to(table[o : o + 1], (cap, lanes)), 0.0)
            for o in range(groups)
        ],
        axis=0,
    ).astype(BF16)


def of_table(shape, lane_dim, t, kind, width, cap):
    lane = iota(shape, lane_dim)
    return flag((lane // width == kind) & (lane % width // cap == t))


def samples_kernel(sample_ref, pick_ref, row_ref):
    tabs, slots, toks = pick_ref.shape
    width = sample_ref.shape[1]
    cap = width // tabs
    own = own_lines(sample_ref[...], slots)
    wanted = (iota((slots, toks), 1) + 1).astype(F32)
    for t in range(tabs):
        mine = of_table((width, toks), 0, t, 0, width, cap)
        pick_ref[t] = flag(dot(own, mine) == wanted)
        row = dot(of_table((8, width), 1, t, 0, width, cap), own, NT)
        row_ref[t : t + 1, :] = row[0:1]


def labels_kernel(label_ref, out_ref):
    dims = out_ref.shape
    row = label_ref[...].astype(F32)
    column = jnp.sum(
        jnp.where(iota(dims, 0) == iota(dims, 1), row, 0.0), axis=1, keepdims=True
    )
    out_ref[...] = jnp.broadcast_to(column, dims)


def halves_of(arrived, block_rows):
    shift = block_rows.bit_length() - 1
    return jnp.concatenate(
        [(arrived >> shift).astype(F32), (arrived & (block_rows - 1)).astype(F32)], axis=1
    )


def fetch_kernel(
    arrived_ref, expired_ref, emb_ref, out_ref,
    gone_ref, held_ref, table_ref, sent_ref, in_sem, out_sem,
):
    groups, width = arrived_ref.shape
    tabs, rows, emb = emb_ref.shape
    cap = width // tabs
    half = rows // 2
    loads = [pltpu.make_async_copy(expired_ref, gone_ref, in_sem.at[tabs])] + [
        pltpu.make_async_copy(emb_ref.at[t], held_ref.at[t], in_sem.at[t]) for t in range(tabs)
    ]
    for load in loads:
        load.start()
    halves = halves_of(arrived_ref[...], half)
    lane = iota((16, emb), 1).astype(F32)
    diag = iota((emb, emb), 0) == iota((emb, emb), 1)
    parts = out_sem.shape[0]
    part = groups // parts
    low = jnp.concatenate([lane.astype(BF16)] * (part * cap // 16), axis=0)
    high = jnp.concatenate([(lane + emb).astype(BF16)] * (part * cap // 16), axis=0)
    one, zero = jnp.ones((part * cap, emb), BF16), jnp.zeros((part * cap, emb), BF16)
    lanes = (2 * width, emb)
    which = [
        jnp.concatenate([of_table(lanes, 0, t, kind, width, cap) for kind in (1, 0)], axis=1)
        for t in range(tabs)
    ]
    stores = []
    for c in range(parts):
        mine = slice(c * part, (c + 1) * part)
        own = own_lines(halves[mine], part * cap)
        for t in range(tabs):
            if c == 0:
                if t == 0:
                    loads[0].wait()
                loads[t + 1].wait()
                for j in range(0, rows, emb):
                    gone = gone_ref[t : t + 1, j : j + emb].astype(F32)
                    column = jnp.sum(jnp.where(diag, gone, 0.0), axis=1, keepdims=True)
                    side = j // half * emb
                    table_ref[t, j % half : j % half + emb, side : side + emb] = jnp.where(
                        column > 0.5, 0.0, held_ref[t, j : j + emb, :]
                    ).astype(BF16)
            found = dot(own, which[t])
            at = found[:, :emb].astype(BF16)
            pick = jnp.concatenate(
                [jnp.where(at == low, one, zero), jnp.where(at == high, one, zero)], axis=1
            )
            both = dot(pick, table_ref[t]).astype(BF16)
            line = jnp.where(found[:, emb:].astype(BF16) == zero, both[:, :emb], both[:, emb:])
            sent_ref[mine, t * cap : (t + 1) * cap, :] = line.reshape(part, cap, emb)
        store = pltpu.make_async_copy(sent_ref.at[mine], out_ref.at[mine], out_sem.at[c])
        store.start()
        stores.append(store)
    for store in stores:
        store.wait()


def wanted_kernel(arrived_ref, row_ref):
    width = arrived_ref.shape[1]
    tabs, _, slots = row_ref.shape
    cap = width // tabs
    own = own_lines(halves_of(arrived_ref[...], 128), slots)
    for t in range(tabs):
        for kind in range(2):
            row_ref[t, 8 * kind : 8 * kind + 8, :] = dot(
                of_table((8, 2 * width), 1, t, kind, width, cap), own, NT
            )


def sublanes(length, wide):
    column = iota((length, 128), 0).astype(F32).astype(BF16)
    return jnp.concatenate([column] * (wide // 128), axis=1)


def down(row, length):
    return jnp.concatenate([row] * (length // 8), axis=0).astype(BF16)


def pool_kernel(rows_ref, sample_ref, inv_ref, out_ref, feature_ref, sem_ref):
    groups, width, emb = rows_ref.shape
    tabs, toks, _ = inv_ref.shape
    cap = width // tabs
    slots = groups * cap
    one, zero = jnp.ones((toks, slots), BF16), jnp.zeros((toks, slots), BF16)
    samples = sublanes(toks, slots)
    copies = []
    for t in range(tabs):
        row = jnp.broadcast_to(sample_ref[t : t + 1, :] - 1.0, (16, slots)).astype(BF16)
        pick = jnp.where(jnp.concatenate([row] * (toks // 16), axis=0) == samples, one, zero)
        pooled = dot(pick, rows_ref[:, t * cap : (t + 1) * cap, :].reshape(slots, emb))
        cols = slice(t * emb, (t + 1) * emb)
        feature_ref[:, cols] = (pooled * inv_ref[t]).astype(BF16)
        for k in range(out_ref.shape[0]):
            copy = pltpu.make_async_copy(
                feature_ref.at[:, cols], out_ref.at[k, :, cols], sem_ref.at[t, k]
            )
            copy.start()
            copies.append(copy)
    for copy in copies:
        copy.wait()


def silu_slope(preact):
    sig = jax.nn.sigmoid(preact)
    return sig * (1.0 + preact * (1.0 - sig))


def dense_kernel(
    at_ref, feat_ref, w0, w1, w2, w3, u0, u1, u2, u3, labels_ref,
    logits_ref, grad_ref, mine_ref, other_ref,
):
    parts, toks, feats = feat_ref.shape
    weights, units = (w0, w1, w2, w3), (u0, u1, u2, u3)
    me, core = at_ref[0], at_ref[1]
    preacts, scores = [], []
    for w, u in zip(weights, units):
        pre = sum(
            dot(feat_ref[q], w[q * feats : (q + 1) * feats, :]) for q in range(parts)
        )
        hidden = jax.nn.silu(pre).astype(BF16).astype(F32)
        preacts.append(pre)
        scores.append(jnp.sum(hidden * u[...], axis=1, keepdims=True))
    logits = jnp.zeros((toks, 1), F32)
    for shard in range(parts):
        far = (me + parts - shard) % parts
        score = scores[0]
        for k in range(1, parts):
            score = jnp.where(far == k, scores[k], score)
        logits = logits + score
    dlogit = (jax.nn.sigmoid(logits) - labels_ref[...])[:, 0:1]
    logits_ref[...] = jnp.broadcast_to(logits, logits_ref.shape)
    start = pl.multiple_of(me * feats, feats)
    grads = jnp.zeros((toks, feats), F32)
    for k, (w, u, pre) in enumerate(zip(weights, units, preacts)):
        dhidden = (dlogit * u[...] * silu_slope(pre)).astype(BF16)
        if k == 0:
            half = dhidden.shape[1] // 2
            low, high = dhidden[:, :half], dhidden[:, half:]
            mine, other = jnp.where(core == 0, low, high), jnp.where(core == 0, high, low)
            for q in range(parts):
                lines = slice(q * feats, (q + 1) * feats)
                part = dot(
                    feat_ref[q],
                    jnp.concatenate([mine, other], axis=1),
                    (((0,), (0,)), ((), ())),
                ).astype(BF16)
                mine_ref[lines, :] = part[:, :half]
                other_ref[lines, :] = part[:, half:]
        grads = grads + dot(dhidden, w[pl.ds(start, feats), :], NT)
    grad_ref[...] = grads


def spread_kernel(grad_ref, inv_ref, pick_ref, out_ref):
    slots = pick_ref.shape[1]
    cap, emb = out_ref.shape[1:]
    grad = (inv_ref[0] * grad_ref[...]).astype(BF16)
    out_ref[...] = dot(pick_ref[0], grad).astype(BF16).reshape(slots // cap, cap, emb)


def update_kernel(grads_ref, wanted_ref, emb_ref, expired_ref, acc_ref, new_ref, new_acc_ref):
    groups, cap, emb = grads_ref.shape
    rows = emb_ref.shape[1]
    slots = groups * cap
    t = pl.program_id(0)
    grads = grads_ref[...].reshape(slots, emb)
    at = down(wanted_ref[0, 0:8, :], 16)
    low = down(wanted_ref[0, 8:16, :], 16)
    low = jnp.concatenate([low] * (emb // 16), axis=0)
    one, zero = jnp.ones((emb, slots), BF16), jnp.zeros((emb, slots), BF16)
    hot = jnp.where(low == sublanes(emb, slots), one, zero)
    gone = expired_ref[pl.ds(t, 1), :]
    fresh_acc = jnp.where(gone == 1, ACC_RESET, acc_ref[pl.ds(t, 1), :])
    kept = jnp.where(gone == 1, 0.0, 1.0)
    diag = iota((emb, emb), 0) == iota((emb, emb), 1)
    for j in range(0, rows, emb):
        here = jnp.concatenate([at == jnp.full_like(at, j // emb)] * (emb // 16), axis=0)
        summed = dot(jnp.where(here, hot, zero), grads)
        cols = slice(j, j + emb)
        old = jnp.sum(jnp.where(diag, fresh_acc[:, cols], 0.0), axis=1, keepdims=True)
        keep = jnp.sum(jnp.where(diag, kept[:, cols], 0.0), axis=1, keepdims=True)
        acc = old + jnp.sum(summed * summed, axis=1, keepdims=True) * (1.0 / emb)
        fresh = jnp.where(keep > 0.5, emb_ref[0, j : j + emb, :], 0.0)
        new_ref[0, j : j + emb, :] = fresh - LEARN_RATE * summed / jnp.sqrt(acc)
        line = jnp.sum(jnp.where(diag, acc, 0.0), axis=0, keepdims=True)
        for table in range(acc_ref.shape[0]):

            @pl.when(t == table)
            def _(table=table, cols=cols, line=line):
                new_acc_ref[table : table + 1, cols] = line


def near_kernel(at_ref, piece_ref, out_ref, sem):
    copy = pltpu.make_async_copy(piece_ref, out_ref.at[at_ref[1]], sem)
    copy.start()
    copy.wait()


def far_kernel(at_ref, piece_ref, begun_ref, out_ref, sem):
    copy = pltpu.make_async_copy(piece_ref, out_ref.at[1 - at_ref[1]], sem)
    copy.start()
    copy.wait()


def shape(dims, dtype):
    return jax.ShapeDtypeStruct(dims, dtype)


def block(dims, index=None):
    if index is None:
        return pl.BlockSpec(dims, lambda *_: (0,) * len(dims))
    return pl.BlockSpec(dims, index)


def params(mib):
    return pltpu.CompilerParams(vmem_limit_bytes=mib << 20)


def cost(flops):
    return pl.CostEstimate(flops=flops, bytes_accessed=1 << 20, transcendentals=0)


def a2a(value, axis):
    return lax.all_to_all(value, axis, split_axis=0, concat_axis=0, tiled=True)


def from_everyone(value, axis):
    size = lax.axis_size(axis)
    return a2a(jnp.broadcast_to(value[None], (size, *value.shape)), axis)


def ring(value, axis, step):
    size = lax.axis_size(axis)
    return lax.ppermute(value, axis, [(i, (i + step) % size) for i in range(size)])


def shards(
    bag_lengths, owners, row_slots, admit_mask, expired, embeddings, accumulator,
    hidden_weight, output_weight, labels,
):
    groups = lax.axis_size(DP)
    parts = lax.axis_size("mp")
    tabs, toks, bag = row_slots.shape
    rows, emb = embeddings.shape[1:]
    cap = 2 * toks * bag // groups
    width = tabs * cap
    slots = groups * cap
    feats = tabs * emb
    core = lax.axis_index(NEAR).astype(I32)
    place = jnp.stack([lax.axis_index("mp").astype(I32), core])

    request, sample, inv = pl.pallas_call(
        slots_kernel,
        out_shape=(
            shape((groups, width), I32),
            shape((groups, width), F32),
            shape((tabs, toks, toks), F32),
        ),
        compiler_params=params(24),
        name="slots",
    )(
        *map(
            functools.partial(pltpu.with_memory_space_constraint, memory_space=pltpu.HBM),
            (
                bag_lengths,
                owners[..., 0].swapaxes(1, 2),
                row_slots.swapaxes(1, 2),
                admit_mask.swapaxes(1, 2),
            ),
        )
    )
    arrived = a2a(request, DP)
    weight, _ = lax.optimization_barrier((hidden_weight, request))
    weights = [weight] + [ring(weight, "mp", k) for k in range(1, parts)]
    pick, sample_row = pl.pallas_call(
        samples_kernel,
        out_shape=(
            pltpu.HBM((tabs, slots, toks), BF16),
            shape((tabs, slots), F32),
        ),
        compiler_params=params(24),
        cost_estimate=cost(4 << 30),
        name="samples",
    )(sample)
    held = functools.partial(pltpu.with_memory_space_constraint, memory_space=pltpu.HBM)
    smem, vmem, hbm = (
        pl.BlockSpec(memory_space=space) for space in (pltpu.SMEM, pltpu.VMEM, pltpu.HBM)
    )
    dma = pltpu.SemaphoreType.DMA
    fetched = pl.pallas_call(
        fetch_kernel,
        in_specs=[vmem, hbm, hbm],
        out_specs=hbm,
        out_shape=pltpu.HBM((groups, width, emb), BF16),
        scratch_shapes=[
            pltpu.VMEM((tabs, rows), I32),
            pltpu.VMEM((tabs, rows, emb), F32),
            pltpu.VMEM((tabs, rows // 2, 2 * emb), BF16),
            pltpu.VMEM((groups, width, emb), BF16),
            dma((tabs + 1,)),
            dma((4,)),
        ],
        compiler_params=params(24),
        name="fetch",
    )(arrived, held(expired), held(embeddings))
    returned = a2a(fetched, DP)
    unit, later = lax.optimization_barrier((output_weight, arrived))
    unit = unit.reshape(1, -1)
    units = [unit] + [ring(unit, "mp", k) for k in range(1, parts)]
    wanted = pl.pallas_call(
        wanted_kernel,
        out_shape=pltpu.HBM((tabs, 16, slots), F32),
        compiler_params=params(24),
        cost_estimate=cost(4 << 30),
        name="wanted",
    )(later)
    features = pl.pallas_call(
        pool_kernel,
        in_specs=[vmem, vmem, vmem],
        out_specs=hbm,
        out_shape=pltpu.HBM((parts, toks, feats), BF16),
        scratch_shapes=[pltpu.VMEM((toks, feats), BF16), dma((tabs, parts))],
        compiler_params=params(24),
        name="pool",
    )(returned, sample_row, inv)
    portion = a2a(features, "mp")
    label_column = pl.pallas_call(
        labels_kernel,
        out_shape=shape((toks, toks), F32),
        compiler_params=params(4),
        name="labels",
    )(labels.reshape(1, toks))
    units_dev = hidden_weight.shape[1]
    lines, half = hidden_weight.shape[0], units_dev // 2
    logits, grad, mine, other = pl.pallas_call(
        dense_kernel,
        in_specs=[pl.BlockSpec(memory_space=pltpu.SMEM)]
        + [pl.BlockSpec(memory_space=pltpu.VMEM)] * (2 * parts + 2),
        out_shape=(
            shape((toks, toks), F32),
            shape((toks, feats), F32),
            shape((lines, half), BF16),
            shape((lines, half), BF16),
        ),
        compiler_params=params(24),
        name="dense",
    )(place, portion, *weights, *units, label_column)
    joined = ring(other, NEAR, 1)
    share = lines // groups
    outgoing = pl.pallas_call(
        spread_kernel,
        grid=(tabs,),
        in_specs=[
            block((toks, emb), lambda t: (0, t)),
            block((1, toks, toks), lambda t: (t, 0, 0)),
            block((1, slots, toks), lambda t: (t, 0, 0)),
        ],
        out_specs=block((groups, cap, emb), lambda t: (0, t, 0)),
        out_shape=shape((groups, width + share, emb), BF16),
        compiler_params=params(24),
        cost_estimate=cost(4 << 30),
        name="spread",
    )(grad, inv, pick)
    pair = (mine.astype(F32) + joined.astype(F32)).astype(BF16)
    pair = pair.reshape(2, groups // 2, share, half).swapaxes(0, 1)
    outgoing = lax.dynamic_update_slice(
        outgoing, pair.reshape(groups, share, half), (0, width, 0)
    )
    gradients = a2a(outgoing, DP)
    shares = gradients[:, width:].reshape(groups // 2, 2, 2, share // 2, half)
    own = shares.astype(F32).sum(axis=0).astype(BF16).swapaxes(0, 1)
    near = from_everyone(own, FAR)
    near = near.transpose(0, 1, 3, 2, 4).reshape(lines // 2, units_dev)
    far = ring(near, NEAR, 1)
    weight_grad = None
    for kernel, piece in ((near_kernel, near), (far_kernel, far)):
        begun = [] if weight_grad is None else [weight_grad]
        weight_grad = pl.pallas_call(
            kernel,
            in_specs=[smem, vmem] + [hbm] * len(begun),
            out_specs=hbm,
            out_shape=pltpu.HBM((2, lines // 2, units_dev), BF16),
            input_output_aliases={2: 0} if begun else {},
            scratch_shapes=[dma],
            compiler_params=params(4),
            name="near" if weight_grad is None else "far",
        )(place, piece, *begun)
    weight_grad = weight_grad.reshape(lines, units_dev)
    new_rows, new_acc = pl.pallas_call(
        update_kernel,
        grid=(tabs,),
        in_specs=[
            block((groups, cap, emb), lambda t: (0, t, 0)),
            block((1, 16, slots), lambda t: (t, 0, 0)),
            block((1, rows, emb), lambda t: (t, 0, 0)),
            block((tabs, rows)),
            block((tabs, rows)),
        ],
        out_specs=(
            block((1, rows, emb), lambda t: (t, 0, 0)),
            block((tabs, rows)),
        ),
        out_shape=(shape(embeddings.shape, F32), shape(accumulator.shape, F32)),
        compiler_params=params(24),
        cost_estimate=cost(4 << 30),
        name="update",
    )(gradients, held(wanted), held(embeddings), expired, accumulator)
    return (new_rows, new_acc, weight_grad, logits[:, 0])


def solution(mesh):
    split = Mesh(mesh.devices.reshape(8, 8, 2, mesh.shape["mp"]), (*DP, "mp"))

    return jax.shard_map(
        shards,
        mesh=split,
        in_specs=(
            P("mp", DP),
            P("mp", DP, None, None),
            P("mp", DP, None),
            P("mp", DP, None),
            P("mp", DP),
            P("mp", DP, None),
            P("mp", DP),
            P(None, "mp"),
            P("mp"),
            P(DP),
        ),
        out_specs=(P("mp", DP, None), P("mp", DP), P(None, "mp"), P(DP)),
        check_vma=False,
    )
```

```python
import functools

import jax
import jax.numpy as jnp
from jax import lax
from jax.experimental import pallas as pl
from jax.experimental.pallas import tpu as pltpu
from jax.sharding import Mesh
from jax.sharding import PartitionSpec as P

DP = ("dp_0", "dp_1", "dp_2")
FAR = ("dp_0", "dp_1")
NEAR = "dp_2"

LEARN_RATE = 0.05
ACC_RESET = 0.001
F32, BF16, I32 = jnp.float32, jnp.bfloat16, jnp.int32
NT = (((1,), (1,)), ((), ()))


def iota(shape, dim):
    return lax.broadcasted_iota(I32, shape, dim)


def dot(a, b, dims=(((1,), (0,)), ((), ()))):
    return lax.dot_general(a, b, dims, preferred_element_type=F32)


def flag(cond):
    return jnp.where(cond, 1.0, 0.0).astype(BF16)


def slots_kernel(len_ref, own_ref, slot_ref, adm_ref, req_ref, sample_ref, inv_ref):
    tabs, bag, toks = own_ref.shape
    groups, width = req_ref.shape
    cap = width // tabs
    row_o, lane = iota((groups, toks), 0), iota((groups, toks), 1)
    tri = jnp.concatenate(
        [flag(row_o < lane), jnp.ones((groups, toks), BF16)], axis=1
    )
    rank_row = iota((cap, toks), 0).astype(F32)
    sample_no = (iota((1, toks), 1) + 1).astype(F32)
    for t in range(tabs):
        hot = [row_o == own_ref[t, p : p + 1, :] for p in range(bag)]
        hot16 = [flag(h) for h in hot]
        counts = dot(jnp.concatenate(hot16, axis=0), tri)
        base = jnp.zeros((groups, toks), F32)
        live_count = jnp.zeros((1, toks), F32)
        values = []
        for p in range(bag):
            part = counts[p * groups : (p + 1) * groups]
            rank = jnp.sum(
                jnp.where(hot[p], part[:, :toks] + base, 0.0), axis=0, keepdims=True
            )
            base = base + part[:, toks:]
            live = (p < len_ref[t : t + 1, :]) & (adm_ref[t, p : p + 1, :] == 1)
            live_count = live_count + jnp.where(live, 1.0, 0.0)
            slot = slot_ref[t, p : p + 1, :]
            here = rank_row == rank
            values.append(
                jnp.concatenate(
                    [
                        jnp.where(here, (slot >> 4).astype(F32), 0.0),
                        jnp.where(here, (slot & 15).astype(F32), 0.0),
                        jnp.where(here & live, sample_no, 0.0),
                    ],
                    axis=0,
                ).astype(BF16)
            )
        found = dot(
            jnp.concatenate(hot16, axis=1), jnp.concatenate(values, axis=1), NT
        )
        cols = slice(t * cap, (t + 1) * cap)
        req_ref[:, cols] = (16.0 * found[:, :cap] + found[:, cap : 2 * cap]).astype(I32)
        sample_ref[:, cols] = found[:, 2 * cap :]
        inv = 1.0 / jnp.maximum(live_count, 1.0)
        column = jnp.sum(
            jnp.where(iota((toks, toks), 0) == iota((toks, toks), 1), inv, 0.0),
            axis=1,
            keepdims=True,
        )
        inv_ref[t] = jnp.broadcast_to(column, (toks, toks))


def own_lines(table, slots):
    groups, lanes = table.shape
    cap = slots // groups
    mine = iota((cap, lanes), 1) % cap == iota((cap, lanes), 0)
    return jnp.concatenate(
        [
            jnp.where(mine, jnp.broadcast_to(table[o : o + 1], (cap, lanes)), 0.0)
            for o in range(groups)
        ],
        axis=0,
    ).astype(BF16)


def of_table(shape, lane_dim, t, kind, width, cap):
    lane = iota(shape, lane_dim)
    return flag((lane // width == kind) & (lane % width // cap == t))


def samples_kernel(sample_ref, pick_ref, row_ref):
    tabs, slots, toks = pick_ref.shape
    width = sample_ref.shape[1]
    cap = width // tabs
    own = own_lines(sample_ref[...], slots)
    wanted = (iota((slots, toks), 1) + 1).astype(F32)
    for t in range(tabs):
        mine = of_table((width, toks), 0, t, 0, width, cap)
        pick_ref[t] = flag(dot(own, mine) == wanted)
        row = dot(of_table((8, width), 1, t, 0, width, cap), own, NT)
        row_ref[t : t + 1, :] = row[0:1]


def labels_kernel(label_ref, out_ref):
    dims = out_ref.shape
    row = label_ref[...].astype(F32)
    column = jnp.sum(
        jnp.where(iota(dims, 0) == iota(dims, 1), row, 0.0), axis=1, keepdims=True
    )
    out_ref[...] = jnp.broadcast_to(column, dims)


def halves_of(arrived, block_rows):
    shift = block_rows.bit_length() - 1
    return jnp.concatenate(
        [(arrived >> shift).astype(F32), (arrived & (block_rows - 1)).astype(F32)], axis=1
    )


def fetch_kernel(
    arrived_ref, expired_ref, emb_ref, out_ref,
    gone_ref, held_ref, table_ref, sent_ref, in_sem, out_sem,
):
    groups, width = arrived_ref.shape
    tabs, rows, emb = emb_ref.shape
    cap = width // tabs
    half = rows // 2
    loads = [pltpu.make_async_copy(expired_ref, gone_ref, in_sem.at[tabs])] + [
        pltpu.make_async_copy(emb_ref.at[t], held_ref.at[t], in_sem.at[t]) for t in range(tabs)
    ]
    for load in loads:
        load.start()
    arrived = arrived_ref[...]
    low = (arrived & (half - 1)).astype(F32).T.astype(BF16)
    side = (arrived >> (half.bit_length() - 1)).astype(F32).T.astype(BF16)
    diag = iota((emb, emb), 0) == iota((emb, emb), 1)
    parts = out_sem.shape[0]
    part = groups // parts
    lane = iota((cap, emb), 1).astype(F32)
    names = lane.astype(BF16), (lane + emb).astype(BF16)
    one, zero = jnp.ones((cap, emb), BF16), jnp.zeros((cap, emb), BF16)
    stores = []
    for c in range(parts):
        mine = slice(c * part, (c + 1) * part)
        for t in range(tabs):
            if c == 0:
                if t == 0:
                    loads[0].wait()
                loads[t + 1].wait()
                for j in range(0, rows, emb):
                    gone = gone_ref[t : t + 1, j : j + emb].astype(F32)
                    column = jnp.sum(jnp.where(diag, gone, 0.0), axis=1, keepdims=True)
                    at = j // half * emb
                    table_ref[t, j % half : j % half + emb, at : at + emb] = jnp.where(
                        column > 0.5, 0.0, held_ref[t, j : j + emb, :]
                    ).astype(BF16)
            lines = slice(t * cap, (t + 1) * cap)
            picks, first = [], []
            for o in range(c * part, (c + 1) * part):
                row = jnp.broadcast_to(low[lines, o : o + 1], (cap, emb))
                picks.append(
                    jnp.concatenate([jnp.where(row == n, one, zero) for n in names], axis=1)
                )
                first.append(jnp.broadcast_to(side[lines, o : o + 1], (cap, emb)) == zero)
            both = dot(jnp.concatenate(picks, axis=0), table_ref[t]).astype(BF16)
            line = jnp.where(jnp.concatenate(first, axis=0), both[:, :emb], both[:, emb:])
            sent_ref[mine, lines, :] = line.reshape(part, cap, emb)
        store = pltpu.make_async_copy(sent_ref.at[mine], out_ref.at[mine], out_sem.at[c])
        store.start()
        stores.append(store)
    for store in stores:
        store.wait()


def wanted_kernel(arrived_ref, row_ref):
    width = arrived_ref.shape[1]
    tabs, _, slots = row_ref.shape
    cap = width // tabs
    own = own_lines(halves_of(arrived_ref[...], 128), slots)
    for t in range(tabs):
        for kind in range(2):
            row_ref[t, 8 * kind : 8 * kind + 8, :] = dot(
                of_table((8, 2 * width), 1, t, kind, width, cap), own, NT
            )


def sublanes(length, wide):
    column = iota((length, 128), 0).astype(F32).astype(BF16)
    return jnp.concatenate([column] * (wide // 128), axis=1)


def down(row, length):
    return jnp.concatenate([row] * (length // 8), axis=0).astype(BF16)


def pool_kernel(rows_ref, sample_ref, inv_ref, out_ref):
    groups, width, emb = rows_ref.shape
    tabs, toks, _ = inv_ref.shape
    cap = width // tabs
    slots = groups * cap
    one, zero = jnp.ones((toks, slots), BF16), jnp.zeros((toks, slots), BF16)
    samples = sublanes(toks, slots)
    for t in range(tabs):
        row = jnp.broadcast_to(sample_ref[t : t + 1, :] - 1.0, (16, slots)).astype(BF16)
        pick = jnp.where(jnp.concatenate([row] * (toks // 16), axis=0) == samples, one, zero)
        pooled = dot(pick, rows_ref[:, t * cap : (t + 1) * cap, :].reshape(slots, emb))
        feature = (pooled * inv_ref[t]).astype(BF16)
        for k in range(out_ref.shape[0]):
            out_ref[k, :, t * emb : (t + 1) * emb] = feature


def silu_slope(preact):
    sig = jax.nn.sigmoid(preact)
    return sig * (1.0 + preact * (1.0 - sig))


def dense_kernel(
    at_ref, feat_ref, w0, w1, w2, w3, u0, u1, u2, u3, labels_ref,
    logits_ref, grad_ref, mine_ref, other_ref, held_ref, sem_ref,
):
    parts, toks, feats = feat_ref.shape
    units = (u0, u1, u2, u3)
    loads = [
        pltpu.make_async_copy(w, held_ref.at[k], sem_ref.at[k])
        for k, w in enumerate((w1, w2, w3))
    ]
    for load in loads:
        load.start()
    weights = [w0] + [held_ref.at[k] for k in range(parts - 1)]
    me, core = at_ref[0], at_ref[1]
    preacts, scores = [], []
    for k, (w, u) in enumerate(zip(weights, units)):
        if k > 0:
            loads[k - 1].wait()
        pre = sum(
            dot(feat_ref[q], w[q * feats : (q + 1) * feats, :]) for q in range(parts)
        )
        hidden = jax.nn.silu(pre).astype(BF16).astype(F32)
        preacts.append(pre)
        scores.append(jnp.sum(hidden * u[...], axis=1, keepdims=True))
    logits = jnp.zeros((toks, 1), F32)
    for shard in range(parts):
        far = (me + parts - shard) % parts
        score = scores[0]
        for k in range(1, parts):
            score = jnp.where(far == k, scores[k], score)
        logits = logits + score
    dlogit = (jax.nn.sigmoid(logits) - labels_ref[...])[:, 0:1]
    logits_ref[...] = jnp.broadcast_to(logits, logits_ref.shape)
    start = pl.multiple_of(me * feats, feats)
    grads = jnp.zeros((toks, feats), F32)
    for k, (w, u, pre) in enumerate(zip(weights, units, preacts)):
        dhidden = (dlogit * u[...] * silu_slope(pre)).astype(BF16)
        if k == 0:
            half = dhidden.shape[1] // 2
            low, high = dhidden[:, :half], dhidden[:, half:]
            mine, other = jnp.where(core == 0, low, high), jnp.where(core == 0, high, low)
            for q in range(parts):
                lines = slice(q * feats, (q + 1) * feats)
                part = dot(
                    feat_ref[q],
                    jnp.concatenate([mine, other], axis=1),
                    (((0,), (0,)), ((), ())),
                ).astype(BF16)
                mine_ref[lines, :] = part[:, :half]
                other_ref[lines, :] = part[:, half:]
        grads = grads + dot(dhidden, w[pl.ds(start, feats), :], NT)
    grad_ref[...] = grads


def spread_kernel(grad_ref, inv_ref, pick_ref, out_ref):
    slots = pick_ref.shape[1]
    cap, emb = out_ref.shape[1:]
    grad = (inv_ref[0] * grad_ref[...]).astype(BF16)
    out_ref[...] = dot(pick_ref[0], grad).astype(BF16).reshape(slots // cap, cap, emb)


def update_kernel(grads_ref, wanted_ref, emb_ref, expired_ref, acc_ref, new_ref, new_acc_ref):
    groups, cap, emb = grads_ref.shape
    rows = emb_ref.shape[1]
    slots = groups * cap
    t = pl.program_id(0)
    grads = grads_ref[...].reshape(slots, emb)
    at = down(wanted_ref[0, 0:8, :], 16)
    low = down(wanted_ref[0, 8:16, :], 16)
    low = jnp.concatenate([low] * (emb // 16), axis=0)
    one, zero = jnp.ones((emb, slots), BF16), jnp.zeros((emb, slots), BF16)
    hot = jnp.where(low == sublanes(emb, slots), one, zero)
    gone = expired_ref[pl.ds(t, 1), :]
    fresh_acc = jnp.where(gone == 1, ACC_RESET, acc_ref[pl.ds(t, 1), :])
    kept = jnp.where(gone == 1, 0.0, 1.0)
    diag = iota((emb, emb), 0) == iota((emb, emb), 1)
    for j in range(0, rows, emb):
        here = jnp.concatenate([at == jnp.full_like(at, j // emb)] * (emb // 16), axis=0)
        summed = dot(jnp.where(here, hot, zero), grads)
        cols = slice(j, j + emb)
        old = jnp.sum(jnp.where(diag, fresh_acc[:, cols], 0.0), axis=1, keepdims=True)
        keep = jnp.sum(jnp.where(diag, kept[:, cols], 0.0), axis=1, keepdims=True)
        acc = old + jnp.sum(summed * summed, axis=1, keepdims=True) * (1.0 / emb)
        fresh = jnp.where(keep > 0.5, emb_ref[0, j : j + emb, :], 0.0)
        new_ref[0, j : j + emb, :] = fresh - LEARN_RATE * summed / jnp.sqrt(acc)
        line = jnp.sum(jnp.where(diag, acc, 0.0), axis=0, keepdims=True)
        for table in range(acc_ref.shape[0]):

            @pl.when(t == table)
            def _(table=table, cols=cols, line=line):
                new_acc_ref[table : table + 1, cols] = line


def near_kernel(at_ref, piece_ref, out_ref, sem):
    copy = pltpu.make_async_copy(piece_ref, out_ref.at[at_ref[1]], sem)
    copy.start()
    copy.wait()


def far_kernel(at_ref, piece_ref, begun_ref, out_ref, sem):
    copy = pltpu.make_async_copy(piece_ref, out_ref.at[1 - at_ref[1]], sem)
    copy.start()
    copy.wait()


def shape(dims, dtype):
    return jax.ShapeDtypeStruct(dims, dtype)


def block(dims, index=None):
    if index is None:
        return pl.BlockSpec(dims, lambda *_: (0,) * len(dims))
    return pl.BlockSpec(dims, index)


def params(mib):
    return pltpu.CompilerParams(vmem_limit_bytes=mib << 20)


def cost(flops):
    return pl.CostEstimate(flops=flops, bytes_accessed=1 << 20, transcendentals=0)


def a2a(value, axis):
    return lax.all_to_all(value, axis, split_axis=0, concat_axis=0, tiled=True)


def from_everyone(value, axis):
    size = lax.axis_size(axis)
    return a2a(jnp.broadcast_to(value[None], (size, *value.shape)), axis)


def ring(value, axis, step):
    size = lax.axis_size(axis)
    return lax.ppermute(value, axis, [(i, (i + step) % size) for i in range(size)])


def shards(
    bag_lengths, owners, row_slots, admit_mask, expired, embeddings, accumulator,
    hidden_weight, output_weight, labels,
):
    groups = lax.axis_size(DP)
    parts = lax.axis_size("mp")
    tabs, toks, bag = row_slots.shape
    rows, emb = embeddings.shape[1:]
    cap = 2 * toks * bag // groups
    width = tabs * cap
    slots = groups * cap
    feats = tabs * emb
    core = lax.axis_index(NEAR).astype(I32)
    place = jnp.stack([lax.axis_index("mp").astype(I32), core])

    request, sample, inv = pl.pallas_call(
        slots_kernel,
        out_shape=(
            shape((groups, width), I32),
            shape((groups, width), F32),
            shape((tabs, toks, toks), F32),
        ),
        compiler_params=params(24),
        name="slots",
    )(
        *map(
            functools.partial(pltpu.with_memory_space_constraint, memory_space=pltpu.HBM),
            (
                bag_lengths,
                owners[..., 0].swapaxes(1, 2),
                row_slots.swapaxes(1, 2),
                admit_mask.swapaxes(1, 2),
            ),
        )
    )
    arrived = a2a(request, DP)
    weight, _ = lax.optimization_barrier((hidden_weight, request))
    weights = [weight] + [ring(weight, "mp", k) for k in range(1, parts)]
    pick, sample_row = pl.pallas_call(
        samples_kernel,
        out_shape=(
            pltpu.HBM((tabs, slots, toks), BF16),
            shape((tabs, slots), F32),
        ),
        compiler_params=params(24),
        cost_estimate=cost(4 << 30),
        name="samples",
    )(sample)
    held = functools.partial(pltpu.with_memory_space_constraint, memory_space=pltpu.HBM)
    smem, vmem, hbm = (
        pl.BlockSpec(memory_space=space) for space in (pltpu.SMEM, pltpu.VMEM, pltpu.HBM)
    )
    dma = pltpu.SemaphoreType.DMA
    fetched = pl.pallas_call(
        fetch_kernel,
        in_specs=[vmem, hbm, hbm],
        out_specs=hbm,
        out_shape=pltpu.HBM((groups, width, emb), BF16),
        scratch_shapes=[
            pltpu.VMEM((tabs, rows), I32),
            pltpu.VMEM((tabs, rows, emb), F32),
            pltpu.VMEM((tabs, rows // 2, 2 * emb), BF16),
            pltpu.VMEM((groups, width, emb), BF16),
            dma((tabs + 1,)),
            dma((8,)),
        ],
        compiler_params=params(24),
        name="fetch",
    )(arrived, held(expired), held(embeddings))
    returned = a2a(fetched, DP)
    unit, later = lax.optimization_barrier((output_weight, arrived))
    unit = unit.reshape(1, -1)
    units = [unit] + [ring(unit, "mp", k) for k in range(1, parts)]
    wanted = pl.pallas_call(
        wanted_kernel,
        out_shape=pltpu.HBM((tabs, 16, slots), F32),
        compiler_params=params(24),
        cost_estimate=cost(4 << 30),
        name="wanted",
    )(later)
    features = pl.pallas_call(
        pool_kernel,
        out_shape=shape((parts, toks, feats), BF16),
        compiler_params=params(24),
        name="pool",
    )(returned, sample_row, inv)
    features, place, weights, units = lax.optimization_barrier(
        (features, place, weights, units)
    )
    portion = a2a(features, "mp")
    label_column = pl.pallas_call(
        labels_kernel,
        out_shape=shape((toks, toks), F32),
        compiler_params=params(4),
        name="labels",
    )(labels.reshape(1, toks))
    units_dev = hidden_weight.shape[1]
    lines, half = hidden_weight.shape[0], units_dev // 2
    logits, grad, mine, other = pl.pallas_call(
        dense_kernel,
        in_specs=[smem, vmem, vmem] + [hbm] * (parts - 1) + [vmem] * (parts + 1),
        out_shape=(
            shape((toks, toks), F32),
            shape((toks, feats), F32),
            shape((lines, half), BF16),
            shape((lines, half), BF16),
        ),
        scratch_shapes=[
            pltpu.VMEM((parts - 1, lines, units_dev), BF16),
            dma((parts - 1,)),
        ],
        compiler_params=params(24),
        name="dense",
    )(place, portion, weights[0], *map(held, weights[1:]), *units, label_column)
    joined = ring(other, NEAR, 1)
    share = lines // groups
    outgoing = pl.pallas_call(
        spread_kernel,
        grid=(tabs,),
        in_specs=[
            block((toks, emb), lambda t: (0, t)),
            block((1, toks, toks), lambda t: (t, 0, 0)),
            block((1, slots, toks), lambda t: (t, 0, 0)),
        ],
        out_specs=block((groups, cap, emb), lambda t: (0, t, 0)),
        out_shape=shape((groups, width + share, emb), BF16),
        compiler_params=params(24),
        cost_estimate=cost(4 << 30),
        name="spread",
    )(grad, inv, pick)
    pair = (mine.astype(F32) + joined.astype(F32)).astype(BF16)
    pair = pair.reshape(2, groups // 2, share, half).swapaxes(0, 1)
    outgoing = lax.dynamic_update_slice(
        outgoing, pair.reshape(groups, share, half), (0, width, 0)
    )
    gradients = a2a(outgoing, DP)
    shares = gradients[:, width:].reshape(groups // 2, 2, 2, share // 2, half)
    own = shares.astype(F32).sum(axis=0).astype(BF16).swapaxes(0, 1)
    near = from_everyone(own, FAR)
    near = near.transpose(0, 1, 3, 2, 4).reshape(lines // 2, units_dev)
    far = ring(near, NEAR, 1)
    weight_grad = None
    for kernel, piece in ((near_kernel, near), (far_kernel, far)):
        begun = [] if weight_grad is None else [weight_grad]
        weight_grad = pl.pallas_call(
            kernel,
            in_specs=[smem, vmem] + [hbm] * len(begun),
            out_specs=hbm,
            out_shape=pltpu.HBM((2, lines // 2, units_dev), BF16),
            input_output_aliases={2: 0} if begun else {},
            scratch_shapes=[dma],
            compiler_params=params(4),
            name="near" if weight_grad is None else "far",
        )(place, piece, *begun)
    weight_grad = weight_grad.reshape(lines, units_dev)
    new_rows, new_acc = pl.pallas_call(
        update_kernel,
        grid=(tabs,),
        in_specs=[
            block((groups, cap, emb), lambda t: (0, t, 0)),
            block((1, 16, slots), lambda t: (t, 0, 0)),
            block((1, rows, emb), lambda t: (t, 0, 0)),
            block((tabs, rows)),
            block((tabs, rows)),
        ],
        out_specs=(
            block((1, rows, emb), lambda t: (t, 0, 0)),
            block((tabs, rows)),
        ),
        out_shape=(shape(embeddings.shape, F32), shape(accumulator.shape, F32)),
        compiler_params=params(24),
        cost_estimate=cost(4 << 30),
        name="update",
    )(gradients, held(wanted), held(embeddings), expired, accumulator)
    return (new_rows, new_acc, weight_grad, logits[:, 0])


def solution(mesh):
    split = Mesh(mesh.devices.reshape(8, 8, 2, mesh.shape["mp"]), (*DP, "mp"))

    return jax.shard_map(
        shards,
        mesh=split,
        in_specs=(
            P("mp", DP),
            P("mp", DP, None, None),
            P("mp", DP, None),
            P("mp", DP, None),
            P("mp", DP),
            P("mp", DP, None),
            P("mp", DP),
            P(None, "mp"),
            P("mp"),
            P(DP),
        ),
        out_specs=(P("mp", DP, None), P("mp", DP), P(None, "mp"), P(DP)),
        check_vma=False,
    )
```

```python
import functools

import jax
import jax.numpy as jnp
from jax import lax
from jax.experimental import pallas as pl
from jax.experimental.pallas import tpu as pltpu
from jax.sharding import Mesh
from jax.sharding import PartitionSpec as P

DP = ("dp_0", "dp_1", "dp_2")
FAR = ("dp_0", "dp_1")
NEAR = "dp_2"

LEARN_RATE = 0.05
ACC_RESET = 0.001
F32, BF16, I32 = jnp.float32, jnp.bfloat16, jnp.int32
NT = (((1,), (1,)), ((), ()))


def iota(shape, dim):
    return lax.broadcasted_iota(I32, shape, dim)


def dot(a, b, dims=(((1,), (0,)), ((), ()))):
    return lax.dot_general(a, b, dims, preferred_element_type=F32)


def flag(cond):
    return jnp.where(cond, 1.0, 0.0).astype(BF16)


def slots_kernel(len_ref, own_ref, slot_ref, adm_ref, req_ref, sample_ref, inv_ref):
    tabs, bag, toks = own_ref.shape
    groups, width = req_ref.shape
    cap = width // tabs
    row_o, lane = iota((groups, toks), 0), iota((groups, toks), 1)
    tri = jnp.concatenate(
        [flag(row_o < lane), jnp.ones((groups, toks), BF16)], axis=1
    )
    rank_row = iota((cap, toks), 0).astype(F32)
    sample_no = (iota((1, toks), 1) + 1).astype(F32)
    for t in range(tabs):
        hot = [row_o == own_ref[t, p : p + 1, :] for p in range(bag)]
        hot16 = [flag(h) for h in hot]
        counts = dot(jnp.concatenate(hot16, axis=0), tri)
        base = jnp.zeros((groups, toks), F32)
        live_count = jnp.zeros((1, toks), F32)
        values = []
        for p in range(bag):
            part = counts[p * groups : (p + 1) * groups]
            rank = jnp.sum(
                jnp.where(hot[p], part[:, :toks] + base, 0.0), axis=0, keepdims=True
            )
            base = base + part[:, toks:]
            live = (p < len_ref[t : t + 1, :]) & (adm_ref[t, p : p + 1, :] == 1)
            live_count = live_count + jnp.where(live, 1.0, 0.0)
            slot = slot_ref[t, p : p + 1, :]
            here = rank_row == rank
            values.append(
                jnp.concatenate(
                    [
                        jnp.where(here, (slot >> 4).astype(F32), 0.0),
                        jnp.where(here, (slot & 15).astype(F32), 0.0),
                        jnp.where(here & live, sample_no, 0.0),
                    ],
                    axis=0,
                ).astype(BF16)
            )
        found = dot(
            jnp.concatenate(hot16, axis=1), jnp.concatenate(values, axis=1), NT
        )
        cols = slice(t * cap, (t + 1) * cap)
        req_ref[:, cols] = (16.0 * found[:, :cap] + found[:, cap : 2 * cap]).astype(I32)
        sample_ref[:, cols] = found[:, 2 * cap :]
        inv = 1.0 / jnp.maximum(live_count, 1.0)
        column = jnp.sum(
            jnp.where(iota((toks, toks), 0) == iota((toks, toks), 1), inv, 0.0),
            axis=1,
            keepdims=True,
        )
        inv_ref[t] = jnp.broadcast_to(column, (toks, toks))


def own_lines(table, slots):
    groups, lanes = table.shape
    cap = slots // groups
    mine = iota((cap, lanes), 1) % cap == iota((cap, lanes), 0)
    return jnp.concatenate(
        [
            jnp.where(mine, jnp.broadcast_to(table[o : o + 1], (cap, lanes)), 0.0)
            for o in range(groups)
        ],
        axis=0,
    ).astype(BF16)


def of_table(shape, lane_dim, t, kind, width, cap):
    lane = iota(shape, lane_dim)
    return flag((lane // width == kind) & (lane % width // cap == t))


def samples_kernel(sample_ref, pick_ref, row_ref):
    tabs, slots, toks = pick_ref.shape
    width = sample_ref.shape[1]
    cap = width // tabs
    own = own_lines(sample_ref[...], slots)
    wanted = (iota((slots, toks), 1) + 1).astype(F32)
    for t in range(tabs):
        mine = of_table((width, toks), 0, t, 0, width, cap)
        pick_ref[t] = flag(dot(own, mine) == wanted)
        row = dot(of_table((8, width), 1, t, 0, width, cap), own, NT)
        row_ref[t : t + 1, :] = row[0:1]


def labels_kernel(label_ref, out_ref):
    dims = out_ref.shape
    row = label_ref[...].astype(F32)
    column = jnp.sum(
        jnp.where(iota(dims, 0) == iota(dims, 1), row, 0.0), axis=1, keepdims=True
    )
    out_ref[...] = jnp.broadcast_to(column, dims)


def halves_of(arrived, block_rows):
    shift = block_rows.bit_length() - 1
    return jnp.concatenate(
        [(arrived >> shift).astype(F32), (arrived & (block_rows - 1)).astype(F32)], axis=1
    )


def fetch_kernel(
    arrived_ref, expired_ref, emb_ref, out_ref,
    gone_ref, held_ref, table_ref, sent_ref, in_sem, out_sem,
):
    groups, width = arrived_ref.shape
    tabs, rows, emb = emb_ref.shape
    cap = width // tabs
    half = rows // 2
    loads = [pltpu.make_async_copy(expired_ref, gone_ref, in_sem.at[tabs])] + [
        pltpu.make_async_copy(emb_ref.at[t], held_ref.at[t], in_sem.at[t]) for t in range(tabs)
    ]
    for load in loads:
        load.start()
    arrived = arrived_ref[...]
    low = (arrived & (half - 1)).astype(F32).T.astype(BF16)
    side = (arrived >> (half.bit_length() - 1)).astype(F32).T.astype(BF16)
    diag = iota((emb, emb), 0) == iota((emb, emb), 1)
    parts = out_sem.shape[0]
    part = groups // parts
    lane = iota((cap, emb), 1).astype(F32)
    names = lane.astype(BF16), (lane + emb).astype(BF16)
    one, zero = jnp.ones((cap, emb), BF16), jnp.zeros((cap, emb), BF16)
    stores = []
    for c in range(parts):
        mine = slice(c * part, (c + 1) * part)
        for t in range(tabs):
            if c == 0:
                if t == 0:
                    loads[0].wait()
                loads[t + 1].wait()
                for j in range(0, rows, emb):
                    gone = gone_ref[t : t + 1, j : j + emb].astype(F32)
                    column = jnp.sum(jnp.where(diag, gone, 0.0), axis=1, keepdims=True)
                    at = j // half * emb
                    table_ref[t, j % half : j % half + emb, at : at + emb] = jnp.where(
                        column > 0.5, 0.0, held_ref[t, j : j + emb, :]
                    ).astype(BF16)
            lines = slice(t * cap, (t + 1) * cap)
            picks, first = [], []
            for o in range(c * part, (c + 1) * part):
                row = jnp.broadcast_to(low[lines, o : o + 1], (cap, emb))
                picks.append(
                    jnp.concatenate([jnp.where(row == n, one, zero) for n in names], axis=1)
                )
                first.append(jnp.broadcast_to(side[lines, o : o + 1], (cap, emb)) == zero)
            both = dot(jnp.concatenate(picks, axis=0), table_ref[t]).astype(BF16)
            line = jnp.where(jnp.concatenate(first, axis=0), both[:, :emb], both[:, emb:])
            sent_ref[mine, lines, :] = line.reshape(part, cap, emb)
        store = pltpu.make_async_copy(sent_ref.at[mine], out_ref.at[mine], out_sem.at[c])
        store.start()
        stores.append(store)
    for store in stores:
        store.wait()


def wanted_kernel(arrived_ref, row_ref):
    width = arrived_ref.shape[1]
    tabs, _, slots = row_ref.shape
    cap = width // tabs
    own = own_lines(halves_of(arrived_ref[...], 128), slots)
    for t in range(tabs):
        for kind in range(2):
            row_ref[t, 8 * kind : 8 * kind + 8, :] = dot(
                of_table((8, 2 * width), 1, t, kind, width, cap), own, NT
            )


def sublanes(length, wide):
    column = iota((length, 128), 0).astype(F32).astype(BF16)
    return jnp.concatenate([column] * (wide // 128), axis=1)


def down(row, length):
    return jnp.concatenate([row] * (length // 8), axis=0).astype(BF16)


def pool_kernel(rows_ref, sample_ref, inv_ref, out_ref):
    groups, width, emb = rows_ref.shape
    tabs, toks, _ = inv_ref.shape
    cap = width // tabs
    slots = groups * cap
    one, zero = jnp.ones((toks, slots), BF16), jnp.zeros((toks, slots), BF16)
    samples = sublanes(toks, slots)
    for t in range(tabs):
        row = jnp.broadcast_to(sample_ref[t : t + 1, :] - 1.0, (16, slots)).astype(BF16)
        pick = jnp.where(jnp.concatenate([row] * (toks // 16), axis=0) == samples, one, zero)
        pooled = dot(pick, rows_ref[:, t * cap : (t + 1) * cap, :].reshape(slots, emb))
        feature = (pooled * inv_ref[t]).astype(BF16)
        for k in range(out_ref.shape[0]):
            out_ref[k, :, t * emb : (t + 1) * emb] = feature


def silu_slope(preact):
    sig = jax.nn.sigmoid(preact)
    return sig * (1.0 + preact * (1.0 - sig))


def dense_kernel(
    at_ref, feat_ref, own_ref, near_ref, far_ref, u0, u1, u2, u3, labels_ref,
    logits_ref, grad_ref, mine_ref, other_ref,
):
    parts, toks, feats = feat_ref.shape
    units = (u0, u1, u2, u3)
    me, core = at_ref[0], at_ref[1]
    order = [(2 * core + q) % parts for q in range(parts)]
    preacts, scores = [], []
    for k, u in enumerate(units):
        pre = jnp.zeros((toks, u.shape[1]), F32)
        for q, at in enumerate(order):
            if k == 0:
                w = own_ref[pl.ds(pl.multiple_of(at * feats, feats), feats), :]
            else:
                half = near_ref if q < parts // 2 else far_ref
                start = q % (parts // 2) * feats
                w = half[k - 1, start : start + feats, :]
            pre = pre + dot(feat_ref[at], w)
        hidden = jax.nn.silu(pre).astype(BF16).astype(F32)
        preacts.append(pre)
        scores.append(jnp.sum(hidden * u[...], axis=1, keepdims=True))
    logits = jnp.zeros((toks, 1), F32)
    for shard in range(parts):
        far = (me + parts - shard) % parts
        score = scores[0]
        for k in range(1, parts):
            score = jnp.where(far == k, scores[k], score)
        logits = logits + score
    dlogit = (jax.nn.sigmoid(logits) - labels_ref[...])[:, 0:1]
    logits_ref[...] = jnp.broadcast_to(logits, logits_ref.shape)
    grads = jnp.zeros((toks, feats), F32)
    for k, (u, pre) in enumerate(zip(units, preacts)):
        dhidden = (dlogit * u[...] * silu_slope(pre)).astype(BF16)
        if k == 0:
            half = dhidden.shape[1] // 2
            low, high = dhidden[:, :half], dhidden[:, half:]
            mine, other = jnp.where(core == 0, low, high), jnp.where(core == 0, high, low)
            for q in range(parts):
                lines = slice(q * feats, (q + 1) * feats)
                part = dot(
                    feat_ref[q],
                    jnp.concatenate([mine, other], axis=1),
                    (((0,), (0,)), ((), ())),
                ).astype(BF16)
                mine_ref[lines, :] = part[:, :half]
                other_ref[lines, :] = part[:, half:]
            w = own_ref[pl.ds(pl.multiple_of(me * feats, feats), feats), :]
        else:
            lines = pl.ds(pl.multiple_of(me % (parts // 2) * feats, feats), feats)
            w = jnp.where(
                me // (parts // 2) == core, near_ref[k - 1, lines, :], far_ref[k - 1, lines, :]
            )
        grads = grads + dot(dhidden, w, NT)
    grad_ref[...] = grads


def spread_kernel(grad_ref, inv_ref, pick_ref, out_ref):
    slots = pick_ref.shape[1]
    cap, emb = out_ref.shape[1:]
    grad = (inv_ref[0] * grad_ref[...]).astype(BF16)
    out_ref[...] = dot(pick_ref[0], grad).astype(BF16).reshape(slots // cap, cap, emb)


def update_kernel(grads_ref, wanted_ref, emb_ref, expired_ref, acc_ref, new_ref, new_acc_ref):
    groups, cap, emb = grads_ref.shape
    rows = emb_ref.shape[1]
    slots = groups * cap
    t = pl.program_id(0)
    grads = grads_ref[...].reshape(slots, emb)
    at = down(wanted_ref[0, 0:8, :], 16)
    low = down(wanted_ref[0, 8:16, :], 16)
    low = jnp.concatenate([low] * (emb // 16), axis=0)
    one, zero = jnp.ones((emb, slots), BF16), jnp.zeros((emb, slots), BF16)
    hot = jnp.where(low == sublanes(emb, slots), one, zero)
    gone = expired_ref[pl.ds(t, 1), :]
    fresh_acc = jnp.where(gone == 1, ACC_RESET, acc_ref[pl.ds(t, 1), :])
    kept = jnp.where(gone == 1, 0.0, 1.0)
    diag = iota((emb, emb), 0) == iota((emb, emb), 1)
    for j in range(0, rows, emb):
        here = jnp.concatenate([at == jnp.full_like(at, j // emb)] * (emb // 16), axis=0)
        summed = dot(jnp.where(here, hot, zero), grads)
        cols = slice(j, j + emb)
        old = jnp.sum(jnp.where(diag, fresh_acc[:, cols], 0.0), axis=1, keepdims=True)
        keep = jnp.sum(jnp.where(diag, kept[:, cols], 0.0), axis=1, keepdims=True)
        acc = old + jnp.sum(summed * summed, axis=1, keepdims=True) * (1.0 / emb)
        fresh = jnp.where(keep > 0.5, emb_ref[0, j : j + emb, :], 0.0)
        new_ref[0, j : j + emb, :] = fresh - LEARN_RATE * summed / jnp.sqrt(acc)
        line = jnp.sum(jnp.where(diag, acc, 0.0), axis=0, keepdims=True)
        for table in range(acc_ref.shape[0]):

            @pl.when(t == table)
            def _(table=table, cols=cols, line=line):
                new_acc_ref[table : table + 1, cols] = line


def shape(dims, dtype):
    return jax.ShapeDtypeStruct(dims, dtype)


def block(dims, index=None):
    if index is None:
        return pl.BlockSpec(dims, lambda *_: (0,) * len(dims))
    return pl.BlockSpec(dims, index)


def params(mib):
    return pltpu.CompilerParams(vmem_limit_bytes=mib << 20)


def cost(flops):
    return pl.CostEstimate(flops=flops, bytes_accessed=1 << 20, transcendentals=0)


def a2a(value, axis):
    return lax.all_to_all(value, axis, split_axis=0, concat_axis=0, tiled=True)


def from_everyone(value, axis):
    size = lax.axis_size(axis)
    return a2a(jnp.broadcast_to(value[None], (size, *value.shape)), axis)


def ring(value, axis, step):
    size = lax.axis_size(axis)
    return lax.ppermute(value, axis, [(i, (i + step) % size) for i in range(size)])


def shards(
    bag_lengths, owners, row_slots, admit_mask, expired, embeddings, accumulator,
    hidden_weight, output_weight, labels,
):
    groups = lax.axis_size(DP)
    parts = lax.axis_size("mp")
    tabs, toks, bag = row_slots.shape
    rows, emb = embeddings.shape[1:]
    cap = 2 * toks * bag // groups
    width = tabs * cap
    slots = groups * cap
    feats = tabs * emb
    core = lax.axis_index(NEAR).astype(I32)
    place = jnp.stack([lax.axis_index("mp").astype(I32), core])

    request, sample, inv = pl.pallas_call(
        slots_kernel,
        out_shape=(
            shape((groups, width), I32),
            shape((groups, width), F32),
            shape((tabs, toks, toks), F32),
        ),
        compiler_params=params(24),
        name="slots",
    )(
        *map(
            functools.partial(pltpu.with_memory_space_constraint, memory_space=pltpu.HBM),
            (
                bag_lengths,
                owners[..., 0].swapaxes(1, 2),
                row_slots.swapaxes(1, 2),
                admit_mask.swapaxes(1, 2),
            ),
        )
    )
    arrived = a2a(request, DP)
    lines, units_dev = hidden_weight.shape
    weight, _ = lax.optimization_barrier((hidden_weight, request))
    mine = lax.dynamic_slice(weight, (core * (lines // 2), 0), (lines // 2, units_dev))
    near_weights = jnp.stack([ring(mine, "mp", k) for k in range(1, parts)])
    far_weights = ring(near_weights, NEAR, 1)
    pick, sample_row = pl.pallas_call(
        samples_kernel,
        out_shape=(
            pltpu.HBM((tabs, slots, toks), BF16),
            shape((tabs, slots), F32),
        ),
        compiler_params=params(24),
        cost_estimate=cost(4 << 30),
        name="samples",
    )(sample)
    held = functools.partial(pltpu.with_memory_space_constraint, memory_space=pltpu.HBM)
    smem, vmem, hbm = (
        pl.BlockSpec(memory_space=space) for space in (pltpu.SMEM, pltpu.VMEM, pltpu.HBM)
    )
    dma = pltpu.SemaphoreType.DMA
    fetched = pl.pallas_call(
        fetch_kernel,
        in_specs=[vmem, hbm, hbm],
        out_specs=hbm,
        out_shape=pltpu.HBM((groups, width, emb), BF16),
        scratch_shapes=[
            pltpu.VMEM((tabs, rows), I32),
            pltpu.VMEM((tabs, rows, emb), F32),
            pltpu.VMEM((tabs, rows // 2, 2 * emb), BF16),
            pltpu.VMEM((groups, width, emb), BF16),
            dma((tabs + 1,)),
            dma((8,)),
        ],
        compiler_params=params(24),
        name="fetch",
    )(arrived, held(expired), held(embeddings))
    returned = a2a(fetched, DP)
    unit, later = lax.optimization_barrier((output_weight, arrived))
    unit = unit.reshape(1, -1)
    units = [unit] + [ring(unit, "mp", k) for k in range(1, parts)]
    wanted = pl.pallas_call(
        wanted_kernel,
        out_shape=pltpu.HBM((tabs, 16, slots), F32),
        compiler_params=params(24),
        cost_estimate=cost(4 << 30),
        name="wanted",
    )(later)
    features = pl.pallas_call(
        pool_kernel,
        out_shape=shape((parts, toks, feats), BF16),
        compiler_params=params(24),
        name="pool",
    )(returned, sample_row, inv)
    features, place, near_weights, far_weights, units = lax.optimization_barrier(
        (features, place, near_weights, far_weights, units)
    )
    portion = a2a(features, "mp")
    label_column = pl.pallas_call(
        labels_kernel,
        out_shape=shape((toks, toks), F32),
        compiler_params=params(4),
        name="labels",
    )(labels.reshape(1, toks))
    half = units_dev // 2
    logits, grad, mine, other = pl.pallas_call(
        dense_kernel,
        in_specs=[smem] + [vmem] * (parts + 5),
        out_shape=(
            shape((toks, toks), F32),
            shape((toks, feats), F32),
            shape((lines, half), BF16),
            shape((lines, half), BF16),
        ),
        compiler_params=params(24),
        name="dense",
    )(place, portion, hidden_weight, near_weights, far_weights, *units, label_column)
    joined = ring(other, NEAR, 1)
    share = lines // groups
    outgoing = pl.pallas_call(
        spread_kernel,
        grid=(tabs,),
        in_specs=[
            block((toks, emb), lambda t: (0, t)),
            block((1, toks, toks), lambda t: (t, 0, 0)),
            block((1, slots, toks), lambda t: (t, 0, 0)),
        ],
        out_specs=block((groups, cap, emb), lambda t: (0, t, 0)),
        out_shape=shape((groups, width + share, emb), BF16),
        compiler_params=params(24),
        cost_estimate=cost(4 << 30),
        name="spread",
    )(grad, inv, pick)
    pair = (mine.astype(F32) + joined.astype(F32)).astype(BF16)
    pair = pair.reshape(2, groups // 2, share, half).swapaxes(0, 1)
    outgoing = lax.dynamic_update_slice(
        outgoing, pair.reshape(groups, share, half), (0, width, 0)
    )
    gradients = a2a(outgoing, DP)
    shares = gradients[:, width:].reshape(groups // 2, 2, 2, share // 2, half)
    own = shares.astype(F32).sum(axis=0).astype(BF16).swapaxes(0, 1)
    near = from_everyone(own, FAR)
    near = near.transpose(0, 1, 3, 2, 4).reshape(lines // 2, units_dev)
    far = ring(near, NEAR, 1)
    weight_grad = jnp.concatenate(
        [jnp.where(core == 0, near, far), jnp.where(core == 0, far, near)]
    )
    new_rows, new_acc = pl.pallas_call(
        update_kernel,
        grid=(tabs,),
        in_specs=[
            block((groups, cap, emb), lambda t: (0, t, 0)),
            block((1, 16, slots), lambda t: (t, 0, 0)),
            block((1, rows, emb), lambda t: (t, 0, 0)),
            block((tabs, rows)),
            block((tabs, rows)),
        ],
        out_specs=(
            block((1, rows, emb), lambda t: (t, 0, 0)),
            block((tabs, rows)),
        ),
        out_shape=(shape(embeddings.shape, F32), shape(accumulator.shape, F32)),
        compiler_params=params(24),
        cost_estimate=cost(4 << 30),
        name="update",
    )(gradients, held(wanted), held(embeddings), expired, accumulator)
    return (new_rows, new_acc, weight_grad, logits[:, 0])


def solution(mesh):
    split = Mesh(mesh.devices.reshape(8, 8, 2, mesh.shape["mp"]), (*DP, "mp"))

    return jax.shard_map(
        shards,
        mesh=split,
        in_specs=(
            P("mp", DP),
            P("mp", DP, None, None),
            P("mp", DP, None),
            P("mp", DP, None),
            P("mp", DP),
            P("mp", DP, None),
            P("mp", DP),
            P(None, "mp"),
            P("mp"),
            P(DP),
        ),
        out_specs=(P("mp", DP, None), P("mp", DP), P(None, "mp"), P(DP)),
        check_vma=False,
    )
```

```python
import functools

import jax
import jax.numpy as jnp
from jax import lax
from jax.experimental import pallas as pl
from jax.experimental.pallas import tpu as pltpu
from jax.sharding import Mesh
from jax.sharding import PartitionSpec as P

DP = ("dp_0", "dp_1", "dp_2")
FAR = ("dp_0", "dp_1")
NEAR = "dp_2"

LEARN_RATE = 0.05
ACC_RESET = 0.001
F32, BF16, I32 = jnp.float32, jnp.bfloat16, jnp.int32
NT = (((1,), (1,)), ((), ()))


def iota(shape, dim):
    return lax.broadcasted_iota(I32, shape, dim)


def dot(a, b, dims=(((1,), (0,)), ((), ()))):
    return lax.dot_general(a, b, dims, preferred_element_type=F32)


def flag(cond):
    return jnp.where(cond, 1.0, 0.0).astype(BF16)


def slots_kernel(len_ref, own_ref, slot_ref, adm_ref, req_ref, sample_ref, inv_ref):
    tabs, bag, toks = own_ref.shape
    groups, width = req_ref.shape
    cap = width // tabs
    row_o, lane = iota((groups, toks), 0), iota((groups, toks), 1)
    tri = jnp.concatenate(
        [flag(row_o < lane), jnp.ones((groups, toks), BF16)], axis=1
    )
    rank_row = iota((cap, toks), 0).astype(F32)
    sample_no = (iota((1, toks), 1) + 1).astype(F32)
    for t in range(tabs):
        hot = [row_o == own_ref[t, p : p + 1, :] for p in range(bag)]
        hot16 = [flag(h) for h in hot]
        counts = dot(jnp.concatenate(hot16, axis=0), tri)
        base = jnp.zeros((groups, toks), F32)
        live_count = jnp.zeros((1, toks), F32)
        values = []
        for p in range(bag):
            part = counts[p * groups : (p + 1) * groups]
            rank = jnp.sum(
                jnp.where(hot[p], part[:, :toks] + base, 0.0), axis=0, keepdims=True
            )
            base = base + part[:, toks:]
            live = (p < len_ref[t : t + 1, :]) & (adm_ref[t, p : p + 1, :] == 1)
            live_count = live_count + jnp.where(live, 1.0, 0.0)
            slot = slot_ref[t, p : p + 1, :]
            here = rank_row == rank
            values.append(
                jnp.concatenate(
                    [
                        jnp.where(here, (slot >> 4).astype(F32), 0.0),
                        jnp.where(here, (slot & 15).astype(F32), 0.0),
                        jnp.where(here & live, sample_no, 0.0),
                    ],
                    axis=0,
                ).astype(BF16)
            )
        found = dot(
            jnp.concatenate(hot16, axis=1), jnp.concatenate(values, axis=1), NT
        )
        cols = slice(t * cap, (t + 1) * cap)
        req_ref[:, cols] = (16.0 * found[:, :cap] + found[:, cap : 2 * cap]).astype(I32)
        sample_ref[:, cols] = found[:, 2 * cap :]
        inv = 1.0 / jnp.maximum(live_count, 1.0)
        column = jnp.sum(
            jnp.where(iota((toks, toks), 0) == iota((toks, toks), 1), inv, 0.0),
            axis=1,
            keepdims=True,
        )
        inv_ref[t] = jnp.broadcast_to(column, (toks, toks))


def own_lines(table, slots):
    groups, lanes = table.shape
    cap = slots // groups
    mine = iota((cap, lanes), 1) % cap == iota((cap, lanes), 0)
    return jnp.concatenate(
        [
            jnp.where(mine, jnp.broadcast_to(table[o : o + 1], (cap, lanes)), 0.0)
            for o in range(groups)
        ],
        axis=0,
    ).astype(BF16)


def of_table(shape, lane_dim, t, kind, width, cap):
    lane = iota(shape, lane_dim)
    return flag((lane // width == kind) & (lane % width // cap == t))


def samples_kernel(sample_ref, inv_ref, pick_ref, row_ref):
    tabs, slots, toks = pick_ref.shape
    width = sample_ref.shape[1]
    cap = width // tabs
    own = own_lines(sample_ref[...], slots)
    wanted = (iota((slots, toks), 1) + 1).astype(F32)
    for t in range(tabs):
        mine = of_table((width, toks), 0, t, 0, width, cap)
        pick_ref[t] = flag(dot(own, mine) == wanted)
        row = dot(of_table((8, width), 1, t, 0, width, cap), own, NT)[0:1]
        row_ref[t, :toks] = inv_ref[t]
        row_ref[t, toks:] = jnp.concatenate(
            [row[:, j : j + toks] for j in range(0, slots, toks)], axis=0
        )


def labels_kernel(label_ref, out_ref):
    dims = out_ref.shape
    row = label_ref[...].astype(F32)
    column = jnp.sum(
        jnp.where(iota(dims, 0) == iota(dims, 1), row, 0.0), axis=1, keepdims=True
    )
    out_ref[...] = jnp.broadcast_to(column, dims)


def halves_of(arrived, block_rows):
    shift = block_rows.bit_length() - 1
    return jnp.concatenate(
        [(arrived >> shift).astype(F32), (arrived & (block_rows - 1)).astype(F32)], axis=1
    )


def fetch_kernel(
    arrived_ref, expired_ref, emb_ref, out_ref,
    gone_ref, held_ref, table_ref, sent_ref, in_sem, out_sem,
):
    groups, width = arrived_ref.shape
    tabs, rows, emb = emb_ref.shape
    cap = width // tabs
    half = rows // 2
    loads = [pltpu.make_async_copy(expired_ref, gone_ref, in_sem.at[tabs])] + [
        pltpu.make_async_copy(emb_ref.at[t], held_ref.at[t], in_sem.at[t]) for t in range(tabs)
    ]
    for load in loads:
        load.start()
    arrived = arrived_ref[...]
    place = (arrived & (half - 1)) + 1
    signed = jnp.where(arrived < half, place, -place).astype(F32).T.astype(BF16)
    diag = iota((emb, emb), 0) == iota((emb, emb), 1)
    parts = out_sem.shape[0]
    part = groups // parts
    lane = (iota((cap, emb), 1) + 1).astype(F32)
    names = lane.astype(BF16), (lane + emb).astype(BF16)
    one, zero = jnp.ones((cap, emb), BF16), jnp.zeros((cap, emb), BF16)
    stores = []
    for c in range(parts):
        mine = slice(c * part, (c + 1) * part)
        for t in range(tabs):
            if c == 0:
                if t == 0:
                    loads[0].wait()
                loads[t + 1].wait()
                for j in range(0, rows, emb):
                    gone = gone_ref[t : t + 1, j : j + emb].astype(F32)
                    column = jnp.sum(jnp.where(diag, gone, 0.0), axis=1, keepdims=True)
                    to = j // half * emb
                    table_ref[t, j % half : j % half + emb, to : to + emb] = jnp.where(
                        column > 0.5, 0.0, held_ref[t, j : j + emb, :]
                    ).astype(BF16)
            lines = slice(t * cap, (t + 1) * cap)
            picks, first = [], []
            for o in range(c * part, (c + 1) * part):
                row = jnp.broadcast_to(signed[lines, o : o + 1], (cap, emb))
                at = jnp.abs(row)
                picks.append(
                    jnp.concatenate([jnp.where(at == n, one, zero) for n in names], axis=1)
                )
                first.append(row > zero)
            both = dot(jnp.concatenate(picks, axis=0), table_ref[t]).astype(BF16)
            line = jnp.where(jnp.concatenate(first, axis=0), both[:, :emb], both[:, emb:])
            sent_ref[mine, lines, :] = line.reshape(part, cap, emb)
        store = pltpu.make_async_copy(sent_ref.at[mine], out_ref.at[mine], out_sem.at[c])
        store.start()
        stores.append(store)
    for store in stores:
        store.wait()


def wanted_kernel(arrived_ref, row_ref):
    width = arrived_ref.shape[1]
    tabs, _, slots = row_ref.shape
    cap = width // tabs
    own = own_lines(halves_of(arrived_ref[...], 128), slots)
    for t in range(tabs):
        for kind in range(2):
            row_ref[t, 8 * kind : 8 * kind + 8, :] = dot(
                of_table((8, 2 * width), 1, t, kind, width, cap), own, NT
            )


def sublanes(length, wide):
    column = iota((length, 128), 0).astype(F32).astype(BF16)
    return jnp.concatenate([column] * (wide // 128), axis=1)


def down(row, length):
    return jnp.concatenate([row] * (length // 8), axis=0).astype(BF16)


def pool_kernel(rows_ref, sample_ref, out_ref):
    groups, width, emb = rows_ref.shape
    tabs, _, toks = sample_ref.shape
    cap = width // tabs
    slots = groups * cap
    one, zero = jnp.ones((toks, slots), BF16), jnp.zeros((toks, slots), BF16)
    samples = sublanes(toks, slots)
    for t in range(tabs):
        row = jnp.concatenate(
            [
                jnp.broadcast_to(sample_ref[t, j : j + 1, :] - 1.0, (16, toks))
                for j in range(toks, toks + slots // toks)
            ],
            axis=1,
        ).astype(BF16)
        pick = jnp.where(jnp.concatenate([row] * (toks // 16), axis=0) == samples, one, zero)
        pooled = dot(pick, rows_ref[:, t * cap : (t + 1) * cap, :].reshape(slots, emb))
        feature = (pooled * sample_ref[t, :toks]).astype(BF16)
        for k in range(out_ref.shape[0]):
            out_ref[k, :, t * emb : (t + 1) * emb] = feature


def silu_slope(preact):
    sig = jax.nn.sigmoid(preact)
    return sig * (1.0 + preact * (1.0 - sig))


def dense_kernel(
    at_ref, feat_ref, own_ref, near_ref, far_ref, u0, u1, u2, u3, labels_ref,
    logits_ref, grad_ref, mine_ref, other_ref,
):
    parts, toks, feats = feat_ref.shape
    units = (u0, u1, u2, u3)
    me, core = at_ref[0], at_ref[1]
    order = [(2 * core + q) % parts for q in range(parts)]
    preacts, scores = [], []
    for k, u in enumerate(units):
        pre = jnp.zeros((toks, u.shape[1]), F32)
        for q, at in enumerate(order):
            if k == 0:
                w = own_ref[pl.ds(pl.multiple_of(at * feats, feats), feats), :]
            else:
                half = near_ref if q < parts // 2 else far_ref
                start = q % (parts // 2) * feats
                w = half[k - 1, start : start + feats, :]
            pre = pre + dot(feat_ref[at], w)
        hidden = jax.nn.silu(pre).astype(BF16).astype(F32)
        preacts.append(pre)
        scores.append(jnp.sum(hidden * u[...], axis=1, keepdims=True))
    logits = jnp.zeros((toks, 1), F32)
    for shard in range(parts):
        far = (me + parts - shard) % parts
        score = scores[0]
        for k in range(1, parts):
            score = jnp.where(far == k, scores[k], score)
        logits = logits + score
    dlogit = (jax.nn.sigmoid(logits) - labels_ref[...])[:, 0:1]
    logits_ref[...] = jnp.broadcast_to(logits, logits_ref.shape)
    grads = jnp.zeros((toks, feats), F32)
    for k, (u, pre) in enumerate(zip(units, preacts)):
        dhidden = (dlogit * u[...] * silu_slope(pre)).astype(BF16)
        if k == 0:
            half = dhidden.shape[1] // 2
            low, high = dhidden[:, :half], dhidden[:, half:]
            mine, other = jnp.where(core == 0, low, high), jnp.where(core == 0, high, low)
            for q in range(parts):
                lines = slice(q * feats, (q + 1) * feats)
                part = dot(
                    feat_ref[q],
                    jnp.concatenate([mine, other], axis=1),
                    (((0,), (0,)), ((), ())),
                ).astype(BF16)
                mine_ref[lines, :] = part[:, :half]
                other_ref[lines, :] = part[:, half:]
            w = own_ref[pl.ds(pl.multiple_of(me * feats, feats), feats), :]
        else:
            lines = pl.ds(pl.multiple_of(me % (parts // 2) * feats, feats), feats)
            w = jnp.where(
                me // (parts // 2) == core, near_ref[k - 1, lines, :], far_ref[k - 1, lines, :]
            )
        grads = grads + dot(dhidden, w, NT)
    grad_ref[...] = grads


def spread_kernel(grad_ref, inv_ref, pick_ref, out_ref):
    slots = pick_ref.shape[1]
    cap, emb = out_ref.shape[1:]
    grad = (inv_ref[0] * grad_ref[...]).astype(BF16)
    out_ref[...] = dot(pick_ref[0], grad).astype(BF16).reshape(slots // cap, cap, emb)


def update_kernel(grads_ref, wanted_ref, emb_ref, expired_ref, acc_ref, new_ref, new_acc_ref):
    groups, cap, emb = grads_ref.shape
    rows = emb_ref.shape[1]
    slots = groups * cap
    t = pl.program_id(0)
    grads = grads_ref[...].reshape(slots, emb)
    at = down(wanted_ref[0, 0:8, :], 16)
    low = down(wanted_ref[0, 8:16, :], 16)
    low = jnp.concatenate([low] * (emb // 16), axis=0)
    one, zero = jnp.ones((emb, slots), BF16), jnp.zeros((emb, slots), BF16)
    hot = jnp.where(low == sublanes(emb, slots), one, zero)
    gone = expired_ref[pl.ds(t, 1), :]
    fresh_acc = jnp.where(gone == 1, ACC_RESET, acc_ref[pl.ds(t, 1), :])
    kept = jnp.where(gone == 1, 0.0, 1.0)
    diag = iota((emb, emb), 0) == iota((emb, emb), 1)
    for j in range(0, rows, emb):
        here = jnp.concatenate([at == jnp.full_like(at, j // emb)] * (emb // 16), axis=0)
        summed = dot(jnp.where(here, hot, zero), grads)
        cols = slice(j, j + emb)
        old = jnp.sum(jnp.where(diag, fresh_acc[:, cols], 0.0), axis=1, keepdims=True)
        keep = jnp.sum(jnp.where(diag, kept[:, cols], 0.0), axis=1, keepdims=True)
        acc = old + jnp.sum(summed * summed, axis=1, keepdims=True) * (1.0 / emb)
        fresh = jnp.where(keep > 0.5, emb_ref[0, j : j + emb, :], 0.0)
        new_ref[0, j : j + emb, :] = fresh - LEARN_RATE * summed / jnp.sqrt(acc)
        line = jnp.sum(jnp.where(diag, acc, 0.0), axis=0, keepdims=True)
        for table in range(acc_ref.shape[0]):

            @pl.when(t == table)
            def _(table=table, cols=cols, line=line):
                new_acc_ref[table : table + 1, cols] = line


def shape(dims, dtype):
    return jax.ShapeDtypeStruct(dims, dtype)


def block(dims, index=None):
    if index is None:
        return pl.BlockSpec(dims, lambda *_: (0,) * len(dims))
    return pl.BlockSpec(dims, index)


def params(mib):
    return pltpu.CompilerParams(vmem_limit_bytes=mib << 20)


def cost(flops):
    return pl.CostEstimate(flops=flops, bytes_accessed=1 << 20, transcendentals=0)


def a2a(value, axis):
    return lax.all_to_all(value, axis, split_axis=0, concat_axis=0, tiled=True)


def from_everyone(value, axis):
    size = lax.axis_size(axis)
    return a2a(jnp.broadcast_to(value[None], (size, *value.shape)), axis)


def ring(value, axis, step):
    size = lax.axis_size(axis)
    return lax.ppermute(value, axis, [(i, (i + step) % size) for i in range(size)])


def shards(
    bag_lengths, owners, row_slots, admit_mask, expired, embeddings, accumulator,
    hidden_weight, output_weight, labels,
):
    groups = lax.axis_size(DP)
    parts = lax.axis_size("mp")
    tabs, toks, bag = row_slots.shape
    rows, emb = embeddings.shape[1:]
    cap = 2 * toks * bag // groups
    width = tabs * cap
    slots = groups * cap
    feats = tabs * emb
    core = lax.axis_index(NEAR).astype(I32)
    place = jnp.stack([lax.axis_index("mp").astype(I32), core])

    request, sample, inv = pl.pallas_call(
        slots_kernel,
        out_shape=(
            shape((groups, width), I32),
            shape((groups, width), F32),
            shape((tabs, toks, toks), F32),
        ),
        compiler_params=params(24),
        name="slots",
    )(
        *map(
            functools.partial(pltpu.with_memory_space_constraint, memory_space=pltpu.HBM),
            (
                bag_lengths,
                owners[..., 0].swapaxes(1, 2),
                row_slots.swapaxes(1, 2),
                admit_mask.swapaxes(1, 2),
            ),
        )
    )
    arrived = a2a(request, DP)
    lines, units_dev = hidden_weight.shape
    weight, _ = lax.optimization_barrier((hidden_weight, request))
    mine = lax.dynamic_slice(weight, (core * (lines // 2), 0), (lines // 2, units_dev))
    near_weights = jnp.stack([ring(mine, "mp", k) for k in range(1, parts)])
    far_weights = ring(near_weights, NEAR, 1)
    pick, sample_row = pl.pallas_call(
        samples_kernel,
        out_shape=(
            pltpu.HBM((tabs, slots, toks), BF16),
            shape((tabs, toks + slots // toks, toks), F32),
        ),
        compiler_params=params(24),
        cost_estimate=cost(4 << 30),
        name="samples",
    )(sample, inv)
    held = functools.partial(pltpu.with_memory_space_constraint, memory_space=pltpu.HBM)
    smem, vmem, hbm = (
        pl.BlockSpec(memory_space=space) for space in (pltpu.SMEM, pltpu.VMEM, pltpu.HBM)
    )
    dma = pltpu.SemaphoreType.DMA
    fetched = pl.pallas_call(
        fetch_kernel,
        in_specs=[vmem, hbm, hbm],
        out_specs=hbm,
        out_shape=pltpu.HBM((groups, width, emb), BF16),
        scratch_shapes=[
            pltpu.VMEM((tabs, rows), I32),
            pltpu.VMEM((tabs, rows, emb), F32),
            pltpu.VMEM((tabs, rows // 2, 2 * emb), BF16),
            pltpu.VMEM((groups, width, emb), BF16),
            dma((tabs + 1,)),
            dma((8,)),
        ],
        compiler_params=params(24),
        name="fetch",
    )(arrived, held(expired), held(embeddings))
    returned = a2a(fetched, DP)
    unit, later = lax.optimization_barrier((output_weight, arrived))
    unit = unit.reshape(1, -1)
    units = [unit] + [ring(unit, "mp", k) for k in range(1, parts)]
    wanted = pl.pallas_call(
        wanted_kernel,
        out_shape=pltpu.HBM((tabs, 16, slots), F32),
        compiler_params=params(24),
        cost_estimate=cost(4 << 30),
        name="wanted",
    )(later)
    features = pl.pallas_call(
        pool_kernel,
        out_shape=shape((parts, toks, feats), BF16),
        compiler_params=params(24),
        name="pool",
    )(returned, sample_row)
    features, place, near_weights, far_weights, units = lax.optimization_barrier(
        (features, place, near_weights, far_weights, units)
    )
    portion = a2a(features, "mp")
    label_column = pl.pallas_call(
        labels_kernel,
        out_shape=shape((toks, toks), F32),
        compiler_params=params(4),
        name="labels",
    )(labels.reshape(1, toks))
    half = units_dev // 2
    logits, grad, mine, other = pl.pallas_call(
        dense_kernel,
        in_specs=[smem] + [vmem] * (parts + 5),
        out_shape=(
            shape((toks, toks), F32),
            shape((toks, feats), F32),
            shape((lines, half), BF16),
            shape((lines, half), BF16),
        ),
        compiler_params=params(24),
        name="dense",
    )(place, portion, hidden_weight, near_weights, far_weights, *units, label_column)
    joined = ring(other, NEAR, 1)
    share = lines // groups
    outgoing = pl.pallas_call(
        spread_kernel,
        grid=(tabs,),
        in_specs=[
            block((toks, emb), lambda t: (0, t)),
            block((1, toks, toks), lambda t: (t, 0, 0)),
            block((1, slots, toks), lambda t: (t, 0, 0)),
        ],
        out_specs=block((groups, cap, emb), lambda t: (0, t, 0)),
        out_shape=shape((groups, width + share, emb), BF16),
        compiler_params=params(24),
        cost_estimate=cost(4 << 30),
        name="spread",
    )(grad, inv, pick)
    pair = (mine.astype(F32) + joined.astype(F32)).astype(BF16)
    pair = pair.reshape(2, groups // 2, share, half).swapaxes(0, 1)
    outgoing = lax.dynamic_update_slice(
        outgoing, pair.reshape(groups, share, half), (0, width, 0)
    )
    gradients = a2a(outgoing, DP)
    shares = gradients[:, width:].reshape(groups // 2, 2, 2, share // 2, half)
    own = shares.astype(F32).sum(axis=0).astype(BF16).swapaxes(0, 1)
    near = from_everyone(own, FAR)
    near = near.transpose(0, 1, 3, 2, 4).reshape(lines // 2, units_dev)
    far = ring(near, NEAR, 1)
    weight_grad = jnp.concatenate(
        [jnp.where(core == 0, near, far), jnp.where(core == 0, far, near)]
    )
    new_rows, new_acc = pl.pallas_call(
        update_kernel,
        grid=(tabs,),
        in_specs=[
            block((groups, cap, emb), lambda t: (0, t, 0)),
            block((1, 16, slots), lambda t: (t, 0, 0)),
            block((1, rows, emb), lambda t: (t, 0, 0)),
            block((tabs, rows)),
            block((tabs, rows)),
        ],
        out_specs=(
            block((1, rows, emb), lambda t: (t, 0, 0)),
            block((tabs, rows)),
        ),
        out_shape=(shape(embeddings.shape, F32), shape(accumulator.shape, F32)),
        compiler_params=params(24),
        cost_estimate=cost(4 << 30),
        name="update",
    )(gradients, held(wanted), held(embeddings), expired, accumulator)
    return (new_rows, new_acc, weight_grad, logits[:, 0])


def solution(mesh):
    split = Mesh(mesh.devices.reshape(8, 8, 2, mesh.shape["mp"]), (*DP, "mp"))

    return jax.shard_map(
        shards,
        mesh=split,
        in_specs=(
            P("mp", DP),
            P("mp", DP, None, None),
            P("mp", DP, None),
            P("mp", DP, None),
            P("mp", DP),
            P("mp", DP, None),
            P("mp", DP),
            P(None, "mp"),
            P("mp"),
            P(DP),
        ),
        out_specs=(P("mp", DP, None), P("mp", DP), P(None, "mp"), P(DP)),
        check_vma=False,
    )
```

```python
import functools

import jax
import jax.numpy as jnp
from jax import lax
from jax.experimental import pallas as pl
from jax.experimental.pallas import tpu as pltpu
from jax.sharding import Mesh
from jax.sharding import PartitionSpec as P

DP = ("dp_0", "dp_1", "dp_2")
FAR = ("dp_0", "dp_1")
NEAR = "dp_2"

LEARN_RATE = 0.05
ACC_RESET = 0.001
F32, BF16, I32 = jnp.float32, jnp.bfloat16, jnp.int32
NT = (((1,), (1,)), ((), ()))


def iota(shape, dim):
    return lax.broadcasted_iota(I32, shape, dim)


def dot(a, b, dims=(((1,), (0,)), ((), ()))):
    return lax.dot_general(a, b, dims, preferred_element_type=F32)


def flag(cond):
    return jnp.where(cond, 1.0, 0.0).astype(BF16)


def slots_kernel(len_ref, own_ref, slot_ref, adm_ref, req_ref, sample_ref, inv_ref):
    tabs, bag, toks = own_ref.shape
    groups, width = req_ref.shape
    cap = width // tabs
    square = (toks, toks)
    tri = jnp.concatenate(
        [flag(iota(square, 0) < iota(square, 1)), jnp.ones(square, BF16)], axis=1
    )
    rank_row = iota((cap, toks), 0).astype(F32)
    sample_no = (iota((1, toks), 1) + 1).astype(F32)
    name = iota((groups, toks), 0).astype(F32).astype(BF16)
    one, zero = jnp.ones((groups, toks), BF16), jnp.zeros((groups, toks), BF16)
    hot, counts = [], []
    for t in range(tabs):
        owner = own_ref[t].astype(F32)
        rows = [jnp.broadcast_to(owner[p : p + 1], (groups, toks)) for p in range(bag)]
        hot.append([jnp.where(name == row.astype(BF16), one, zero) for row in rows])
        counts.append(dot(jnp.concatenate(hot[t], axis=0), tri))
    for t in range(tabs):
        base = jnp.zeros((groups, toks), F32)
        live_count = jnp.zeros((1, toks), F32)
        values = []
        for p in range(bag):
            part = counts[t][p * groups : (p + 1) * groups]
            before = part[:, :toks] + base
            rank = jnp.sum(hot[t][p].astype(F32) * before, axis=0, keepdims=True)
            base = base + part[:, toks:]
            live = (p < len_ref[t : t + 1, :]) & (adm_ref[t, p : p + 1, :] == 1)
            live_count = live_count + jnp.where(live, 1.0, 0.0)
            slot = slot_ref[t, p : p + 1, :]
            here = rank_row == rank
            values.append(
                jnp.concatenate(
                    [
                        jnp.where(here, (slot >> 4).astype(F32), 0.0),
                        jnp.where(here, (slot & 15).astype(F32), 0.0),
                        jnp.where(here & live, sample_no, 0.0),
                    ],
                    axis=0,
                ).astype(BF16)
            )
        found = dot(jnp.concatenate(hot[t], axis=1), jnp.concatenate(values, axis=1), NT)
        cols = slice(t * cap, (t + 1) * cap)
        req_ref[:, cols] = (16.0 * found[:, :cap] + found[:, cap : 2 * cap]).astype(I32)
        sample_ref[:, cols] = found[:, 2 * cap :]
        inv = 1.0 / jnp.maximum(live_count, 1.0)
        column = jnp.sum(
            jnp.where(iota(square, 0) == iota(square, 1), inv, 0.0), axis=1, keepdims=True
        )
        inv_ref[t] = jnp.broadcast_to(column, square)


def own_lines(table, slots):
    groups, lanes = table.shape
    cap = slots // groups
    mine = iota((cap, lanes), 1) % cap == iota((cap, lanes), 0)
    return jnp.concatenate(
        [
            jnp.where(mine, jnp.broadcast_to(table[o : o + 1], (cap, lanes)), 0.0)
            for o in range(groups)
        ],
        axis=0,
    ).astype(BF16)


def of_table(shape, lane_dim, t, kind, width, cap):
    lane = iota(shape, lane_dim)
    return flag((lane // width == kind) & (lane % width // cap == t))


def samples_kernel(sample_ref, pick_ref, row_ref):
    tabs, slots, toks = pick_ref.shape
    width = sample_ref.shape[1]
    cap = width // tabs
    own = own_lines(sample_ref[...], slots)
    wanted = (iota((slots, toks), 1) + 1).astype(F32)
    for t in range(tabs):
        mine = of_table((width, toks), 0, t, 0, width, cap)
        pick_ref[t] = flag(dot(own, mine) == wanted)
        row = dot(of_table((8, width), 1, t, 0, width, cap), own, NT)
        row_ref[t : t + 1, :] = row[0:1]


def labels_kernel(label_ref, out_ref):
    dims = out_ref.shape
    row = label_ref[...].astype(F32)
    column = jnp.sum(
        jnp.where(iota(dims, 0) == iota(dims, 1), row, 0.0), axis=1, keepdims=True
    )
    out_ref[...] = jnp.broadcast_to(column, dims)


def halves_of(arrived, block_rows):
    shift = block_rows.bit_length() - 1
    return jnp.concatenate(
        [(arrived >> shift).astype(F32), (arrived & (block_rows - 1)).astype(F32)], axis=1
    )


def fetch_kernel(
    arrived_ref, expired_ref, emb_ref, out_ref,
    gone_ref, held_ref, table_ref, sent_ref, in_sem, out_sem,
):
    groups, width = arrived_ref.shape
    tabs, rows, emb = emb_ref.shape
    cap = width // tabs
    half = rows // 2
    loads = [pltpu.make_async_copy(expired_ref, gone_ref, in_sem.at[tabs])] + [
        pltpu.make_async_copy(emb_ref.at[t], held_ref.at[t], in_sem.at[t]) for t in range(tabs)
    ]
    for load in loads:
        load.start()
    arrived = arrived_ref[...]
    place = (arrived & (half - 1)) + 1
    signed = jnp.where(arrived < half, place, -place).astype(F32).T.astype(BF16)
    parts = out_sem.shape[0]
    part = groups // parts
    lane = (iota((cap, emb), 1) + 1).astype(F32)
    names = lane.astype(BF16), (lane + emb).astype(BF16)
    one, zero = jnp.ones((cap, emb), BF16), jnp.zeros((cap, emb), BF16)
    stores = []
    for c in range(parts):
        mine = slice(c * part, (c + 1) * part)
        for t in range(tabs):
            if c == 0:
                if t == 0:
                    loads[0].wait()
                    gone = gone_ref[...].astype(F32).T.astype(BF16)
                loads[t + 1].wait()
                for at in range(2):
                    table = held_ref[t, at * half : (at + 1) * half, :].astype(BF16)
                    lost = jnp.broadcast_to(gone[at * half : (at + 1) * half, t : t + 1], table.shape)
                    table_ref[t, :, at * emb : (at + 1) * emb] = jnp.where(
                        lost == jnp.zeros_like(lost), table, jnp.zeros_like(table)
                    )
            lines = slice(t * cap, (t + 1) * cap)
            picks, first = [], []
            for o in range(c * part, (c + 1) * part):
                row = jnp.broadcast_to(signed[lines, o : o + 1], (cap, emb))
                at = jnp.abs(row)
                picks.append(
                    jnp.concatenate([jnp.where(at == n, one, zero) for n in names], axis=1)
                )
                first.append(row > zero)
            both = dot(jnp.concatenate(picks, axis=0), table_ref[t]).astype(BF16)
            line = jnp.where(jnp.concatenate(first, axis=0), both[:, :emb], both[:, emb:])
            sent_ref[mine, lines, :] = line.reshape(part, cap, emb)
        store = pltpu.make_async_copy(sent_ref.at[mine], out_ref.at[mine], out_sem.at[c])
        store.start()
        stores.append(store)
    for store in stores:
        store.wait()


def wanted_kernel(arrived_ref, row_ref):
    width = arrived_ref.shape[1]
    tabs, _, slots = row_ref.shape
    cap = width // tabs
    own = own_lines(halves_of(arrived_ref[...], 128), slots)
    for t in range(tabs):
        for kind in range(2):
            row_ref[t, 8 * kind : 8 * kind + 8, :] = dot(
                of_table((8, 2 * width), 1, t, kind, width, cap), own, NT
            )


def sublanes(length, wide):
    column = iota((length, 128), 0).astype(F32).astype(BF16)
    return jnp.concatenate([column] * (wide // 128), axis=1)


def down(row, length):
    return jnp.concatenate([row] * (length // 8), axis=0).astype(BF16)


def pool_kernel(rows_ref, sample_ref, inv_ref, out_ref):
    groups, width, emb = rows_ref.shape
    tabs, toks, _ = inv_ref.shape
    cap = width // tabs
    slots = groups * cap
    one, zero = jnp.ones((toks, slots), BF16), jnp.zeros((toks, slots), BF16)
    samples = sublanes(toks, slots)
    for t in range(tabs):
        row = jnp.broadcast_to(sample_ref[t : t + 1, :] - 1.0, (16, slots)).astype(BF16)
        pick = jnp.where(jnp.concatenate([row] * (toks // 16), axis=0) == samples, one, zero)
        pooled = dot(pick, rows_ref[:, t * cap : (t + 1) * cap, :].reshape(slots, emb))
        feature = (pooled * inv_ref[t]).astype(BF16)
        for k in range(out_ref.shape[0]):
            out_ref[k, :, t * emb : (t + 1) * emb] = feature


def silu_slope(preact):
    sig = jax.nn.sigmoid(preact)
    return sig * (1.0 + preact * (1.0 - sig))


def dense_kernel(
    at_ref, feat_ref, own_ref, near_ref, far_ref, u0, u1, u2, u3, labels_ref,
    logits_ref, grad_ref, mine_ref, other_ref,
):
    parts, toks, feats = feat_ref.shape
    units = (u0, u1, u2, u3)
    me, core = at_ref[0], at_ref[1]
    order = [(2 * core + q) % parts for q in range(parts)]
    preacts, scores = [], []
    for k, u in enumerate(units):
        pre = jnp.zeros((toks, u.shape[1]), F32)
        for q, at in enumerate(order):
            if k == 0:
                w = own_ref[pl.ds(pl.multiple_of(at * feats, feats), feats), :]
            else:
                half = near_ref if q < parts // 2 else far_ref
                start = q % (parts // 2) * feats
                w = half[k - 1, start : start + feats, :]
            pre = pre + dot(feat_ref[at], w)
        hidden = jax.nn.silu(pre).astype(BF16).astype(F32)
        preacts.append(pre)
        scores.append(jnp.sum(hidden * u[...], axis=1, keepdims=True))
    logits = jnp.zeros((toks, 1), F32)
    for shard in range(parts):
        far = (me + parts - shard) % parts
        score = scores[0]
        for k in range(1, parts):
            score = jnp.where(far == k, scores[k], score)
        logits = logits + score
    dlogit = (jax.nn.sigmoid(logits) - labels_ref[...])[:, 0:1]
    logits_ref[...] = jnp.broadcast_to(logits, logits_ref.shape)
    grads = jnp.zeros((toks, feats), F32)
    for k, (u, pre) in enumerate(zip(units, preacts)):
        dhidden = (dlogit * u[...] * silu_slope(pre)).astype(BF16)
        if k == 0:
            half = dhidden.shape[1] // 2
            low, high = dhidden[:, :half], dhidden[:, half:]
            mine, other = jnp.where(core == 0, low, high), jnp.where(core == 0, high, low)
            for q in range(parts):
                lines = slice(q * feats, (q + 1) * feats)
                part = dot(
                    feat_ref[q],
                    jnp.concatenate([mine, other], axis=1),
                    (((0,), (0,)), ((), ())),
                ).astype(BF16)
                mine_ref[lines, :] = part[:, :half]
                other_ref[lines, :] = part[:, half:]
            w = own_ref[pl.ds(pl.multiple_of(me * feats, feats), feats), :]
        else:
            lines = pl.ds(pl.multiple_of(me % (parts // 2) * feats, feats), feats)
            w = jnp.where(
                me // (parts // 2) == core, near_ref[k - 1, lines, :], far_ref[k - 1, lines, :]
            )
        grads = grads + dot(dhidden, w, NT)
    grad_ref[...] = grads


def spread_kernel(grad_ref, inv_ref, pick_ref, out_ref):
    slots = pick_ref.shape[1]
    cap, emb = out_ref.shape[1:]
    grad = (inv_ref[0] * grad_ref[...]).astype(BF16)
    out_ref[...] = dot(pick_ref[0], grad).astype(BF16).reshape(slots // cap, cap, emb)


def update_kernel(grads_ref, wanted_ref, emb_ref, expired_ref, acc_ref, new_ref, new_acc_ref):
    groups, cap, emb = grads_ref.shape
    rows = emb_ref.shape[1]
    slots = groups * cap
    t = pl.program_id(0)
    grads = grads_ref[...].reshape(slots, emb)
    at = down(wanted_ref[0, 0:8, :], 16)
    low = down(wanted_ref[0, 8:16, :], 16)
    low = jnp.concatenate([low] * (emb // 16), axis=0)
    one, zero = jnp.ones((emb, slots), BF16), jnp.zeros((emb, slots), BF16)
    hot = jnp.where(low == sublanes(emb, slots), one, zero)
    gone = expired_ref[pl.ds(t, 1), :]
    fresh_acc = jnp.where(gone == 1, ACC_RESET, acc_ref[pl.ds(t, 1), :])
    kept = jnp.where(gone == 1, 0.0, 1.0)
    diag = iota((emb, emb), 0) == iota((emb, emb), 1)
    for j in range(0, rows, emb):
        here = jnp.concatenate([at == jnp.full_like(at, j // emb)] * (emb // 16), axis=0)
        summed = dot(jnp.where(here, hot, zero), grads)
        cols = slice(j, j + emb)
        old = jnp.sum(jnp.where(diag, fresh_acc[:, cols], 0.0), axis=1, keepdims=True)
        keep = jnp.sum(jnp.where(diag, kept[:, cols], 0.0), axis=1, keepdims=True)
        acc = old + jnp.sum(summed * summed, axis=1, keepdims=True) * (1.0 / emb)
        fresh = jnp.where(keep > 0.5, emb_ref[0, j : j + emb, :], 0.0)
        new_ref[0, j : j + emb, :] = fresh - LEARN_RATE * summed / jnp.sqrt(acc)
        line = jnp.sum(jnp.where(diag, acc, 0.0), axis=0, keepdims=True)
        for table in range(acc_ref.shape[0]):

            @pl.when(t == table)
            def _(table=table, cols=cols, line=line):
                new_acc_ref[table : table + 1, cols] = line


def shape(dims, dtype):
    return jax.ShapeDtypeStruct(dims, dtype)


def block(dims, index=None):
    if index is None:
        return pl.BlockSpec(dims, lambda *_: (0,) * len(dims))
    return pl.BlockSpec(dims, index)


def params(mib):
    return pltpu.CompilerParams(vmem_limit_bytes=mib << 20)


def cost(flops):
    return pl.CostEstimate(flops=flops, bytes_accessed=1 << 20, transcendentals=0)


def a2a(value, axis):
    return lax.all_to_all(value, axis, split_axis=0, concat_axis=0, tiled=True)


def from_everyone(value, axis):
    size = lax.axis_size(axis)
    return a2a(jnp.broadcast_to(value[None], (size, *value.shape)), axis)


def ring(value, axis, step):
    size = lax.axis_size(axis)
    return lax.ppermute(value, axis, [(i, (i + step) % size) for i in range(size)])


def shards(
    bag_lengths, owners, row_slots, admit_mask, expired, embeddings, accumulator,
    hidden_weight, output_weight, labels,
):
    groups = lax.axis_size(DP)
    parts = lax.axis_size("mp")
    tabs, toks, bag = row_slots.shape
    rows, emb = embeddings.shape[1:]
    cap = 2 * toks * bag // groups
    width = tabs * cap
    slots = groups * cap
    feats = tabs * emb
    core = lax.axis_index(NEAR).astype(I32)
    place = jnp.stack([lax.axis_index("mp").astype(I32), core])

    request, sample, inv = pl.pallas_call(
        slots_kernel,
        out_shape=(
            shape((groups, width), I32),
            shape((groups, width), F32),
            shape((tabs, toks, toks), F32),
        ),
        compiler_params=params(24),
        name="slots",
    )(
        *map(
            functools.partial(pltpu.with_memory_space_constraint, memory_space=pltpu.HBM),
            (
                bag_lengths,
                owners[..., 0].swapaxes(1, 2),
                row_slots.swapaxes(1, 2),
                admit_mask.swapaxes(1, 2),
            ),
        )
    )
    arrived = a2a(request, DP)
    lines, units_dev = hidden_weight.shape
    weight, _ = lax.optimization_barrier((hidden_weight, request))
    mine = lax.dynamic_slice(weight, (core * (lines // 2), 0), (lines // 2, units_dev))
    near_weights = jnp.stack([ring(mine, "mp", k) for k in range(1, parts)])
    far_weights = ring(near_weights, NEAR, 1)
    pick, sample_row = pl.pallas_call(
        samples_kernel,
        out_shape=(
            pltpu.HBM((tabs, slots, toks), BF16),
            shape((tabs, slots), F32),
        ),
        compiler_params=params(24),
        cost_estimate=cost(4 << 30),
        name="samples",
    )(sample)
    held = functools.partial(pltpu.with_memory_space_constraint, memory_space=pltpu.HBM)
    smem, vmem, hbm = (
        pl.BlockSpec(memory_space=space) for space in (pltpu.SMEM, pltpu.VMEM, pltpu.HBM)
    )
    dma = pltpu.SemaphoreType.DMA
    fetched = pl.pallas_call(
        fetch_kernel,
        in_specs=[vmem, hbm, hbm],
        out_specs=hbm,
        out_shape=pltpu.HBM((groups, width, emb), BF16),
        scratch_shapes=[
            pltpu.VMEM((tabs, rows), I32),
            pltpu.VMEM((tabs, rows, emb), F32),
            pltpu.VMEM((tabs, rows // 2, 2 * emb), BF16),
            pltpu.VMEM((groups, width, emb), BF16),
            dma((tabs + 1,)),
            dma((8,)),
        ],
        compiler_params=params(24),
        name="fetch",
    )(arrived, held(expired), held(embeddings))
    returned = a2a(fetched, DP)
    unit, later = lax.optimization_barrier((output_weight, arrived))
    unit = unit.reshape(1, -1)
    units = [unit] + [ring(unit, "mp", k) for k in range(1, parts)]
    wanted = pl.pallas_call(
        wanted_kernel,
        out_shape=pltpu.HBM((tabs, 16, slots), F32),
        compiler_params=params(24),
        cost_estimate=cost(4 << 30),
        name="wanted",
    )(later)
    features = pl.pallas_call(
        pool_kernel,
        out_shape=shape((parts, toks, feats), BF16),
        compiler_params=params(24),
        name="pool",
    )(returned, sample_row, inv)
    features, place, near_weights, far_weights, units = lax.optimization_barrier(
        (features, place, near_weights, far_weights, units)
    )
    portion = a2a(features, "mp")
    label_column = pl.pallas_call(
        labels_kernel,
        out_shape=shape((toks, toks), F32),
        compiler_params=params(4),
        name="labels",
    )(labels.reshape(1, toks))
    half = units_dev // 2
    logits, grad, mine, other = pl.pallas_call(
        dense_kernel,
        in_specs=[smem] + [vmem] * (parts + 5),
        out_shape=(
            shape((toks, toks), F32),
            shape((toks, feats), F32),
            shape((lines, half), BF16),
            shape((lines, half), BF16),
        ),
        compiler_params=params(24),
        name="dense",
    )(place, portion, held(hidden_weight), near_weights, far_weights, *units, label_column)
    joined = ring(other, NEAR, 1)
    share = lines // groups
    outgoing = pl.pallas_call(
        spread_kernel,
        grid=(tabs,),
        in_specs=[
            block((toks, emb), lambda t: (0, t)),
            block((1, toks, toks), lambda t: (t, 0, 0)),
            block((1, slots, toks), lambda t: (t, 0, 0)),
        ],
        out_specs=block((groups, cap, emb), lambda t: (0, t, 0)),
        out_shape=shape((groups, width + share, emb), BF16),
        compiler_params=params(24),
        cost_estimate=cost(4 << 30),
        name="spread",
    )(grad, inv, pick)
    pair = (mine.astype(F32) + joined.astype(F32)).astype(BF16)
    pair = pair.reshape(2, groups // 2, share, half).swapaxes(0, 1)
    outgoing = lax.dynamic_update_slice(
        outgoing, pair.reshape(groups, share, half), (0, width, 0)
    )
    gradients = a2a(outgoing, DP)
    shares = gradients[:, width:].reshape(groups // 2, 2, 2, share // 2, half)
    own = shares.astype(F32).sum(axis=0).astype(BF16).swapaxes(0, 1)
    near = from_everyone(own, FAR)
    near = near.transpose(0, 1, 3, 2, 4).reshape(lines // 2, units_dev)
    far = ring(near, NEAR, 1)
    weight_grad = jnp.concatenate(
        [jnp.where(core == 0, near, far), jnp.where(core == 0, far, near)]
    )
    new_rows, new_acc = pl.pallas_call(
        update_kernel,
        grid=(tabs,),
        in_specs=[
            block((groups, cap, emb), lambda t: (0, t, 0)),
            block((1, 16, slots), lambda t: (t, 0, 0)),
            block((1, rows, emb), lambda t: (t, 0, 0)),
            block((tabs, rows)),
            block((tabs, rows)),
        ],
        out_specs=(
            block((1, rows, emb), lambda t: (t, 0, 0)),
            block((tabs, rows)),
        ),
        out_shape=(shape(embeddings.shape, F32), shape(accumulator.shape, F32)),
        compiler_params=params(24),
        cost_estimate=cost(4 << 30),
        name="update",
    )(gradients, held(wanted), held(embeddings), expired, accumulator)
    return (new_rows, new_acc, weight_grad, logits[:, 0])


def solution(mesh):
    split = Mesh(mesh.devices.reshape(8, 8, 2, mesh.shape["mp"]), (*DP, "mp"))

    return jax.shard_map(
        shards,
        mesh=split,
        in_specs=(
            P("mp", DP),
            P("mp", DP, None, None),
            P("mp", DP, None),
            P("mp", DP, None),
            P("mp", DP),
            P("mp", DP, None),
            P("mp", DP),
            P(None, "mp"),
            P("mp"),
            P(DP),
        ),
        out_specs=(P("mp", DP, None), P("mp", DP), P(None, "mp"), P(DP)),
        check_vma=False,
    )
```

```python
import functools

import jax
import jax.numpy as jnp
from jax import lax
from jax.experimental import pallas as pl
from jax.experimental.pallas import tpu as pltpu
from jax.sharding import Mesh
from jax.sharding import PartitionSpec as P

DP = ("dp_0", "dp_1", "dp_2")
FAR = ("dp_0", "dp_1")
NEAR = "dp_2"

LEARN_RATE = 0.05
ACC_RESET = 0.001
F32, BF16, I32 = jnp.float32, jnp.bfloat16, jnp.int32
NT = (((1,), (1,)), ((), ()))


def iota(shape, dim):
    return lax.broadcasted_iota(I32, shape, dim)


def dot(a, b, dims=(((1,), (0,)), ((), ()))):
    return lax.dot_general(a, b, dims, preferred_element_type=F32)


def flag(cond):
    return jnp.where(cond, 1.0, 0.0).astype(BF16)


def slots_kernel(len_ref, own_ref, slot_ref, adm_ref, req_ref, sample_ref, inv_ref):
    tabs, bag, toks = own_ref.shape
    groups, width = req_ref.shape
    cap = width // tabs
    square = (toks, toks)
    tri = jnp.concatenate(
        [flag(iota(square, 0) < iota(square, 1)), jnp.ones(square, BF16)], axis=1
    )
    rank_row = iota((cap, toks), 0).astype(F32)
    sample_no = (iota((1, toks), 1) + 1).astype(F32)
    name = iota((groups, toks), 0).astype(F32).astype(BF16)
    one, zero = jnp.ones((groups, toks), BF16), jnp.zeros((groups, toks), BF16)
    hot, counts = [], []
    for t in range(tabs):
        owner = own_ref[t].astype(F32)
        rows = [jnp.broadcast_to(owner[p : p + 1], (groups, toks)) for p in range(bag)]
        hot.append([jnp.where(name == row.astype(BF16), one, zero) for row in rows])
        counts.append(dot(jnp.concatenate(hot[t], axis=0), tri))
    for t in range(tabs):
        base = jnp.zeros((groups, toks), F32)
        live_count = jnp.zeros((1, toks), F32)
        values = []
        for p in range(bag):
            part = counts[t][p * groups : (p + 1) * groups]
            before = part[:, :toks] + base
            rank = jnp.sum(hot[t][p].astype(F32) * before, axis=0, keepdims=True)
            base = base + part[:, toks:]
            live = (p < len_ref[t : t + 1, :]) & (adm_ref[t, p : p + 1, :] == 1)
            live_count = live_count + jnp.where(live, 1.0, 0.0)
            slot = slot_ref[t, p : p + 1, :]
            here = rank_row == rank
            values.append(
                jnp.concatenate(
                    [
                        jnp.where(here, (slot >> 4).astype(F32), 0.0),
                        jnp.where(here, (slot & 15).astype(F32), 0.0),
                        jnp.where(here & live, sample_no, 0.0),
                    ],
                    axis=0,
                ).astype(BF16)
            )
        found = dot(jnp.concatenate(hot[t], axis=1), jnp.concatenate(values, axis=1), NT)
        cols = slice(t * cap, (t + 1) * cap)
        req_ref[:, cols] = (16.0 * found[:, :cap] + found[:, cap : 2 * cap]).astype(I32)
        sample_ref[:, cols] = found[:, 2 * cap :]
        inv = 1.0 / jnp.maximum(live_count, 1.0)
        column = jnp.sum(
            jnp.where(iota(square, 0) == iota(square, 1), inv, 0.0), axis=1, keepdims=True
        )
        inv_ref[t] = jnp.broadcast_to(column, square)


def own_lines(table, slots):
    groups, lanes = table.shape
    cap = slots // groups
    mine = iota((cap, lanes), 1) % cap == iota((cap, lanes), 0)
    return jnp.concatenate(
        [
            jnp.where(mine, jnp.broadcast_to(table[o : o + 1], (cap, lanes)), 0.0)
            for o in range(groups)
        ],
        axis=0,
    ).astype(BF16)


def of_table(shape, lane_dim, t, kind, width, cap):
    lane = iota(shape, lane_dim)
    return flag((lane // width == kind) & (lane % width // cap == t))


def samples_kernel(sample_ref, pick_ref, row_ref):
    tabs, slots, toks = pick_ref.shape
    width = sample_ref.shape[1]
    cap = width // tabs
    own = own_lines(sample_ref[...], slots)
    wanted = (iota((slots, toks), 1) + 1).astype(F32)
    for t in range(tabs):
        mine = of_table((width, toks), 0, t, 0, width, cap)
        pick_ref[t] = flag(dot(own, mine) == wanted)
        row = dot(of_table((8, width), 1, t, 0, width, cap), own, NT)
        row_ref[t : t + 1, :] = row[0:1]


def labels_kernel(label_ref, out_ref):
    dims = out_ref.shape
    row = label_ref[...].astype(F32)
    column = jnp.sum(
        jnp.where(iota(dims, 0) == iota(dims, 1), row, 0.0), axis=1, keepdims=True
    )
    out_ref[...] = jnp.broadcast_to(column, dims)


def halves_of(arrived, block_rows):
    shift = block_rows.bit_length() - 1
    return jnp.concatenate(
        [(arrived >> shift).astype(F32), (arrived & (block_rows - 1)).astype(F32)], axis=1
    )


def fetch_kernel(
    arrived_ref, expired_ref, emb_ref, out_ref,
    gone_ref, held_ref, table_ref, sent_ref, in_sem, out_sem,
):
    groups, width = arrived_ref.shape
    tabs, rows, emb = emb_ref.shape
    cap = width // tabs
    half = rows // 2
    loads = [pltpu.make_async_copy(expired_ref, gone_ref, in_sem.at[tabs])] + [
        pltpu.make_async_copy(emb_ref.at[t], held_ref.at[t], in_sem.at[t]) for t in range(tabs)
    ]
    for load in loads:
        load.start()
    arrived = arrived_ref[...]
    place = (arrived & (half - 1)) + 1
    signed = jnp.where(arrived < half, place, -place).astype(F32).T.astype(BF16)
    parts = out_sem.shape[0]
    part = groups // parts
    lane = (iota((cap, emb), 1) + 1).astype(F32)
    names = lane.astype(BF16), (lane + emb).astype(BF16)
    one, zero = jnp.ones((cap, emb), BF16), jnp.zeros((cap, emb), BF16)
    stores = []
    for c in range(parts):
        mine = slice(c * part, (c + 1) * part)
        for t in range(tabs):
            if c == 0:
                if t == 0:
                    loads[0].wait()
                    gone = gone_ref[...].astype(F32).T.astype(BF16)
                loads[t + 1].wait()
                for at in range(2):
                    table = held_ref[t, at * half : (at + 1) * half, :].astype(BF16)
                    lost = jnp.broadcast_to(gone[at * half : (at + 1) * half, t : t + 1], table.shape)
                    table_ref[t, :, at * emb : (at + 1) * emb] = jnp.where(
                        lost == jnp.zeros_like(lost), table, jnp.zeros_like(table)
                    )
            lines = slice(t * cap, (t + 1) * cap)
            picks, first = [], []
            for o in range(c * part, (c + 1) * part):
                row = jnp.broadcast_to(signed[lines, o : o + 1], (cap, emb))
                at = jnp.abs(row)
                picks.append(
                    jnp.concatenate([jnp.where(at == n, one, zero) for n in names], axis=1)
                )
                first.append(row > zero)
            both = dot(jnp.concatenate(picks, axis=0), table_ref[t]).astype(BF16)
            line = jnp.where(jnp.concatenate(first, axis=0), both[:, :emb], both[:, emb:])
            sent_ref[mine, lines, :] = line.reshape(part, cap, emb)
        store = pltpu.make_async_copy(sent_ref.at[mine], out_ref.at[mine], out_sem.at[c])
        store.start()
        stores.append(store)
    for store in stores:
        store.wait()


def wanted_kernel(arrived_ref, row_ref):
    width = arrived_ref.shape[1]
    tabs, _, slots = row_ref.shape
    cap = width // tabs
    own = own_lines(halves_of(arrived_ref[...], 128), slots)
    for t in range(tabs):
        for kind in range(2):
            row_ref[t, 8 * kind : 8 * kind + 8, :] = dot(
                of_table((8, 2 * width), 1, t, kind, width, cap), own, NT
            )


def sublanes(length, wide):
    column = iota((length, 128), 0).astype(F32).astype(BF16)
    return jnp.concatenate([column] * (wide // 128), axis=1)


def down(row, length):
    return jnp.concatenate([row] * (length // 8), axis=0).astype(BF16)


def pool_kernel(rows_ref, sample_ref, inv_ref, out_ref):
    groups, width, emb = rows_ref.shape
    tabs, toks, _ = inv_ref.shape
    cap = width // tabs
    slots = groups * cap
    one, zero = jnp.ones((toks, slots), BF16), jnp.zeros((toks, slots), BF16)
    samples = sublanes(toks, slots)
    for t in range(tabs):
        row = jnp.broadcast_to(sample_ref[t : t + 1, :] - 1.0, (16, slots)).astype(BF16)
        pick = jnp.where(jnp.concatenate([row] * (toks // 16), axis=0) == samples, one, zero)
        pooled = dot(pick, rows_ref[:, t * cap : (t + 1) * cap, :].reshape(slots, emb))
        feature = (pooled * inv_ref[t]).astype(BF16)
        for k in range(out_ref.shape[0]):
            out_ref[k, :, t * emb : (t + 1) * emb] = feature


def silu_slope(preact):
    sig = jax.nn.sigmoid(preact)
    return sig * (1.0 + preact * (1.0 - sig))


def dense_kernel(
    at_ref, feat_ref, own_ref, near_ref, far_ref, u0, u1, u2, u3, labels_ref,
    logits_ref, grad_ref, mine_ref, other_ref,
):
    parts, toks, feats = feat_ref.shape
    units = (u0, u1, u2, u3)
    me, core = at_ref[0], at_ref[1]
    order = [(2 * core + q) % parts for q in range(parts)]
    preacts, scores = [], []
    for k, u in enumerate(units):
        pre = jnp.zeros((toks, u.shape[1]), F32)
        for q, at in enumerate(order):
            if k == 0:
                w = own_ref[pl.ds(pl.multiple_of(at * feats, feats), feats), :]
            else:
                half = near_ref if q < parts // 2 else far_ref
                start = q % (parts // 2) * feats
                w = half[k - 1, start : start + feats, :]
            pre = pre + dot(feat_ref[at], w)
        hidden = jax.nn.silu(pre).astype(BF16).astype(F32)
        preacts.append(pre)
        scores.append(jnp.sum(hidden * u[...], axis=1, keepdims=True))
    logits = jnp.zeros((toks, 1), F32)
    for shard in range(parts):
        far = (me + parts - shard) % parts
        score = scores[0]
        for k in range(1, parts):
            score = jnp.where(far == k, scores[k], score)
        logits = logits + score
    dlogit = (jax.nn.sigmoid(logits) - labels_ref[...])[:, 0:1]
    logits_ref[...] = jnp.broadcast_to(logits, logits_ref.shape)
    grads = jnp.zeros((toks, feats), F32)
    for k, (u, pre) in enumerate(zip(units, preacts)):
        dhidden = (dlogit * u[...] * silu_slope(pre)).astype(BF16)
        if k == 0:
            half = dhidden.shape[1] // 2
            low, high = dhidden[:, :half], dhidden[:, half:]
            mine, other = jnp.where(core == 0, low, high), jnp.where(core == 0, high, low)
            for q in range(parts):
                lines = slice(q * feats, (q + 1) * feats)
                part = dot(
                    feat_ref[q],
                    jnp.concatenate([mine, other], axis=1),
                    (((0,), (0,)), ((), ())),
                ).astype(BF16)
                mine_ref[lines, :] = part[:, :half]
                other_ref[lines, :] = part[:, half:]
            w = own_ref[pl.ds(pl.multiple_of(me * feats, feats), feats), :]
        else:
            lines = pl.ds(pl.multiple_of(me % (parts // 2) * feats, feats), feats)
            w = jnp.where(
                me // (parts // 2) == core, near_ref[k - 1, lines, :], far_ref[k - 1, lines, :]
            )
        grads = grads + dot(dhidden, w, NT)
    grad_ref[...] = grads


def spread_kernel(grad_ref, inv_ref, pick_ref, out_ref):
    slots = pick_ref.shape[1]
    cap, emb = out_ref.shape[1:]
    grad = (inv_ref[0] * grad_ref[...]).astype(BF16)
    out_ref[...] = dot(pick_ref[0], grad).astype(BF16).reshape(slots // cap, cap, emb)


def update_kernel(grads_ref, wanted_ref, emb_ref, expired_ref, acc_ref, new_ref, new_acc_ref):
    groups, _, emb = grads_ref.shape
    _, rows = expired_ref.shape
    slots = wanted_ref.shape[2]
    cap = slots // groups
    t = pl.program_id(0)
    lines = pl.ds(pl.multiple_of(t * cap, cap), cap)
    grads = grads_ref[:, lines, :].reshape(slots, emb)
    at = down(wanted_ref[0, 0:8, :], 16)
    low = down(wanted_ref[0, 8:16, :], 16)
    low = jnp.concatenate([low] * (emb // 16), axis=0)
    one, zero = jnp.ones((emb, slots), BF16), jnp.zeros((emb, slots), BF16)
    hot = jnp.where(low == sublanes(emb, slots), one, zero)
    picks = []
    for j in range(rows // emb):
        here = jnp.concatenate([at == jnp.full_like(at, j)] * (emb // 16), axis=0)
        picks.append(jnp.where(here, hot, zero))
    sums = dot(jnp.concatenate(picks, axis=0), grads)
    gone = expired_ref[pl.ds(t, 1), :]
    fresh_acc = jnp.where(gone == 1, ACC_RESET, acc_ref[pl.ds(t, 1), :])
    kept = jnp.where(gone == 1, 0.0, 1.0)
    diag = iota((emb, emb), 0) == iota((emb, emb), 1)
    for j in range(0, rows, emb):
        summed = sums[j : j + emb]
        cols = slice(j, j + emb)
        old = jnp.sum(jnp.where(diag, fresh_acc[:, cols], 0.0), axis=1, keepdims=True)
        keep = jnp.sum(jnp.where(diag, kept[:, cols], 0.0), axis=1, keepdims=True)
        acc = old + jnp.sum(summed * summed, axis=1, keepdims=True) * (1.0 / emb)
        fresh = jnp.where(keep > 0.5, emb_ref[0, j : j + emb, :], 0.0)
        new_ref[0, j : j + emb, :] = fresh - LEARN_RATE * summed / jnp.sqrt(acc)
        line = jnp.sum(jnp.where(diag, acc, 0.0), axis=0, keepdims=True)
        for table in range(acc_ref.shape[0]):

            @pl.when(t == table)
            def _(table=table, cols=cols, line=line):
                new_acc_ref[table : table + 1, cols] = line


def shape(dims, dtype):
    return jax.ShapeDtypeStruct(dims, dtype)


def block(dims, index=None):
    if index is None:
        return pl.BlockSpec(dims, lambda *_: (0,) * len(dims))
    return pl.BlockSpec(dims, index)


def params(mib):
    return pltpu.CompilerParams(vmem_limit_bytes=mib << 20)


def cost(flops):
    return pl.CostEstimate(flops=flops, bytes_accessed=1 << 20, transcendentals=0)


def a2a(value, axis):
    return lax.all_to_all(value, axis, split_axis=0, concat_axis=0, tiled=True)


def from_everyone(value, axis):
    size = lax.axis_size(axis)
    return a2a(jnp.broadcast_to(value[None], (size, *value.shape)), axis)


def ring(value, axis, step):
    size = lax.axis_size(axis)
    return lax.ppermute(value, axis, [(i, (i + step) % size) for i in range(size)])


def shards(
    bag_lengths, owners, row_slots, admit_mask, expired, embeddings, accumulator,
    hidden_weight, output_weight, labels,
):
    groups = lax.axis_size(DP)
    parts = lax.axis_size("mp")
    tabs, toks, bag = row_slots.shape
    rows, emb = embeddings.shape[1:]
    cap = 2 * toks * bag // groups
    width = tabs * cap
    slots = groups * cap
    feats = tabs * emb
    core = lax.axis_index(NEAR).astype(I32)
    place = jnp.stack([lax.axis_index("mp").astype(I32), core])

    request, sample, inv = pl.pallas_call(
        slots_kernel,
        out_shape=(
            shape((groups, width), I32),
            shape((groups, width), F32),
            shape((tabs, toks, toks), F32),
        ),
        compiler_params=params(24),
        name="slots",
    )(
        *map(
            functools.partial(pltpu.with_memory_space_constraint, memory_space=pltpu.HBM),
            (
                bag_lengths,
                owners[..., 0].swapaxes(1, 2),
                row_slots.swapaxes(1, 2),
                admit_mask.swapaxes(1, 2),
            ),
        )
    )
    arrived = a2a(request, DP)
    lines, units_dev = hidden_weight.shape
    weight, _ = lax.optimization_barrier((hidden_weight, request))
    mine = lax.dynamic_slice(weight, (core * (lines // 2), 0), (lines // 2, units_dev))
    near_weights = jnp.stack([ring(mine, "mp", k) for k in range(1, parts)])
    far_weights = ring(near_weights, NEAR, 1)
    pick, sample_row = pl.pallas_call(
        samples_kernel,
        out_shape=(
            pltpu.HBM((tabs, slots, toks), BF16),
            shape((tabs, slots), F32),
        ),
        compiler_params=params(24),
        cost_estimate=cost(4 << 30),
        name="samples",
    )(sample)
    held = functools.partial(pltpu.with_memory_space_constraint, memory_space=pltpu.HBM)
    smem, vmem, hbm = (
        pl.BlockSpec(memory_space=space) for space in (pltpu.SMEM, pltpu.VMEM, pltpu.HBM)
    )
    dma = pltpu.SemaphoreType.DMA
    fetched = pl.pallas_call(
        fetch_kernel,
        in_specs=[vmem, hbm, hbm],
        out_specs=hbm,
        out_shape=pltpu.HBM((groups, width, emb), BF16),
        scratch_shapes=[
            pltpu.VMEM((tabs, rows), I32),
            pltpu.VMEM((tabs, rows, emb), F32),
            pltpu.VMEM((tabs, rows // 2, 2 * emb), BF16),
            pltpu.VMEM((groups, width, emb), BF16),
            dma((tabs + 1,)),
            dma((8,)),
        ],
        compiler_params=params(24),
        name="fetch",
    )(arrived, held(expired), held(embeddings))
    returned = a2a(fetched, DP)
    unit, later = lax.optimization_barrier((output_weight, arrived))
    unit = unit.reshape(1, -1)
    units = [unit] + [ring(unit, "mp", k) for k in range(1, parts)]
    wanted = pl.pallas_call(
        wanted_kernel,
        out_shape=pltpu.HBM((tabs, 16, slots), F32),
        compiler_params=params(24),
        cost_estimate=cost(4 << 30),
        name="wanted",
    )(later)
    features = pl.pallas_call(
        pool_kernel,
        out_shape=shape((parts, toks, feats), BF16),
        compiler_params=params(24),
        name="pool",
    )(returned, sample_row, inv)
    features, place, near_weights, far_weights, units = lax.optimization_barrier(
        (features, place, near_weights, far_weights, units)
    )
    portion = a2a(features, "mp")
    label_column = pl.pallas_call(
        labels_kernel,
        out_shape=shape((toks, toks), F32),
        compiler_params=params(4),
        name="labels",
    )(labels.reshape(1, toks))
    half = units_dev // 2
    logits, grad, mine, other = pl.pallas_call(
        dense_kernel,
        in_specs=[smem] + [vmem] * (parts + 5),
        out_shape=(
            shape((toks, toks), F32),
            shape((toks, feats), F32),
            shape((lines, half), BF16),
            shape((lines, half), BF16),
        ),
        compiler_params=params(24),
        name="dense",
    )(place, portion, held(hidden_weight), near_weights, far_weights, *units, label_column)
    joined = ring(other, NEAR, 1)
    share = lines // groups
    outgoing = pl.pallas_call(
        spread_kernel,
        grid=(tabs,),
        in_specs=[
            block((toks, emb), lambda t: (0, t)),
            block((1, toks, toks), lambda t: (t, 0, 0)),
            block((1, slots, toks), lambda t: (t, 0, 0)),
        ],
        out_specs=block((groups, cap, emb), lambda t: (0, t, 0)),
        out_shape=shape((groups, width + share, emb), BF16),
        compiler_params=params(24),
        cost_estimate=cost(4 << 30),
        name="spread",
    )(grad, inv, pick)
    pair = (mine.astype(F32) + joined.astype(F32)).astype(BF16)
    pair = pair.reshape(2, groups // 2, share, half).swapaxes(0, 1)
    outgoing = lax.dynamic_update_slice(
        outgoing, pair.reshape(groups, share, half), (0, width, 0)
    )
    gradients = a2a(outgoing, DP)
    shares = gradients[:, width:].reshape(groups // 2, 2, 2, share // 2, half)
    own = shares.astype(F32).sum(axis=0).astype(BF16).swapaxes(0, 1)
    near = from_everyone(own, FAR)
    near = near.transpose(0, 1, 3, 2, 4).reshape(lines // 2, units_dev)
    far = ring(near, NEAR, 1)
    weight_grad = jnp.concatenate(
        [jnp.where(core == 0, near, far), jnp.where(core == 0, far, near)]
    )
    new_rows, new_acc = pl.pallas_call(
        update_kernel,
        grid=(tabs,),
        in_specs=[
            vmem,
            block((1, 16, slots), lambda t: (t, 0, 0)),
            block((1, rows, emb), lambda t: (t, 0, 0)),
            block((tabs, rows)),
            block((tabs, rows)),
        ],
        out_specs=(
            block((1, rows, emb), lambda t: (t, 0, 0)),
            block((tabs, rows)),
        ),
        out_shape=(shape(embeddings.shape, F32), shape(accumulator.shape, F32)),
        compiler_params=params(24),
        cost_estimate=cost(4 << 30),
        name="update",
    )(gradients, held(wanted), held(embeddings), expired, accumulator)
    return (new_rows, new_acc, weight_grad, logits[:, 0])


def solution(mesh):
    split = Mesh(mesh.devices.reshape(8, 8, 2, mesh.shape["mp"]), (*DP, "mp"))

    return jax.shard_map(
        shards,
        mesh=split,
        in_specs=(
            P("mp", DP),
            P("mp", DP, None, None),
            P("mp", DP, None),
            P("mp", DP, None),
            P("mp", DP),
            P("mp", DP, None),
            P("mp", DP),
            P(None, "mp"),
            P("mp"),
            P(DP),
        ),
        out_specs=(P("mp", DP, None), P("mp", DP), P(None, "mp"), P(DP)),
        check_vma=False,
    )
```
